128 devices in a mesh: dp: 1, tp: 128 (over z, y, x, core).
Axes of the slice: x: 4, y: 4, z: 4, core: 2. Of those that a mesh axis runs over, the one named last changes fastest.
Arguments:
- x_rows: bfloat16 [4096, 16384], P(('dp', 'tp'))
- norm_gain: float32 [16384], replicated
- w_q: bfloat16 [16384, 128, 128], P(None, 'tp')
- w_k: bfloat16 [16384, 1024], P(None, 'tp')
- w_v: bfloat16 [16384, 1024], P(None, 'tp')
Outputs:
- output 1: bfloat16 [4096, 128, 128], P('dp', 'tp')
- output 2: bfloat16 [4096, 128, 128], P('dp', 'tp')
- output 3: bfloat16 [4096, 128, 128], P('dp', 'tp')
All inputs are finite; a program needn't handle non-finite values.
Results may differ from the reference program's by a relative error of at most 0.001.
Values are sent between devices in bfloat16 or wider.
A program may use at most 1 GiB of HBM per device.

```python
import jax
import jax.numpy as jnp
from jax import lax

TOKENS = 4096
D_MODEL = 16384
Q_HEADS = 128
KV_COUNT = 8
HEAD_DIM = 128
GROUP_SIZE = 128
EPSILON = 1e-6


def setup_inputs(seed: int = 0, part: int = 0) -> dict:
    key = jax.random.key(seed)
    shared_key, rows_key = jax.random.split(key)
    part_key = jax.random.fold_in(rows_key, part)
    x_rows = jax.random.normal(part_key, (TOKENS, D_MODEL), jnp.float32).astype(jnp.bfloat16)
    gain_key, q_key, k_key, v_key = jax.random.split(shared_key, 4)
    norm_gain = jax.random.uniform(gain_key, (D_MODEL,), jnp.float32, 0.4, 1.6)
    weight_scale = D_MODEL ** -0.5
    w_q = (jax.random.normal(q_key, (D_MODEL, Q_HEADS, HEAD_DIM), jnp.float32) * weight_scale).astype(jnp.bfloat16)
    w_k = (jax.random.normal(k_key, (D_MODEL, KV_COUNT * HEAD_DIM), jnp.float32) * weight_scale).astype(jnp.bfloat16)
    w_v = (jax.random.normal(v_key, (D_MODEL, KV_COUNT * HEAD_DIM), jnp.float32) * weight_scale).astype(jnp.bfloat16)
    return {"x_rows": x_rows, "norm_gain": norm_gain, "w_q": w_q, "w_k": w_k, "w_v": w_v}


def reference(x_rows, norm_gain, w_q, w_k, w_v):
    x_wide = x_rows.astype(jnp.float32)
    mean_sq = jnp.mean(x_wide * x_wide, axis=-1, keepdims=True)
    normed = (x_wide * lax.rsqrt(mean_sq + EPSILON) * norm_gain).astype(jnp.bfloat16)
    q_flat = jnp.dot(normed, w_q.reshape(D_MODEL, Q_HEADS * HEAD_DIM), preferred_element_type=jnp.float32)
    q_out = q_flat.astype(jnp.bfloat16).reshape(TOKENS, Q_HEADS, HEAD_DIM)
    head_share = GROUP_SIZE // KV_COUNT
    k_flat = jnp.dot(normed, w_k, preferred_element_type=jnp.float32).astype(jnp.bfloat16)
    v_flat = jnp.dot(normed, w_v, preferred_element_type=jnp.float32).astype(jnp.bfloat16)
    k_out = jnp.repeat(k_flat.reshape(TOKENS, KV_COUNT, HEAD_DIM), head_share, axis=1)
    v_out = jnp.repeat(v_flat.reshape(TOKENS, KV_COUNT, HEAD_DIM), head_share, axis=1)
    return (q_out, k_out, v_out)
```

```python
import functools

import jax
import jax.numpy as jnp
from jax import lax
from jax.experimental import pallas as pl
from jax.experimental.pallas import tpu as pltpu
from jax.sharding import PartitionSpec as P

EPSILON = 1e-6
MESH = pl.DeviceIdType.MESH
DMA = pltpu.SemaphoreType.DMA


def rem(a, b):
    return lax.rem(a, b)


def kernel(
    depth, x_hbm, gain, wq_hbm, wkv_hbm, q_out, k_out, v_out,
    x_in, other, rows, wq, wkv, q_part, kv_part, q_got, kv_got, pieces, acc,
    load_sem, row_recv, wq_recv, wkv_recv, row_send, w_send, q_send, q_send_last, kv_send, q_recv, kv_recv,
    piece_send, piece_recv, pair_sem,
):
    half = depth // 2
    step = min(2048, half)
    steps = half // step
    me = lax.axis_index("tp")
    c = rem(me, 2)
    x = rem(me // 2, 4)
    y = rem(me // 8, 4)
    z = me // 32
    u = z + c * (y - z)
    v = y + c * (z - y)
    mate = me + 1 - 2 * c
    d = 1 - c

    def chip(xx, uu, vv):
        zz = uu + c * (vv - uu)
        yy = vv + c * (uu - vv)
        return ((zz * 4 + yy) * 4 + xx) * 2

    def plus(a, n):
        return rem(a + n, 4)

    def send(src, dst, send_sem, recv_sem, target):
        copy = pltpu.make_async_remote_copy(
            src_ref=src, dst_ref=dst, send_sem=send_sem, recv_sem=recv_sem, device_id={"tp": target}, device_id_type=MESH
        )
        copy.start()

    def got(ref, sem):
        pltpu.make_async_copy(ref, ref, sem).wait()

    load_x = pltpu.make_async_copy(x_hbm, x_in, load_sem.at[0])
    load_x.start()
    own_columns = pl.ds(pl.multiple_of(c * half, half), half)
    mate_columns = pl.ds(pl.multiple_of(d * half, half), half)
    load_wq = pltpu.make_async_copy(wq_hbm.at[own_columns, :], wq.at[u, c], load_sem.at[1])
    load_wq.start()
    load_wkv = pltpu.make_async_copy(wkv_hbm.at[:, own_columns], wkv.at[u, c], load_sem.at[2])
    load_wkv.start()

    barrier = pltpu.get_barrier_semaphore()
    y_pair = y + 1 - 2 * rem(y, 2)
    peers = [mate]
    for n in (1, 2, 3):
        for k in (0, 1):
            peers.append(((z * 4 + plus(y, n)) * 4 + x) * 2 + k)
            peers.append(((plus(z, n) * 4 + y) * 4 + x) * 2 + k)
        peers.append(((z * 4 + y) * 4 + plus(x, n)) * 2 + c)
        peers.append(((z * 4 + y_pair) * 4 + plus(x, n)) * 2 + c)
    for peer in peers:
        pl.semaphore_signal(barrier, inc=1, device_id={"tp": peer}, device_id_type=MESH)
    pl.semaphore_wait(barrier, len(peers))

    counts = {"row": 0, "w": 0}

    def send_row(xx, vv, k, target):
        send(rows.at[xx, vv, k], rows.at[xx, vv, k], row_send.at[counts["row"]], row_recv.at[xx, vv, k], target)
        counts["row"] += 1

    def row_got(xx, vv, k):
        got(rows.at[xx, vv, k], row_recv.at[xx, vv, k])

    def send_w(uu, k, target, q_src=None, kv_src=None, to=None):
        to = uu if to is None else to
        q_src = wq.at[uu, k] if q_src is None else q_src
        kv_src = wkv.at[uu, k] if kv_src is None else kv_src
        send(q_src, wq.at[to, k], w_send.at[counts["w"], 0], wq_recv.at[to, k], target)
        send(kv_src, wkv.at[to, k], w_send.at[counts["w"], 1], wkv_recv.at[to, k], target)
        counts["w"] += 1

    def w_got(uu, k):
        got(wq.at[uu, k], wq_recv.at[uu, k])
        got(wkv.at[uu, k], wkv_recv.at[uu, k])

    x_next, x_last = chip(plus(x, 1), u, v) + c, chip(plus(x, 3), u, v) + c
    v_next, v_last = chip(x, u, plus(v, 1)) + c, chip(x, u, plus(v, 3)) + c
    u_next, u_last = chip(x, plus(u, 1), v) + c, chip(x, plus(u, 3), v) + c

    send_w(u, c, mate, wq_hbm.at[mate_columns, :], wkv_hbm.at[:, mate_columns], to=v)
    send_w(u, c, u_next, wq_hbm.at[own_columns, :], wkv_hbm.at[:, own_columns])
    send_w(u, c, u_last, wq_hbm.at[own_columns, :], wkv_hbm.at[:, own_columns])

    load_x.wait()
    width = min(1024, half)

    def squares(j, total):
        part = x_in[:, pl.ds(pl.multiple_of(j * width, width), width)].astype(jnp.float32)
        return total + part * part

    total = lax.fori_loop(0, depth // width, squares, jnp.zeros((32, width), jnp.float32))
    scale = lax.rsqrt(jnp.sum(total, axis=1, keepdims=True) / depth + EPSILON)

    def normed(first):
        columns = pl.ds(pl.multiple_of(first, width), width)
        return (x_in[:, columns].astype(jnp.float32) * scale * gain[:, columns]).astype(jnp.bfloat16)

    @pl.loop(0, half // width)
    def _(j):
        columns = pl.ds(pl.multiple_of(j * width, width), width)
        other[:, columns] = normed(d * half + j * width)
        rows[x, v, c, :, columns] = normed(c * half + j * width)

    send(other, rows.at[x, u, c], row_send.at[counts["row"]], row_recv.at[x, u, c], mate)
    counts["row"] += 1
    for target in (x_next, x_last, v_next, v_last):
        send_row(x, v, c, target)
    row_got(x, v, d)
    for target in (x_next, x_last, v_next, v_last):
        send_row(x, v, d, target)
    w_got(u, d)
    send_w(u, d, u_next)
    send_w(u, d, u_last)

    row_got(x, plus(v, 3), c)
    send_row(x, plus(v, 3), c, v_next)
    row_got(plus(x, 3), v, c)
    send_row(plus(x, 3), v, c, x_next)
    row_got(x, plus(v, 1), c)
    for near in (3, 1):
        send_row(x, plus(v, near), c, x_next)
        send_row(x, plus(v, near), c, x_last)
    row_got(x, plus(v, 1), d)
    send_row(x, plus(v, 1), d, v_last)
    row_got(plus(x, 1), v, d)
    send_row(plus(x, 1), v, d, x_last)
    row_got(x, plus(v, 3), d)
    for near in (3, 1):
        send_row(x, plus(v, near), d, x_next)
        send_row(x, plus(v, near), d, x_last)
    for k in (c, d):
        row_got(x, plus(v, 2), k)
        send_row(x, plus(v, 2), k, x_next)
        send_row(x, plus(v, 2), k, x_last)

    def forward_x(vv):
        row_got(plus(x, 3), vv, c)
        send_row(plus(x, 3), vv, c, x_next)
        row_got(plus(x, 1), vv, d)
        send_row(plus(x, 1), vv, d, x_last)

    w_got(plus(u, 3), c)
    send_w(plus(u, 3), c, u_next)
    forward_x(plus(v, 3))
    w_got(plus(u, 1), d)
    send_w(plus(u, 1), d, u_last)
    forward_x(plus(v, 1))
    forward_x(plus(v, 2))
    for n in range(4):
        row_got(plus(x, 3), plus(v, n), d)
        row_got(plus(x, 1), plus(v, n), c)
    load_wq.wait()
    load_wkv.wait()
    w_got(plus(u, 3), d)
    w_got(plus(u, 1), c)
    w_got(plus(u, 2), c)
    w_got(plus(u, 2), d)

    def depth_slice(j):
        return pl.ds(pl.multiple_of(j * step, step), step)

    def q_product(load_rows, count, store):
        @pl.loop(0, 4)
        def _(uu):
            @pl.loop(0, steps)
            def _(j):
                right = jnp.concatenate([wq[uu, 0, depth_slice(j), :], wq[uu, 1, depth_slice(j), :]], axis=1)
                term = jnp.dot(load_rows(j), right, preferred_element_type=jnp.float32)

                @pl.when(j == 0)
                def _():
                    acc[pl.ds(0, count), :] = term

                @pl.when(j > 0)
                def _():
                    acc[pl.ds(0, count), :] += term

            for k in (0, 1):
                store(uu, k, acc[pl.ds(0, count), pl.ds(k * 128, 128)])

    targets = []
    for du in range(4):
        for dk in (0, 1):
            if du or dk:
                targets.append((plus(u, du), rem(c + dk, 2)))

    @pl.loop(0, 3)
    def _(g):
        xx = plus(x, g + g // 2)

        def store(uu, k, value):
            q_part[xx, uu, k] = value.reshape(4, 64, 128)

        q_product(lambda j: rows[xx, :, :, :, depth_slice(j)].reshape(256, step), 256, store)
        for n, (uu, k) in enumerate(targets):
            send(q_part.at[xx, uu, k], q_got.at[c, u, xx], q_send.at[g, n], q_recv.at[c, u], chip(x, uu, v) + k)

    far = plus(x, 2)

    @pl.loop(0, 4)
    def _(t):
        vv = plus(v, t + (t // 2) * (1 - 2 * (t // 3)))
        row_got(far, vv, c)
        row_got(far, vv, d)

        def store(uu, k, value):
            q_part[far, uu, k, vv] = value

        q_product(lambda j: rows[far, vv, :, :, depth_slice(j)].reshape(64, step), 64, store)
        for n, (uu, k) in enumerate(targets):
            send(q_part.at[far, uu, k, vv], q_got.at[c, u, far, vv], q_send_last.at[t, n], q_recv.at[c, u], chip(x, uu, v) + k)

        @pl.loop(0, steps)
        def _(j):
            term = lax.dot_general(
                wkv[:, :, :, depth_slice(j)].reshape(128, step),
                rows[:, vv, :, :, depth_slice(j)].reshape(256, step),
                (((1,), (1,)), ((), ())),
                preferred_element_type=jnp.float32,
            )

            @pl.when(j == 0)
            def _():
                acc[pl.ds(0, 128), :] = term

            @pl.when(j > 0)
            def _():
                acc[pl.ds(0, 128), :] += term

        kv_part[vv] = acc[pl.ds(0, 128), :].reshape(4, 2, 16, 256)
        for n, (uu, k) in enumerate(targets):
            send(kv_part.at[vv, uu, k], kv_got.at[c, u, vv], kv_send.at[t, n], kv_recv.at[c, u], chip(x, uu, v) + k)

    for n in range(4):
        q_got[c, u, n] = q_part[n, u, c]
        kv_got[c, u, n] = kv_part[n, u, c]
    for n in (1, 2, 3):
        got(kv_got.at[c, plus(u, n)], kv_recv.at[c, plus(u, n)])
    for n in range(4):
        got(kv_got.at[d, n], kv_recv.at[d, n])

    place = rem(y, 2) * 4 + x
    for zz in range(4):
        for yy in range(4):
            pieces[c, place, :, pl.ds((zz * 4 + yy) * 256, 256)] = (kv_got[0, zz, yy] + kv_got[1, yy, zz]).astype(jnp.bfloat16)
    for n in range(1, 8):
        there = rem(place + n, 8)
        target = ((z * 4 + (y // 2) * 2 + there // 4) * 4 + rem(there, 4)) * 2 + c
        send(pieces.at[c, place], pieces.at[c, place], piece_send.at[n], piece_recv.at[place], target)

    for n in (1, 2, 3):
        got(q_got.at[c, plus(u, n)], q_recv.at[c, plus(u, n)])
    for n in range(4):
        got(q_got.at[d, n], q_recv.at[d, n])

    @pl.loop(0, 4)
    def _(zz):
        @pl.loop(0, 4)
        def _(yy):
            for xx in range(4):
                q_out[zz, yy, xx] = (q_got[0, zz, xx, yy] + q_got[1, yy, xx, zz]).astype(jnp.bfloat16)

    for n in range(1, 8):
        there = rem(place + n, 8)
        got(pieces.at[c, there], piece_recv.at[there])
    pair = pltpu.make_async_remote_copy(
        src_ref=pieces.at[c], dst_ref=pieces.at[c], send_sem=pair_sem.at[0], recv_sem=pair_sem.at[1],
        device_id={"tp": mate}, device_id_type=MESH,
    )
    pair.start()
    got(pieces.at[d], pair_sem.at[1])

    @pl.loop(0, 16)
    def _(b):
        columns = pl.ds(pl.multiple_of(b * 256, 256), 256)
        wide = [pieces[k, n, :, columns].astype(jnp.float32) for n in range(8) for k in (0, 1)]
        out_rows = pl.ds(pl.multiple_of(b * 256, 256), 256)
        k_out[out_rows, :] = jnp.concatenate([w[0:8] for w in wide], axis=0).T.astype(jnp.bfloat16)
        v_out[out_rows, :] = jnp.concatenate([w[8:16] for w in wide], axis=0).T.astype(jnp.bfloat16)

    def left(ref, sem):
        pltpu.make_async_copy(ref, ref, sem).wait()

    for n in range(counts["row"]):
        left(rows.at[0, 0, 0], row_send.at[n])
    for n in range(counts["w"]):
        left(wq.at[0, 0], w_send.at[n, 0])
        left(wkv.at[0, 0], w_send.at[n, 1])
    for n in range(len(targets)):
        for g in range(3):
            left(q_part.at[0, 0, 0], q_send.at[g, n])
        for t in range(4):
            left(q_part.at[0, 0, 0, 0], q_send_last.at[t, n])
            left(kv_part.at[0, 0, 0], kv_send.at[t, n])
    for n in range(1, 8):
        left(pieces.at[0, 0], piece_send.at[n])
    left(pieces.at[0], pair_sem.at[0])


def solution(mesh):
    def local_step(x_rows, norm_gain, w_q, w_k, w_v):
        depth = x_rows.shape[1]
        half = depth // 2
        gain = norm_gain.reshape(1, depth)
        wq = w_q.reshape(depth, 128)
        wkv = jnp.concatenate([w_k.T, w_v.T], axis=0)
        any_space = pl.BlockSpec(memory_space=pl.ANY)
        vmem = pl.BlockSpec(memory_space=pltpu.VMEM)
        bf16, f32 = jnp.bfloat16, jnp.float32
        q, k, v = pl.pallas_call(
            functools.partial(kernel, depth),
            out_shape=(
                jax.ShapeDtypeStruct((4, 4, 4, 64, 128), bf16),
                jax.ShapeDtypeStruct((4096, 128), bf16),
                jax.ShapeDtypeStruct((4096, 128), bf16),
            ),
            in_specs=[any_space, vmem, any_space, any_space],
            out_specs=(vmem, vmem, vmem),
            scratch_shapes=[
                pltpu.VMEM((32, depth), bf16),
                pltpu.VMEM((32, half), bf16),
                pltpu.VMEM((4, 4, 2, 32, half), bf16),
                pltpu.VMEM((4, 2, half, 128), bf16),
                pltpu.VMEM((4, 2, 16, half), bf16),
                pltpu.VMEM((4, 4, 2, 4, 64, 128), f32),
                pltpu.VMEM((4, 4, 2, 16, 256), f32),
                pltpu.VMEM((2, 4, 4, 4, 64, 128), f32),
                pltpu.VMEM((2, 4, 4, 16, 256), f32),
                pltpu.VMEM((2, 8, 16, 4096), bf16),
                pltpu.VMEM((256, 256), f32),
                DMA((3,)),
                DMA((4, 4, 2)),
                DMA((4, 2)),
                DMA((4, 2)),
                DMA((31,)),
                DMA((7, 2)),
                DMA((3, 7)),
                DMA((4, 7)),
                DMA((4, 7)),
                DMA((2, 4)),
                DMA((2, 4)),
                DMA((8,)),
                DMA((8,)),
                DMA((2,)),
            ],
            compiler_params=pltpu.CompilerParams(collective_id=0, has_side_effects=True, vmem_limit_bytes=67043328),
        )(x_rows, gain, wq, wkv)
        return q.reshape(4096, 1, 128), k[:, None, :], v[:, None, :]

    return jax.shard_map(
        local_step,
        mesh=mesh,
        in_specs=(P(("dp", "tp"), None), P(None), P(None, "tp", None), P(None, "tp"), P(None, "tp")),
        out_specs=(P("dp", "tp", None), P("dp", "tp", None), P("dp", "tp", None)),
        check_vma=False,
    )
```

```python
import functools

import jax
import jax.numpy as jnp
from jax import lax
from jax.experimental import pallas as pl
from jax.experimental.pallas import tpu as pltpu
from jax.sharding import PartitionSpec as P

EPSILON = 1e-6
MESH = pl.DeviceIdType.MESH
DMA = pltpu.SemaphoreType.DMA


def rem(a, b):
    return lax.rem(a, b)


def kernel(
    depth, split, x_hbm, gain, wq_hbm, wk_hbm, wv_hbm, q_out, k_out, v_out,
    x_in, other, wkv_other, rows, wq, wkv, q_part, kv_part, q_got, kv_got, pieces,
    load_sem, wide_recv, thin_recv, row_send, wq_recv, wkv_recv, w_send, q_send, q_send_far, kv_send, q_recv, kv_recv,
    piece_send, piece_recv, pair_send, pair_recv,
):
    half = depth // 2
    me = lax.axis_index("tp")
    c = rem(me, 2)
    x = rem(me // 2, 4)
    y = rem(me // 8, 4)
    z = me // 32
    u = z + c * (y - z)
    v = y + c * (z - y)
    mate = me + 1 - 2 * c
    d = 1 - c

    def chip(xx, uu, vv):
        zz = uu + c * (vv - uu)
        yy = vv + c * (uu - vv)
        return ((zz * 4 + yy) * 4 + xx) * 2

    def plus(a, n):
        return rem(a + n, 4)

    def send(src, dst, send_sem, recv_sem, target):
        copy = pltpu.make_async_remote_copy(
            src_ref=src, dst_ref=dst, send_sem=send_sem, recv_sem=recv_sem, device_id={"tp": target}, device_id_type=MESH
        )
        copy.start()

    def got(ref, sem):
        pltpu.make_async_copy(ref, ref, sem).wait()

    load_x = pltpu.make_async_copy(x_hbm, x_in, load_sem.at[0])
    load_x.start()
    own_columns = pl.ds(pl.multiple_of(c * half, half), half)
    mate_columns = pl.ds(pl.multiple_of(d * half, half), half)
    loads = [
        pltpu.make_async_copy(wk_hbm.at[:, mate_columns], wkv_other.at[0:8], load_sem.at[1]),
        pltpu.make_async_copy(wv_hbm.at[:, mate_columns], wkv_other.at[8:16], load_sem.at[2]),
        pltpu.make_async_copy(wk_hbm.at[:, own_columns], wkv.at[u, c, 0:8], load_sem.at[3]),
        pltpu.make_async_copy(wv_hbm.at[:, own_columns], wkv.at[u, c, 8:16], load_sem.at[4]),
    ]
    for load in loads:
        load.start()
    load_wq = pltpu.make_async_copy(wq_hbm.at[own_columns, :], wq.at[u, c], load_sem.at[5])
    load_wq.start()

    barrier = pltpu.get_barrier_semaphore()
    y_pair = y + 1 - 2 * rem(y, 2)
    peers = [mate]
    for n in (1, 2, 3):
        for k in (0, 1):
            peers.append(((z * 4 + plus(y, n)) * 4 + x) * 2 + k)
            peers.append(((plus(z, n) * 4 + y) * 4 + x) * 2 + k)
        peers.append(((z * 4 + y) * 4 + plus(x, n)) * 2 + c)
        peers.append(((z * 4 + y_pair) * 4 + plus(x, n)) * 2 + c)
    for peer in peers:
        pl.semaphore_signal(barrier, inc=1, device_id={"tp": peer}, device_id_type=MESH)

    load_x.wait()
    width = min(1024, half)

    def squares(j, total):
        part = x_in[:, pl.ds(pl.multiple_of(j * width, width), width)].astype(jnp.float32)
        return total + part * part

    total = lax.fori_loop(0, depth // width, squares, jnp.zeros((32, width), jnp.float32))
    scale = lax.rsqrt(jnp.sum(total, axis=1, keepdims=True) / depth + EPSILON)

    def normed(first):
        columns = pl.ds(pl.multiple_of(first, width), width)
        return (x_in[:, columns].astype(jnp.float32) * scale * gain[:, columns]).astype(jnp.bfloat16)

    @pl.loop(0, half // width)
    def _(j):
        columns = pl.ds(pl.multiple_of(j * width, width), width)
        other[:, columns] = normed(d * half + j * width)
        rows[x, v, c, :, columns] = normed(c * half + j * width)

    for load in loads:
        load.wait()
    pl.semaphore_wait(barrier, len(peers))

    counts = {"row": 0, "w": 0, "kinds": []}
    wide, thin = slice(0, split), slice(split, half)

    def row_sem():
        counts["row"] += 1
        return row_send.at[counts["row"] - 1]

    def send_wide(xx, vv, k, *to):
        for target in to:
            send(rows.at[xx, vv, k, :, wide], rows.at[xx, vv, k, :, wide], row_sem(), wide_recv.at[xx, vv, k], target)
            counts["kinds"].append(wide)

    def send_thin(xx, vv, k, *to):
        for target in to:
            send(rows.at[xx, vv, k, :, thin], rows.at[xx, vv, k, :, thin], row_sem(), thin_recv.at[xx, vv, k], target)
            counts["kinds"].append(thin)

    def wide_got(xx, vv, k):
        got(rows.at[xx, vv, k, :, wide], wide_recv.at[xx, vv, k])

    def thin_got(xx, vv, k):
        got(rows.at[xx, vv, k, :, thin], thin_recv.at[xx, vv, k])

    def send_w(q_src, kv_src, uu, k, target):
        send(q_src, wq.at[uu, k], w_send.at[counts["w"], 0], wq_recv.at[uu, k], target)
        send(kv_src, wkv.at[uu, k], w_send.at[counts["w"], 1], wkv_recv.at[uu, k], target)
        counts["w"] += 1

    def pass_w(uu, k, target):
        send_w(wq.at[uu, k], wkv.at[uu, k], uu, k, target)

    def w_got(uu, k):
        got(wq.at[uu, k], wq_recv.at[uu, k])
        got(wkv.at[uu, k], wkv_recv.at[uu, k])

    x_next, x_last = chip(plus(x, 1), u, v) + c, chip(plus(x, 3), u, v) + c
    v_next, v_last = chip(x, u, plus(v, 1)) + c, chip(x, u, plus(v, 3)) + c
    u_next, u_last = chip(x, plus(u, 1), v) + c, chip(x, plus(u, 3), v) + c
    xp, xm, xo = plus(x, 1), plus(x, 3), plus(x, 2)
    vp, vm, vo = plus(v, 1), plus(v, 3), plus(v, 2)
    up, um, uo = plus(u, 1), plus(u, 3), plus(u, 2)

    send(other, rows.at[x, u, c], row_sem(), wide_recv.at[x, u, c], mate)
    send_thin(x, v, c, x_next, x_last)
    send_wide(x, v, c, v_next, v_last)
    send_w(wq_hbm.at[own_columns, :], wkv.at[u, c], u, c, u_next)
    send_w(wq_hbm.at[own_columns, :], wkv.at[u, c], u, c, u_last)
    send_w(wq_hbm.at[mate_columns, :], wkv_other, v, c, mate)
    got(rows.at[x, v, d], wide_recv.at[x, v, d])
    send_thin(x, v, d, x_next, x_last)
    send_wide(x, v, c, x_next, x_last)
    send_wide(x, v, d, x_next, x_last, v_next, v_last)
    for k in (c, d):
        send_thin(x, v, k, v_next, v_last)
    w_got(u, d)
    pass_w(u, d, u_next)
    pass_w(u, d, u_last)

    thin_got(xm, v, c)
    send_thin(xm, v, c, x_next)
    thin_got(xp, v, d)
    send_thin(xp, v, d, x_last)
    thin_got(xm, v, d)
    thin_got(xp, v, c)
    for xx in (xm, xp):
        for k in (c, d):
            send_thin(xx, v, k, v_next, v_last)

    wide_got(x, vm, c)
    send_wide(x, vm, c, v_next)
    wide_got(xm, v, c)
    send_wide(xm, v, c, x_next)
    wide_got(x, vp, c)
    for vv in (vm, vp):
        send_wide(x, vv, c, x_next, x_last)
    wide_got(x, vp, d)
    send_wide(x, vp, d, v_last)
    wide_got(xp, v, d)
    send_wide(xp, v, d, x_last)
    wide_got(x, vm, d)
    for vv in (vm, vp):
        send_wide(x, vv, d, x_next, x_last)
    for k in (c, d):
        thin_got(xo, v, k)
        send_thin(xo, v, k, v_next, v_last)
    for k in (c, d):
        wide_got(x, vo, k)
        send_wide(x, vo, k, x_next, x_last)
    for xx in (x, xm, xp, xo):
        thin_got(xx, vm, c)
        send_thin(xx, vm, c, v_next)
        thin_got(xx, vp, d)
        send_thin(xx, vp, d, v_last)

    def forward_x(vv):
        wide_got(xm, vv, c)
        send_wide(xm, vv, c, x_next)
        wide_got(xp, vv, d)
        send_wide(xp, vv, d, x_last)

    targets = []
    for du in range(4):
        for dk in (0, 1):
            if du or dk:
                targets.append((plus(u, du), rem(c + dk, 2)))

    def q_block(xx, uu):
        right = jnp.concatenate([wq[uu, 0], wq[uu, 1]], axis=1)
        value = jnp.dot(rows[xx].reshape(256, half), right, preferred_element_type=jnp.float32)
        for k in (0, 1):
            q_part[xx, uu, k] = value[:, k * 128:(k + 1) * 128].reshape(4, 64, 128)

    def kv_block(xx):
        value = lax.dot_general(
            wkv[...].reshape(128, half), rows[xx].reshape(256, half), (((1,), (1,)), ((), ())), preferred_element_type=jnp.float32
        )
        kv_part[xx] = value.reshape(4, 2, 16, 256)

    def send_q(g, xx):
        for n, (uu, k) in enumerate(targets):
            send(q_part.at[xx, uu, k], q_got.at[c, u, xx], q_send.at[g, n], q_recv.at[c, u, xx], chip(x, uu, v) + k)
        q_got[c, u, xx] = q_part[xx, u, c]

    def send_kv(g, xx):
        for n, (uu, k) in enumerate(targets):
            send(kv_part.at[xx, uu, k], kv_got.at[c, u, xx], kv_send.at[g, n], kv_recv.at[c, u, xx], chip(x, uu, v) + k)
        kv_got[c, u, xx] = kv_part[xx, u, c]

    senders = [(c, plus(u, n)) for n in (1, 2, 3)] + [(d, n) for n in range(4)]
    place = rem(y, 2) * 4 + x

    def add_kv(g, xx):
        for role, n in senders:
            got(kv_got.at[role, n, xx], kv_recv.at[role, n, xx])
        for zz in range(4):
            second = jnp.concatenate([kv_got[1, yy, xx][:, zz * 64:(zz + 1) * 64] for yy in range(4)], axis=1)
            pieces[c, g, place, :, pl.ds(zz * 256, 256)] = (kv_got[0, zz, xx] + second).astype(jnp.bfloat16)
        for n in range(1, 8):
            there = rem(place + n, 8)
            target = ((z * 4 + (y // 2) * 2 + there // 4) * 4 + rem(there, 4)) * 2 + c
            send(pieces.at[c, g, place], pieces.at[c, g, place], piece_send.at[g, n], piece_recv.at[g, place], target)

    def add_q(xx):
        for role, n in senders:
            got(q_got.at[role, n, xx], q_recv.at[role, n, xx])

        @pl.loop(0, 4)
        def _(zz):
            for yy in range(4):
                q_out[zz, yy, xx] = (q_got[0, zz, xx, yy] + q_got[1, yy, xx, zz]).astype(jnp.bfloat16)

    def share_kv(g):
        for n in range(1, 8):
            there = rem(place + n, 8)
            got(pieces.at[c, g, there], piece_recv.at[g, there])
        send(pieces.at[c, g], pieces.at[c, g], pair_send.at[g], pair_recv.at[g], mate)

    def finish_kv():
        for g in range(4):
            got(pieces.at[d, g], pair_recv.at[g])

        @pl.loop(0, 4)
        def _(zz):
            columns = pl.ds(pl.multiple_of(zz * 256, 256), 256)
            for xx in range(4):
                places = [((0, 2, 3, 1)[(xx - n) % 4], n) for n in range(8)]
                wide_pieces = [pieces[k, g, n, :, columns].astype(jnp.float32) for g, n in places for k in (0, 1)]
                for out, first in ((k_out, 0), (v_out, 8)):
                    value = jnp.concatenate([w[first:first + 8] for w in wide_pieces], axis=0).T.astype(jnp.bfloat16)
                    out[zz, :, xx] = value.reshape(4, 64, 128)

    w_got(um, c)
    pass_w(um, c, u_next)
    forward_x(vm)
    load_wq.wait()
    for k in (c, d):
        thin_got(x, vo, k)
    for vv, k in ((vm, d), (vp, c)):
        thin_got(x, vv, k)
    q_block(x, u)
    w_got(up, d)
    pass_w(up, d, u_last)
    forward_x(vp)
    w_got(um, d)
    w_got(up, c)
    q_block(x, um)
    q_block(x, up)
    forward_x(vo)
    w_got(uo, c)
    w_got(uo, d)
    q_block(x, uo)
    send_q(0, x)
    kv_block(x)
    send_kv(0, x)

    def near_group(g, xx, k):
        for vv in (v, vm, vp, vo):
            wide_got(xx, vv, k)
        for vv, kk in ((vm, d), (vp, c), (vo, c), (vo, d)):
            thin_got(xx, vv, kk)

        @pl.loop(0, 4)
        def _(uu):
            q_block(xx, uu)

        send_q(g, xx)
        kv_block(xx)
        send_kv(g, xx)

    near_group(1, xm, d)
    add_kv(0, x)
    add_q(x)
    near_group(2, xp, c)
    add_kv(1, xm)
    add_q(xm)
    share_kv(0)

    for vv, kk in ((vm, d), (vp, c), (vo, c), (vo, d)):
        thin_got(xo, vv, kk)

    def far_rows(t, vv):
        @pl.loop(0, 4)
        def _(uu):
            right = jnp.concatenate([wq[uu, 0], wq[uu, 1]], axis=1)
            value = jnp.dot(rows[xo, vv].reshape(64, half), right, preferred_element_type=jnp.float32)
            for k in (0, 1):
                q_part[xo, uu, k, vv] = value[:, k * 128:(k + 1) * 128]

        for n, (uu, k) in enumerate(targets):
            send(q_part.at[xo, uu, k, vv], q_got.at[c, u, xo, vv], q_send_far.at[t, n], q_recv.at[c, u, xo], chip(x, uu, v) + k)
        q_got[c, u, xo, vv] = q_part[xo, u, c, vv]

    for t, vv in enumerate((v, vm, vp, vo)):
        wide_got(xo, vv, c)
        wide_got(xo, vv, d)
        if t == 3:
            kv_block(xo)
            send_kv(3, xo)
        far_rows(t, vv)
        if t == 0:
            add_kv(2, xp)
            add_q(xp)
            share_kv(1)
        if t == 1:
            share_kv(2)
    add_kv(3, xo)
    add_q(xo)
    share_kv(3)
    finish_kv()

    got(other, row_send.at[0])
    for n, kind in enumerate(counts["kinds"]):
        got(rows.at[0, 0, 0, :, kind], row_send.at[n + 1])
    for n in range(counts["w"]):
        got(wq.at[0, 0], w_send.at[n, 0])
        got(wkv.at[0, 0], w_send.at[n, 1])
    for n in range(len(targets)):
        for g in range(3):
            got(q_part.at[0, 0, 0], q_send.at[g, n])
        for t in range(4):
            got(q_part.at[0, 0, 0, 0], q_send_far.at[t, n])
            got(kv_part.at[0, 0, 0], kv_send.at[t, n])
    for g in range(4):
        for n in range(1, 8):
            got(pieces.at[0, 0, 0], piece_send.at[g, n])
        got(pieces.at[0, 0], pair_send.at[g])


def solution(mesh):
    def local_step(x_rows, norm_gain, w_q, w_k, w_v):
        depth = x_rows.shape[1]
        half = depth // 2
        any_space = pl.BlockSpec(memory_space=pl.ANY)
        vmem = pl.BlockSpec(memory_space=pltpu.VMEM)
        bf16, f32 = jnp.bfloat16, jnp.float32
        out = jax.ShapeDtypeStruct((4, 4, 4, 64, 128), bf16)
        outs = pl.pallas_call(
            functools.partial(kernel, depth, half - half // 8),
            out_shape=(out, out, out),
            in_specs=[any_space, vmem, any_space, any_space, any_space],
            out_specs=(vmem, vmem, vmem),
            scratch_shapes=[
                pltpu.VMEM((32, depth), bf16),
                pltpu.VMEM((32, half), bf16),
                pltpu.VMEM((16, half), bf16),
                pltpu.VMEM((4, 4, 2, 32, half), bf16),
                pltpu.VMEM((4, 2, half, 128), bf16),
                pltpu.VMEM((4, 2, 16, half), bf16),
                pltpu.VMEM((4, 4, 2, 4, 64, 128), f32),
                pltpu.VMEM((4, 4, 2, 16, 256), f32),
                pltpu.VMEM((2, 4, 4, 4, 64, 128), f32),
                pltpu.VMEM((2, 4, 4, 16, 256), f32),
                pltpu.VMEM((2, 4, 8, 16, 1024), bf16),
                DMA((6,)),
                DMA((4, 4, 2)),
                DMA((4, 4, 2)),
                DMA((61,)),
                DMA((4, 2)),
                DMA((4, 2)),
                DMA((7, 2)),
                DMA((3, 7)),
                DMA((4, 7)),
                DMA((4, 7)),
                DMA((2, 4, 4)),
                DMA((2, 4, 4)),
                DMA((4, 8)),
                DMA((4, 8)),
                DMA((4,)),
                DMA((4,)),
            ],
            compiler_params=pltpu.CompilerParams(collective_id=0, has_side_effects=True, vmem_limit_bytes=67043328),
        )(x_rows, norm_gain.reshape(1, depth), w_q.reshape(depth, 128), w_k.T, w_v.T)
        return tuple(value.reshape(4096, 1, 128) for value in outs)

    return jax.shard_map(
        local_step,
        mesh=mesh,
        in_specs=(P(("dp", "tp"), None), P(None), P(None, "tp", None), P(None, "tp"), P(None, "tp")),
        out_specs=(P("dp", "tp", None), P("dp", "tp", None), P("dp", "tp", None)),
        check_vma=False,
    )
```

```python
import functools

import jax
import jax.numpy as jnp
from jax import lax
from jax.experimental import pallas as pl
from jax.experimental.pallas import tpu as pltpu
from jax.sharding import PartitionSpec as P

EPSILON = 1e-6
MESH = pl.DeviceIdType.MESH
DMA = pltpu.SemaphoreType.DMA


def rem(a, b):
    return lax.rem(a, b)


def kernel(
    depth, split, x_hbm, gain, wq_hbm, wk_hbm, wv_hbm, q_out, k_out, v_out,
    x_in, other, wkv_other, rows, wq, wkv, q_part, kv_part, q_got, kv_got, pieces,
    load_sem, wide_recv, thin_recv, row_send, wq_recv, wkv_recv, wq_send, wkv_send, q_send, q_send_far, kv_send, q_recv,
    kv_recv,
    piece_send, piece_recv, pair_send, pair_recv,
):
    half = depth // 2
    me = lax.axis_index("tp")
    c = rem(me, 2)
    x = rem(me // 2, 4)
    y = rem(me // 8, 4)
    z = me // 32
    u = z + c * (y - z)
    v = y + c * (z - y)
    mate = me + 1 - 2 * c
    d = 1 - c

    def chip(xx, uu, vv):
        zz = uu + c * (vv - uu)
        yy = vv + c * (uu - vv)
        return ((zz * 4 + yy) * 4 + xx) * 2

    def plus(a, n):
        return rem(a + n, 4)

    def send(src, dst, send_sem, recv_sem, target):
        copy = pltpu.make_async_remote_copy(
            src_ref=src, dst_ref=dst, send_sem=send_sem, recv_sem=recv_sem, device_id={"tp": target}, device_id_type=MESH
        )
        copy.start()

    def got(ref, sem):
        pltpu.make_async_copy(ref, ref, sem).wait()

    load_x = pltpu.make_async_copy(x_hbm, x_in, load_sem.at[0])
    load_x.start()
    own_columns = pl.ds(pl.multiple_of(c * half, half), half)
    mate_columns = pl.ds(pl.multiple_of(d * half, half), half)
    loads = [
        pltpu.make_async_copy(wk_hbm.at[:, mate_columns], wkv_other.at[0:8], load_sem.at[1]),
        pltpu.make_async_copy(wv_hbm.at[:, mate_columns], wkv_other.at[8:16], load_sem.at[2]),
        pltpu.make_async_copy(wk_hbm.at[:, own_columns], wkv.at[u, c, 0:8], load_sem.at[3]),
        pltpu.make_async_copy(wv_hbm.at[:, own_columns], wkv.at[u, c, 8:16], load_sem.at[4]),
    ]
    for load in loads:
        load.start()
    load_wq = pltpu.make_async_copy(wq_hbm.at[own_columns, :], wq.at[u, c], load_sem.at[5])
    load_wq.start()

    barrier = pltpu.get_barrier_semaphore()
    y_pair = y + 1 - 2 * rem(y, 2)
    peers = [mate]
    for n in (1, 2, 3):
        for k in (0, 1):
            peers.append(((z * 4 + plus(y, n)) * 4 + x) * 2 + k)
            peers.append(((plus(z, n) * 4 + y) * 4 + x) * 2 + k)
        peers.append(((z * 4 + y) * 4 + plus(x, n)) * 2 + c)
        peers.append(((z * 4 + y_pair) * 4 + plus(x, n)) * 2 + c)
    for peer in peers:
        pl.semaphore_signal(barrier, inc=1, device_id={"tp": peer}, device_id_type=MESH)

    load_x.wait()
    width = min(1024, half)

    def squares(j, total):
        part = x_in[:, pl.ds(pl.multiple_of(j * width, width), width)].astype(jnp.float32)
        return total + part * part

    total = lax.fori_loop(0, depth // width, squares, jnp.zeros((32, width), jnp.float32))
    scale = lax.rsqrt(jnp.sum(total, axis=1, keepdims=True) / depth + EPSILON)

    def normed(first):
        columns = pl.ds(pl.multiple_of(first, width), width)
        return (x_in[:, columns].astype(jnp.float32) * scale * gain[:, columns]).astype(jnp.bfloat16)

    @pl.loop(0, half // width)
    def _(j):
        columns = pl.ds(pl.multiple_of(j * width, width), width)
        other[:, columns] = normed(d * half + j * width)
        rows[x, v, c, :, columns] = normed(c * half + j * width)

    for load in loads:
        load.wait()
    pl.semaphore_wait(barrier, len(peers))

    counts = {"row": 0, "wq": 0, "wkv": 0, "kinds": []}
    wide, thin = slice(0, split), slice(split, half)

    def row_sem():
        counts["row"] += 1
        return row_send.at[counts["row"] - 1]

    def send_wide(xx, vv, k, *to):
        for target in to:
            send(rows.at[xx, vv, k, :, wide], rows.at[xx, vv, k, :, wide], row_sem(), wide_recv.at[xx, vv, k], target)
            counts["kinds"].append(wide)

    def send_thin(xx, vv, k, *to):
        for target in to:
            send(rows.at[xx, vv, k, :, thin], rows.at[xx, vv, k, :, thin], row_sem(), thin_recv.at[xx, vv, k], target)
            counts["kinds"].append(thin)

    def wide_got(xx, vv, k):
        got(rows.at[xx, vv, k, :, wide], wide_recv.at[xx, vv, k])

    def thin_got(xx, vv, k):
        got(rows.at[xx, vv, k, :, thin], thin_recv.at[xx, vv, k])

    def send_wq(src, uu, k, target):
        send(src, wq.at[uu, k], wq_send.at[counts["wq"]], wq_recv.at[uu, k], target)
        counts["wq"] += 1

    def send_wkv(src, uu, k, target):
        send(src, wkv.at[uu, k], wkv_send.at[counts["wkv"]], wkv_recv.at[uu, k], target)
        counts["wkv"] += 1

    def wq_got(uu, k):
        got(wq.at[uu, k], wq_recv.at[uu, k])

    def wkv_got(uu, k):
        got(wkv.at[uu, k], wkv_recv.at[uu, k])

    x_next, x_last = chip(plus(x, 1), u, v) + c, chip(plus(x, 3), u, v) + c
    v_next, v_last = chip(x, u, plus(v, 1)) + c, chip(x, u, plus(v, 3)) + c
    u_next, u_last = chip(x, plus(u, 1), v) + c, chip(x, plus(u, 3), v) + c
    xp, xm, xo = plus(x, 1), plus(x, 3), plus(x, 2)
    vp, vm, vo = plus(v, 1), plus(v, 3), plus(v, 2)
    up, um, uo = plus(u, 1), plus(u, 3), plus(u, 2)

    near_x, near_v, near_u = (x_next, x_last), (v_next, v_last), (u_next, u_last)
    x_far, v_far, u_far = chip(xo, u, v) + c, chip(x, u, vo) + c, chip(x, uo, v) + c

    send(other, rows.at[x, u, c], row_sem(), wide_recv.at[x, u, c], mate)
    send_thin(x, v, c, *near_x, x_far)
    send_wide(x, v, c, *near_v, v_far)
    for target in (*near_u, u_far):
        send_wkv(wkv.at[u, c], u, c, target)
    for target in near_u:
        send_wq(wq_hbm.at[own_columns, :], u, c, target)
    send_wkv(wkv_other, v, c, mate)
    send_wq(wq_hbm.at[mate_columns, :], v, c, mate)
    got(rows.at[x, v, d], wide_recv.at[x, v, d])
    send_thin(x, v, d, *near_x, x_far)
    send_wide(x, v, c, *near_x)
    send_wide(x, v, d, *near_v, v_far)
    send_wide(x, v, d, *near_x)
    for k in (c, d):
        send_thin(x, v, k, *near_v, v_far)
    wkv_got(u, d)
    for target in (*near_u, u_far):
        send_wkv(wkv.at[u, d], u, d, target)
    wq_got(u, d)
    for target in near_u:
        send_wq(wq.at[u, d], u, d, target)
    send_wq(wq_hbm.at[own_columns, :], u, c, u_far)
    send_wq(wq.at[u, d], u, d, u_far)

    for xx in (xm, xp, xo):
        for k in (c, d):
            thin_got(xx, v, k)
            send_thin(xx, v, k, *near_v, v_far)
    for k in (c, d):
        for vv in (vm, vp):
            wide_got(x, vv, k)
            send_wide(x, vv, k, *near_x)
    for k in (c, d):
        wide_got(x, vo, k)
        send_wide(x, vo, k, *near_x)
    for vv in (v, vp, vm, vo):
        for k in (c, d):
            send_wide(x, vv, k, x_far)

    def q_block(xx, uu):
        right = jnp.concatenate([wq[uu, 0], wq[uu, 1]], axis=1)
        value = jnp.dot(rows[xx].reshape(256, half), right, preferred_element_type=jnp.float32)
        for k in (0, 1):
            q_part[xx, uu, k] = value[:, k * 128:(k + 1) * 128].reshape(4, 64, 128)

    def send_q(g, xx, du):
        uu = plus(u, du)
        for k in ((c, d) if du else (d,)):
            send(q_part.at[xx, uu, k], q_got.at[c, u, xx], q_send.at[g, du, k], q_recv.at[c, u, xx], chip(x, uu, v) + k)

    def kv_group(g, xx):
        value = lax.dot_general(
            wkv[...].reshape(128, half), rows[xx].reshape(256, half), (((1,), (1,)), ((), ())), preferred_element_type=jnp.float32
        )
        kv_part[xx] = value.reshape(4, 2, 16, 256)
        for du in (2, 1, 3, 0):
            uu = plus(u, du)
            for k in ((c, d) if du else (d,)):
                send(kv_part.at[xx, uu, k], kv_got.at[c, u, xx], kv_send.at[g, du, k], kv_recv.at[c, u, xx], chip(x, uu, v) + k)
        kv_got[c, u, xx] = kv_part[xx, u, c]

    def far_rows(t):
        vv = plus(v, t + t // 2 - 2 * (t // 3))
        wide_got(xo, vv, c)
        wide_got(xo, vv, d)

        @pl.when(t == 3)
        def _():
            kv_group(3, xo)

        @pl.loop(0, 4)
        def _(j):
            uu = plus(u, 2 + j)
            right = jnp.concatenate([wq[uu, 0], wq[uu, 1]], axis=1)
            value = jnp.dot(rows[xo, vv].reshape(64, half), right, preferred_element_type=jnp.float32)
            for k in (0, 1):
                q_part[xo, uu, k, vv] = value[:, k * 128:(k + 1) * 128]

            def send_far(k):
                send(
                    q_part.at[xo, uu, k, vv], q_got.at[c, u, xo, vv], q_send_far.at[t, uu, k], q_recv.at[c, u, xo],
                    chip(x, uu, v) + k,
                )

            send_far(d)

            @pl.when(j != 2)
            def _():
                send_far(c)

        q_got[c, u, xo, vv] = q_part[xo, u, c, vv]

    senders = [(c, plus(u, n)) for n in (1, 2, 3)] + [(d, n) for n in range(4)]
    place = rem(y, 2) * 4 + x

    def add_kv(g, xx):
        for role, n in senders:
            got(kv_got.at[role, n, xx], kv_recv.at[role, n, xx])
        for zz in range(4):
            second = jnp.concatenate([kv_got[1, yy, xx][:, zz * 64:(zz + 1) * 64] for yy in range(4)], axis=1)
            pieces[c, g, place, :, pl.ds(zz * 256, 256)] = (kv_got[0, zz, xx] + second).astype(jnp.bfloat16)
        for n in range(1, 8):
            there = rem(place + n, 8)
            target = ((z * 4 + (y // 2) * 2 + there // 4) * 4 + rem(there, 4)) * 2 + c
            send(pieces.at[c, g, place], pieces.at[c, g, place], piece_send.at[g, n], piece_recv.at[g, place], target)

    def add_q(xx):
        for role, n in senders:
            got(q_got.at[role, n, xx], q_recv.at[role, n, xx])

        @pl.loop(0, 4)
        def _(zz):
            for yy in range(4):
                q_out[zz, yy, xx] = (q_got[0, zz, xx, yy] + q_got[1, yy, xx, zz]).astype(jnp.bfloat16)

    def share_kv(g):
        for n in range(1, 8):
            there = rem(place + n, 8)
            got(pieces.at[c, g, there], piece_recv.at[g, there])
        send(pieces.at[c, g], pieces.at[c, g], pair_send.at[g], pair_recv.at[g], mate)

    def finish_kv():
        for g in range(4):
            got(pieces.at[d, g], pair_recv.at[g])

        @pl.loop(0, 4)
        def _(zz):
            columns = pl.ds(pl.multiple_of(zz * 256, 256), 256)
            for xx in range(4):
                places = [((xx - n + 1) % 4, n) for n in range(8)]
                wide_pieces = [pieces[k, g, n, :, columns].astype(jnp.float32) for g, n in places for k in (0, 1)]
                for out, first in ((k_out, 0), (v_out, 8)):
                    value = jnp.concatenate([w[first:first + 8] for w in wide_pieces], axis=0).T.astype(jnp.bfloat16)
                    out[zz, :, xx] = value.reshape(4, 64, 128)

    load_wq.wait()
    for vv in (vm, vp, vo):
        for k in (c, d):
            thin_got(x, vv, k)

    @pl.loop(0, 1)
    def _(i):
        q_block(x, plus(u, i))

    for uu in (um, up, uo):
        for k in (c, d):
            wkv_got(uu, k)
    for uu in (um, up):
        for k in (c, d):
            wq_got(uu, k)

    @pl.loop(0, 2)
    def _(i):
        q_block(x, plus(um, 2 * i))

    for xx in (xm, xp):
        for k in (c, d):
            wide_got(xx, v, k)
            for vv in (vm, vp, vo):
                wide_got(xx, vv, k)
                thin_got(xx, vv, k)

    @pl.loop(0, 3)
    def _(g):
        kv_group(g, plus(xm, g))

    @pl.loop(0, 2)
    def _(i):
        @pl.loop(0, 3)
        def _(j):
            q_block(plus(xm, 2 * i), plus(um, j))

    for k in (c, d):
        wq_got(uo, k)

    @pl.loop(0, 3)
    def _(g):
        for du in (1, 3, 0):
            send_q(g, plus(xm, g), du)

    @pl.loop(0, 3)
    def _(g):
        xx = plus(xm, g)
        q_block(xx, uo)
        send_q(g, xx, 2)
        q_got[c, u, xx] = q_part[xx, u, c]

    for vv in (vm, vp, vo):
        for k in (c, d):
            thin_got(xo, vv, k)

    @pl.loop(0, 3)
    def _(t):
        far_rows(t)

    for g in range(3):
        add_kv(g, plus(xm, g))

    @pl.loop(3, 4)
    def _(t):
        far_rows(t)

    add_kv(3, xo)
    for g in range(3):
        add_q(plus(xm, g))
    for g in range(3):
        share_kv(g)
    add_q(xo)
    share_kv(3)
    finish_kv()

    got(other, row_send.at[0])
    for n, kind in enumerate(counts["kinds"]):
        got(rows.at[0, 0, 0, :, kind], row_send.at[n + 1])
    for n in range(counts["wq"]):
        got(wq.at[0, 0], wq_send.at[n])
    for n in range(counts["wkv"]):
        got(wkv.at[0, 0], wkv_send.at[n])
    for du in range(4):
        for k in ((c, d) if du else (d,)):
            for g in range(3):
                got(q_part.at[0, 0, 0], q_send.at[g, du, k])
            for t in range(4):
                got(q_part.at[0, 0, 0, 0], q_send_far.at[t, plus(u, du), k])
                got(kv_part.at[0, 0, 0], kv_send.at[t, du, k])
    for g in range(4):
        for n in range(1, 8):
            got(pieces.at[0, 0, 0], piece_send.at[g, n])
        got(pieces.at[0, 0], pair_send.at[g])


def solution(mesh):
    def local_step(x_rows, norm_gain, w_q, w_k, w_v):
        depth = x_rows.shape[1]
        half = depth // 2
        any_space = pl.BlockSpec(memory_space=pl.ANY)
        vmem = pl.BlockSpec(memory_space=pltpu.VMEM)
        bf16, f32 = jnp.bfloat16, jnp.float32
        out = jax.ShapeDtypeStruct((4, 4, 4, 64, 128), bf16)
        outs = pl.pallas_call(
            functools.partial(kernel, depth, half - half // 8),
            out_shape=(out, out, out),
            in_specs=[any_space, vmem, any_space, any_space, any_space],
            out_specs=(vmem, vmem, vmem),
            scratch_shapes=[
                pltpu.VMEM((32, depth), bf16),
                pltpu.VMEM((32, half), bf16),
                pltpu.VMEM((16, half), bf16),
                pltpu.VMEM((4, 4, 2, 32, half), bf16),
                pltpu.VMEM((4, 2, half, 128), bf16),
                pltpu.VMEM((4, 2, 16, half), bf16),
                pltpu.VMEM((4, 4, 2, 4, 64, 128), f32),
                pltpu.VMEM((4, 4, 2, 16, 256), f32),
                pltpu.VMEM((2, 4, 4, 4, 64, 128), f32),
                pltpu.VMEM((2, 4, 4, 16, 256), f32),
                pltpu.VMEM((2, 4, 8, 16, 1024), bf16),
                DMA((6,)),
                DMA((4, 4, 2)),
                DMA((4, 4, 2)),
                DMA((61,)),
                DMA((4, 2)),
                DMA((4, 2)),
                DMA((7,)),
                DMA((7,)),
                DMA((3, 4, 2)),
                DMA((4, 4, 2)),
                DMA((4, 4, 2)),
                DMA((2, 4, 4)),
                DMA((2, 4, 4)),
                DMA((4, 8)),
                DMA((4, 8)),
                DMA((4,)),
                DMA((4,)),
            ],
            compiler_params=pltpu.CompilerParams(collective_id=0, has_side_effects=True, vmem_limit_bytes=67043328),
        )(x_rows, norm_gain.reshape(1, depth), w_q.reshape(depth, 128), w_k.T, w_v.T)
        return tuple(value.reshape(4096, 1, 128) for value in outs)

    return jax.shard_map(
        local_step,
        mesh=mesh,
        in_specs=(P(("dp", "tp"), None), P(None), P(None, "tp", None), P(None, "tp"), P(None, "tp")),
        out_specs=(P("dp", "tp", None), P("dp", "tp", None), P("dp", "tp", None)),
        check_vma=False,
    )
```

```python
import functools

import jax
import jax.numpy as jnp
from jax import lax
from jax.experimental import pallas as pl
from jax.experimental.pallas import tpu as pltpu
from jax.sharding import PartitionSpec as P

EPSILON = 1e-6
MESH = pl.DeviceIdType.MESH
DMA = pltpu.SemaphoreType.DMA


def rem(a, b):
    return lax.rem(a, b)


def kernel(
    depth, split, x_hbm, gain, wq_hbm, wk_hbm, wv_hbm, q_out, k_out, v_out,
    x_in, other, wkv_other, rows, wq, wkv, q_part, kv_part, q_got, kv_got, pieces,
    load_sem, wide_recv, thin_recv, row_send, wq_recv, wkv_recv, wq_send, wkv_send, q_send, q_send_far, kv_send, q_recv,
    kv_recv,
    piece_send, piece_recv, pair_send, pair_recv,
):
    half = depth // 2
    me = lax.axis_index("tp")
    c = rem(me, 2)
    x = rem(me // 2, 4)
    y = rem(me // 8, 4)
    z = me // 32
    u = z + c * (y - z)
    v = y + c * (z - y)
    mate = me + 1 - 2 * c
    d = 1 - c

    def chip(xx, uu, vv):
        zz = uu + c * (vv - uu)
        yy = vv + c * (uu - vv)
        return ((zz * 4 + yy) * 4 + xx) * 2

    def plus(a, n):
        return rem(a + n, 4)

    def send(src, dst, send_sem, recv_sem, target):
        copy = pltpu.make_async_remote_copy(
            src_ref=src, dst_ref=dst, send_sem=send_sem, recv_sem=recv_sem, device_id={"tp": target}, device_id_type=MESH
        )
        copy.start()

    def got(ref, sem):
        pltpu.make_async_copy(ref, ref, sem).wait()

    load_x = pltpu.make_async_copy(x_hbm, x_in, load_sem.at[0])
    load_x.start()
    own_columns = pl.ds(pl.multiple_of(c * half, half), half)
    mate_columns = pl.ds(pl.multiple_of(d * half, half), half)
    loads = [
        pltpu.make_async_copy(wk_hbm.at[:, mate_columns], wkv_other.at[0:8], load_sem.at[1]),
        pltpu.make_async_copy(wv_hbm.at[:, mate_columns], wkv_other.at[8:16], load_sem.at[2]),
        pltpu.make_async_copy(wk_hbm.at[:, own_columns], wkv.at[u, c, 0:8], load_sem.at[3]),
        pltpu.make_async_copy(wv_hbm.at[:, own_columns], wkv.at[u, c, 8:16], load_sem.at[4]),
    ]
    for load in loads:
        load.start()
    load_wq = pltpu.make_async_copy(wq_hbm.at[own_columns, :], wq.at[u, c], load_sem.at[5])
    load_wq.start()

    barrier = pltpu.get_barrier_semaphore()
    y_pair = y + 1 - 2 * rem(y, 2)
    peers = [mate]
    for n in (1, 2, 3):
        for k in (0, 1):
            peers.append(((z * 4 + plus(y, n)) * 4 + x) * 2 + k)
            peers.append(((plus(z, n) * 4 + y) * 4 + x) * 2 + k)
        peers.append(((z * 4 + y) * 4 + plus(x, n)) * 2 + c)
        peers.append(((z * 4 + y_pair) * 4 + plus(x, n)) * 2 + c)
    for peer in peers:
        pl.semaphore_signal(barrier, inc=1, device_id={"tp": peer}, device_id_type=MESH)

    load_x.wait()
    width = min(1024, half)

    def squares(j, total):
        part = x_in[:, pl.ds(pl.multiple_of(j * width, width), width)].astype(jnp.float32)
        return total + part * part

    total = lax.fori_loop(0, depth // width, squares, jnp.zeros((32, width), jnp.float32))
    scale = lax.rsqrt(jnp.sum(total, axis=1, keepdims=True) / depth + EPSILON)

    def normed(first):
        columns = pl.ds(pl.multiple_of(first, width), width)
        return (x_in[:, columns].astype(jnp.float32) * scale * gain[:, columns]).astype(jnp.bfloat16)

    @pl.loop(0, half // width)
    def _(j):
        columns = pl.ds(pl.multiple_of(j * width, width), width)
        other[:, columns] = normed(d * half + j * width)
        rows[x, v, c, :, columns] = normed(c * half + j * width)

    for load in loads:
        load.wait()
    pl.semaphore_wait(barrier, len(peers))

    counts = {"row": 0, "wq": 0, "wkv": 0, "kinds": []}
    wide, thin = slice(0, split), slice(split, half)

    def row_sem():
        counts["row"] += 1
        return row_send.at[counts["row"] - 1]

    def send_wide(xx, vv, k, *to):
        for target in to:
            send(rows.at[xx, vv, k, :, wide], rows.at[xx, vv, k, :, wide], row_sem(), wide_recv.at[xx, vv, k], target)
            counts["kinds"].append(wide)

    def send_thin(xx, vv, k, *to):
        for target in to:
            send(rows.at[xx, vv, k, :, thin], rows.at[xx, vv, k, :, thin], row_sem(), thin_recv.at[xx, vv, k], target)
            counts["kinds"].append(thin)

    def wide_got(xx, vv, k):
        got(rows.at[xx, vv, k, :, wide], wide_recv.at[xx, vv, k])

    def thin_got(xx, vv, k):
        got(rows.at[xx, vv, k, :, thin], thin_recv.at[xx, vv, k])

    def send_wq(src, uu, k, target):
        send(src, wq.at[uu, k], wq_send.at[counts["wq"]], wq_recv.at[uu, k], target)
        counts["wq"] += 1

    def send_wkv(src, uu, k, target):
        send(src, wkv.at[uu, k], wkv_send.at[counts["wkv"]], wkv_recv.at[uu, k], target)
        counts["wkv"] += 1

    def wq_got(uu, k):
        got(wq.at[uu, k], wq_recv.at[uu, k])

    def wkv_got(uu, k):
        got(wkv.at[uu, k], wkv_recv.at[uu, k])

    x_next, x_last = chip(plus(x, 1), u, v) + c, chip(plus(x, 3), u, v) + c
    v_next, v_last = chip(x, u, plus(v, 1)) + c, chip(x, u, plus(v, 3)) + c
    u_next, u_last = chip(x, plus(u, 1), v) + c, chip(x, plus(u, 3), v) + c
    xp, xm, xo = plus(x, 1), plus(x, 3), plus(x, 2)
    vp, vm, vo = plus(v, 1), plus(v, 3), plus(v, 2)
    up, um, uo = plus(u, 1), plus(u, 3), plus(u, 2)

    near_x, near_v, near_u = (x_next, x_last), (v_next, v_last), (u_next, u_last)

    send(other, rows.at[x, u, c], row_sem(), wide_recv.at[x, u, c], mate)
    send_thin(x, v, c, *near_x)
    send_wide(x, v, c, *near_v)
    for target in near_u:
        send_wkv(wkv.at[u, c], u, c, target)
    for target in near_u:
        send_wq(wq_hbm.at[own_columns, :], u, c, target)
    send_wkv(wkv_other, v, c, mate)
    send_wq(wq_hbm.at[mate_columns, :], v, c, mate)
    got(rows.at[x, v, d], wide_recv.at[x, v, d])
    send_thin(x, v, d, *near_x)
    send_wide(x, v, c, *near_x)
    send_wide(x, v, d, *near_v)
    send_wide(x, v, d, *near_x)
    for k in (c, d):
        send_thin(x, v, k, *near_v)
    wkv_got(u, d)
    for target in near_u:
        send_wkv(wkv.at[u, d], u, d, target)
    wq_got(u, d)
    for target in near_u:
        send_wq(wq.at[u, d], u, d, target)

    def pass_thin_x(vv):
        thin_got(xm, vv, c)
        send_thin(xm, vv, c, x_next)
        thin_got(xp, vv, d)
        send_thin(xp, vv, d, x_last)

    def pass_x(vv):
        wide_got(xm, vv, c)
        send_wide(xm, vv, c, x_next)
        wide_got(xp, vv, d)
        send_wide(xp, vv, d, x_last)

    pass_thin_x(v)
    thin_got(xm, v, d)
    thin_got(xp, v, c)
    for xx in (xm, xp):
        for k in (c, d):
            send_thin(xx, v, k, *near_v)

    wide_got(x, vm, c)
    send_wide(x, vm, c, v_next)
    wkv_got(um, c)
    send_wkv(wkv.at[um, c], um, c, u_next)
    wide_got(xm, v, c)
    send_wide(xm, v, c, x_next)
    wide_got(x, vp, c)
    for vv in (vm, vp):
        send_wide(x, vv, c, *near_x)
    wide_got(x, vp, d)
    send_wide(x, vp, d, v_last)
    wide_got(xp, v, d)
    send_wide(xp, v, d, x_last)
    wide_got(x, vm, d)
    for vv in (vm, vp):
        send_wide(x, vv, d, *near_x)
    for k in (c, d):
        thin_got(xo, v, k)
        send_thin(xo, v, k, *near_v)
    for k in (c, d):
        wide_got(x, vo, k)
        send_wide(x, vo, k, *near_x)
    for xx in (x, xm, xp, xo):
        thin_got(xx, vm, c)
        send_thin(xx, vm, c, v_next)
        thin_got(xx, vp, d)
        send_thin(xx, vp, d, v_last)

    def q_block(xx, uu):
        right = jnp.concatenate([wq[uu, 0], wq[uu, 1]], axis=1)
        value = jnp.dot(rows[xx].reshape(256, half), right, preferred_element_type=jnp.float32)
        for k in (0, 1):
            q_part[xx, uu, k] = value[:, k * 128:(k + 1) * 128].reshape(4, 64, 128)

    def send_q(g, xx, du):
        uu = plus(u, du)
        for k in ((c, d) if du else (d,)):
            send(q_part.at[xx, uu, k], q_got.at[c, u, xx], q_send.at[g, du, k], q_recv.at[c, u, xx], chip(x, uu, v) + k)

    def kv_group(g, xx):
        value = lax.dot_general(
            wkv[...].reshape(128, half), rows[xx].reshape(256, half), (((1,), (1,)), ((), ())), preferred_element_type=jnp.float32
        )
        kv_part[xx] = value.reshape(4, 2, 16, 256)
        for du in (2, 1, 3, 0):
            uu = plus(u, du)
            for k in ((c, d) if du else (d,)):
                send(kv_part.at[xx, uu, k], kv_got.at[c, u, xx], kv_send.at[g, du, k], kv_recv.at[c, u, xx], chip(x, uu, v) + k)
        kv_got[c, u, xx] = kv_part[xx, u, c]

    def far_rows(t):
        vv = plus(v, t + 3)
        wide_got(xo, vv, c)
        wide_got(xo, vv, d)

        @pl.when(t == 3)
        def _():
            kv_group(3, xo)

        @pl.loop(0, 4)
        def _(j):
            uu = plus(u, 2 + j)
            right = jnp.concatenate([wq[uu, 0], wq[uu, 1]], axis=1)
            value = jnp.dot(rows[xo, vv].reshape(64, half), right, preferred_element_type=jnp.float32)
            for k in (0, 1):
                q_part[xo, uu, k, vv] = value[:, k * 128:(k + 1) * 128]

            def send_far(k):
                send(
                    q_part.at[xo, uu, k, vv], q_got.at[c, u, xo, vv], q_send_far.at[t, uu, k], q_recv.at[c, u, xo],
                    chip(x, uu, v) + k,
                )

            send_far(d)

            @pl.when(j != 2)
            def _():
                send_far(c)

        q_got[c, u, xo, vv] = q_part[xo, u, c, vv]

    senders = [(c, plus(u, n)) for n in (1, 2, 3)] + [(d, n) for n in range(4)]
    place = rem(y, 2) * 4 + x

    def add_kv(g, xx):
        for role, n in senders:
            got(kv_got.at[role, n, xx], kv_recv.at[role, n, xx])
        for zz in range(4):
            second = jnp.concatenate([kv_got[1, yy, xx][:, zz * 64:(zz + 1) * 64] for yy in range(4)], axis=1)
            pieces[c, g, place, :, pl.ds(zz * 256, 256)] = (kv_got[0, zz, xx] + second).astype(jnp.bfloat16)
        for n in range(1, 8):
            there = rem(place + n, 8)
            target = ((z * 4 + (y // 2) * 2 + there // 4) * 4 + rem(there, 4)) * 2 + c
            send(pieces.at[c, g, place], pieces.at[c, g, place], piece_send.at[g, n], piece_recv.at[g, place], target)

    def add_q(xx):
        for role, n in senders:
            got(q_got.at[role, n, xx], q_recv.at[role, n, xx])

        @pl.loop(0, 4)
        def _(zz):
            for yy in range(4):
                q_out[zz, yy, xx] = (q_got[0, zz, xx, yy] + q_got[1, yy, xx, zz]).astype(jnp.bfloat16)

    def share_kv(g):
        for n in range(1, 8):
            there = rem(place + n, 8)
            got(pieces.at[c, g, there], piece_recv.at[g, there])
        send(pieces.at[c, g], pieces.at[c, g], pair_send.at[g], pair_recv.at[g], mate)

    def finish_kv():
        for g in range(4):
            got(pieces.at[d, g], pair_recv.at[g])

        @pl.loop(0, 4)
        def _(zz):
            columns = pl.ds(pl.multiple_of(zz * 256, 256), 256)
            for xx in range(4):
                places = [((xx - n + 1) % 4, n) for n in range(8)]
                wide_pieces = [pieces[k, g, n, :, columns].astype(jnp.float32) for g, n in places for k in (0, 1)]
                for out, first in ((k_out, 0), (v_out, 8)):
                    value = jnp.concatenate([w[first:first + 8] for w in wide_pieces], axis=0).T.astype(jnp.bfloat16)
                    out[zz, :, xx] = value.reshape(4, 64, 128)

    load_wq.wait()
    for vv, k in ((vm, d), (vp, c), (vo, c), (vo, d)):
        thin_got(x, vv, k)

    @pl.loop(0, 1)
    def _(i):
        q_block(x, plus(u, i))

    wq_got(um, c)
    send_wq(wq.at[um, c], um, c, u_next)
    wkv_got(up, d)
    send_wkv(wkv.at[up, d], up, d, u_last)
    pass_x(vm)
    wq_got(up, d)
    send_wq(wq.at[up, d], up, d, u_last)
    pass_x(vp)
    wq_got(um, d)
    wq_got(up, c)

    @pl.loop(0, 2)
    def _(i):
        q_block(x, plus(um, 2 * i))

    pass_x(vo)
    wkv_got(um, d)
    wkv_got(up, c)
    for k in (c, d):
        wkv_got(uo, k)
    for xx, k in ((xm, d), (xp, c)):
        for vv in (v, vm, vp, vo):
            wide_got(xx, vv, k)
        for vv, kk in ((vm, d), (vp, c), (vo, c), (vo, d)):
            thin_got(xx, vv, kk)

    @pl.loop(0, 3)
    def _(g):
        kv_group(g, plus(xm, g))

    @pl.loop(0, 2)
    def _(i):
        @pl.loop(0, 3)
        def _(j):
            q_block(plus(xm, 2 * i), plus(um, j))

    for k in (c, d):
        wq_got(uo, k)

    @pl.loop(0, 3)
    def _(g):
        for du in (1, 3, 0):
            send_q(g, plus(xm, g), du)

    @pl.loop(0, 3)
    def _(g):
        xx = plus(xm, g)
        q_block(xx, uo)
        send_q(g, xx, 2)
        q_got[c, u, xx] = q_part[xx, u, c]

    for vv, kk in ((vm, d), (vp, c), (vo, c), (vo, d)):
        thin_got(xo, vv, kk)

    @pl.loop(0, 3)
    def _(t):
        far_rows(t)

    for g in range(3):
        add_kv(g, plus(xm, g))

    @pl.loop(3, 4)
    def _(t):
        far_rows(t)

    add_kv(3, xo)
    for g in range(3):
        add_q(plus(xm, g))
    for g in range(3):
        share_kv(g)
    add_q(xo)
    share_kv(3)
    finish_kv()

    got(other, row_send.at[0])
    for n, kind in enumerate(counts["kinds"]):
        got(rows.at[0, 0, 0, :, kind], row_send.at[n + 1])
    for n in range(counts["wq"]):
        got(wq.at[0, 0], wq_send.at[n])
    for n in range(counts["wkv"]):
        got(wkv.at[0, 0], wkv_send.at[n])
    for du in range(4):
        for k in ((c, d) if du else (d,)):
            for g in range(3):
                got(q_part.at[0, 0, 0], q_send.at[g, du, k])
            for t in range(4):
                got(q_part.at[0, 0, 0, 0], q_send_far.at[t, plus(u, du), k])
                got(kv_part.at[0, 0, 0], kv_send.at[t, du, k])
    for g in range(4):
        for n in range(1, 8):
            got(pieces.at[0, 0, 0], piece_send.at[g, n])
        got(pieces.at[0, 0], pair_send.at[g])


def solution(mesh):
    def local_step(x_rows, norm_gain, w_q, w_k, w_v):
        depth = x_rows.shape[1]
        half = depth // 2
        any_space = pl.BlockSpec(memory_space=pl.ANY)
        vmem = pl.BlockSpec(memory_space=pltpu.VMEM)
        bf16, f32 = jnp.bfloat16, jnp.float32
        out = jax.ShapeDtypeStruct((4, 4, 4, 64, 128), bf16)
        outs = pl.pallas_call(
            functools.partial(kernel, depth, half - half // 8),
            out_shape=(out, out, out),
            in_specs=[any_space, vmem, any_space, any_space, any_space],
            out_specs=(vmem, vmem, vmem),
            scratch_shapes=[
                pltpu.VMEM((32, depth), bf16),
                pltpu.VMEM((32, half), bf16),
                pltpu.VMEM((16, half), bf16),
                pltpu.VMEM((4, 4, 2, 32, half), bf16),
                pltpu.VMEM((4, 2, half, 128), bf16),
                pltpu.VMEM((4, 2, 16, half), bf16),
                pltpu.VMEM((4, 4, 2, 4, 64, 128), f32),
                pltpu.VMEM((4, 4, 2, 16, 256), f32),
                pltpu.VMEM((2, 4, 4, 4, 64, 128), f32),
                pltpu.VMEM((2, 4, 4, 16, 256), f32),
                pltpu.VMEM((2, 4, 8, 16, 1024), bf16),
                DMA((6,)),
                DMA((4, 4, 2)),
                DMA((4, 4, 2)),
                DMA((61,)),
                DMA((4, 2)),
                DMA((4, 2)),
                DMA((7,)),
                DMA((7,)),
                DMA((3, 4, 2)),
                DMA((4, 4, 2)),
                DMA((4, 4, 2)),
                DMA((2, 4, 4)),
                DMA((2, 4, 4)),
                DMA((4, 8)),
                DMA((4, 8)),
                DMA((4,)),
                DMA((4,)),
            ],
            compiler_params=pltpu.CompilerParams(collective_id=0, has_side_effects=True, vmem_limit_bytes=67043328),
        )(x_rows, norm_gain.reshape(1, depth), w_q.reshape(depth, 128), w_k.T, w_v.T)
        return tuple(value.reshape(4096, 1, 128) for value in outs)

    return jax.shard_map(
        local_step,
        mesh=mesh,
        in_specs=(P(("dp", "tp"), None), P(None), P(None, "tp", None), P(None, "tp"), P(None, "tp")),
        out_specs=(P("dp", "tp", None), P("dp", "tp", None), P("dp", "tp", None)),
        check_vma=False,
    )
```

```python
import functools

import jax
import jax.numpy as jnp
from jax import lax
from jax.experimental import pallas as pl
from jax.experimental.pallas import tpu as pltpu
from jax.sharding import PartitionSpec as P

EPSILON = 1e-6
MESH = pl.DeviceIdType.MESH
DMA = pltpu.SemaphoreType.DMA


def rem(a, b):
    return lax.rem(a, b)


def kernel(
    depth, split, x_hbm, gain, wq_hbm, wk_hbm, wv_hbm, q_out, k_out, v_out,
    x_in, other, wkv_other, rows, wq, wkv, q_part, kv_part, q_got, kv_got, pieces,
    load_sem, wide_recv, thin_recv, row_send, wq_recv, wkv_recv, wq_send, wkv_send, q_send, q_send_far, kv_send, q_recv,
    kv_recv,
    piece_send, piece_recv, pair_send, pair_recv,
):
    half = depth // 2
    me = lax.axis_index("tp")
    c = rem(me, 2)
    x = rem(me // 2, 4)
    y = rem(me // 8, 4)
    z = me // 32
    u = z + c * (y - z)
    v = y + c * (z - y)
    mate = me + 1 - 2 * c
    d = 1 - c

    def chip(xx, uu, vv):
        zz = uu + c * (vv - uu)
        yy = vv + c * (uu - vv)
        return ((zz * 4 + yy) * 4 + xx) * 2

    def plus(a, n):
        return rem(a + n, 4)

    def send(src, dst, send_sem, recv_sem, target):
        copy = pltpu.make_async_remote_copy(
            src_ref=src, dst_ref=dst, send_sem=send_sem, recv_sem=recv_sem, device_id={"tp": target}, device_id_type=MESH
        )
        copy.start()

    def got(ref, sem):
        pltpu.make_async_copy(ref, ref, sem).wait()

    load_x = pltpu.make_async_copy(x_hbm, x_in, load_sem.at[0])
    load_x.start()
    own_columns = pl.ds(pl.multiple_of(c * half, half), half)
    mate_columns = pl.ds(pl.multiple_of(d * half, half), half)
    loads = [
        pltpu.make_async_copy(wk_hbm.at[:, mate_columns], wkv_other.at[0:8], load_sem.at[1]),
        pltpu.make_async_copy(wv_hbm.at[:, mate_columns], wkv_other.at[8:16], load_sem.at[2]),
        pltpu.make_async_copy(wk_hbm.at[:, own_columns], wkv.at[u, c, 0:8], load_sem.at[3]),
        pltpu.make_async_copy(wv_hbm.at[:, own_columns], wkv.at[u, c, 8:16], load_sem.at[4]),
    ]
    for load in loads:
        load.start()
    load_wq = pltpu.make_async_copy(wq_hbm.at[own_columns, :], wq.at[u, c], load_sem.at[5])
    load_wq.start()

    barrier = pltpu.get_barrier_semaphore()
    y_pair = y + 1 - 2 * rem(y, 2)
    peers = [mate]
    for n in (1, 2, 3):
        for k in (0, 1):
            peers.append(((z * 4 + plus(y, n)) * 4 + x) * 2 + k)
            peers.append(((plus(z, n) * 4 + y) * 4 + x) * 2 + k)
        peers.append(((z * 4 + y) * 4 + plus(x, n)) * 2 + c)
        peers.append(((z * 4 + y_pair) * 4 + plus(x, n)) * 2 + c)
    for peer in peers:
        pl.semaphore_signal(barrier, inc=1, device_id={"tp": peer}, device_id_type=MESH)

    load_x.wait()
    width = min(1024, half)

    def squares(j, total):
        part = x_in[:, pl.ds(pl.multiple_of(j * width, width), width)].astype(jnp.float32)
        return total + part * part

    total = lax.fori_loop(0, depth // width, squares, jnp.zeros((32, width), jnp.float32))
    scale = lax.rsqrt(jnp.sum(total, axis=1, keepdims=True) / depth + EPSILON)

    def normed(first):
        columns = pl.ds(pl.multiple_of(first, width), width)
        return (x_in[:, columns].astype(jnp.float32) * scale * gain[:, columns]).astype(jnp.bfloat16)

    @pl.loop(0, half // width)
    def _(j):
        columns = pl.ds(pl.multiple_of(j * width, width), width)
        other[:, columns] = normed(d * half + j * width)
        rows[x, v, c, :, columns] = normed(c * half + j * width)

    for load in loads:
        load.wait()
    pl.semaphore_wait(barrier, len(peers))

    counts = {"row": 0, "wq": 0, "wkv": 0, "kinds": []}
    wide, thin = slice(0, split), slice(split, half)

    def row_sem():
        counts["row"] += 1
        return row_send.at[counts["row"] - 1]

    def send_wide(xx, vv, k, *to):
        for target in to:
            send(rows.at[xx, vv, k, :, wide], rows.at[xx, vv, k, :, wide], row_sem(), wide_recv.at[xx, vv, k], target)
            counts["kinds"].append(wide)

    def send_thin(xx, vv, k, *to):
        for target in to:
            send(rows.at[xx, vv, k, :, thin], rows.at[xx, vv, k, :, thin], row_sem(), thin_recv.at[xx, vv, k], target)
            counts["kinds"].append(thin)

    def wide_got(xx, vv, k):
        got(rows.at[xx, vv, k, :, wide], wide_recv.at[xx, vv, k])

    def thin_got(xx, vv, k):
        got(rows.at[xx, vv, k, :, thin], thin_recv.at[xx, vv, k])

    def send_wq(src, uu, k, target):
        send(src, wq.at[uu, k], wq_send.at[counts["wq"]], wq_recv.at[uu, k], target)
        counts["wq"] += 1

    def send_wkv(src, uu, k, target):
        send(src, wkv.at[uu, k], wkv_send.at[counts["wkv"]], wkv_recv.at[uu, k], target)
        counts["wkv"] += 1

    def wq_got(uu, k):
        got(wq.at[uu, k], wq_recv.at[uu, k])

    def wkv_got(uu, k):
        got(wkv.at[uu, k], wkv_recv.at[uu, k])

    x_next, x_last = chip(plus(x, 1), u, v) + c, chip(plus(x, 3), u, v) + c
    v_next, v_last = chip(x, u, plus(v, 1)) + c, chip(x, u, plus(v, 3)) + c
    u_next, u_last = chip(x, plus(u, 1), v) + c, chip(x, plus(u, 3), v) + c
    xp, xm, xo = plus(x, 1), plus(x, 3), plus(x, 2)
    vp, vm, vo = plus(v, 1), plus(v, 3), plus(v, 2)
    up, um, uo = plus(u, 1), plus(u, 3), plus(u, 2)

    near_x, near_v, near_u = (x_next, x_last), (v_next, v_last), (u_next, u_last)

    send(other, rows.at[x, u, c], row_sem(), wide_recv.at[x, u, c], mate)
    send_thin(x, v, c, *near_x)
    send_wide(x, v, c, *near_v)
    for target in near_u:
        send_wkv(wkv.at[u, c], u, c, target)
    for target in near_u:
        send_wq(wq_hbm.at[own_columns, :], u, c, target)
    send_wkv(wkv_other, v, c, mate)
    send_wq(wq_hbm.at[mate_columns, :], v, c, mate)
    got(rows.at[x, v, d], wide_recv.at[x, v, d])
    send_thin(x, v, d, *near_x)
    send_wide(x, v, c, *near_x)
    send_wide(x, v, d, *near_v)
    send_wide(x, v, d, *near_x)
    for k in (c, d):
        send_thin(x, v, k, *near_v)
    wkv_got(u, d)
    for target in near_u:
        send_wkv(wkv.at[u, d], u, d, target)
    wq_got(u, d)
    for target in near_u:
        send_wq(wq.at[u, d], u, d, target)

    def pass_thin_x(vv):
        thin_got(xm, vv, c)
        send_thin(xm, vv, c, x_next)
        thin_got(xp, vv, d)
        send_thin(xp, vv, d, x_last)

    def pass_x(vv):
        wide_got(xm, vv, c)
        send_wide(xm, vv, c, x_next)
        wide_got(xp, vv, d)
        send_wide(xp, vv, d, x_last)

    pass_thin_x(v)
    thin_got(xm, v, d)
    thin_got(xp, v, c)
    for xx in (xm, xp):
        for k in (c, d):
            send_thin(xx, v, k, *near_v)

    wide_got(x, vm, c)
    send_wide(x, vm, c, v_next)
    wkv_got(um, c)
    send_wkv(wkv.at[um, c], um, c, u_next)
    wide_got(xm, v, c)
    send_wide(xm, v, c, x_next)
    wide_got(x, vp, c)
    for vv in (vm, vp):
        send_wide(x, vv, c, *near_x)
    wide_got(x, vp, d)
    send_wide(x, vp, d, v_last)
    wide_got(xp, v, d)
    send_wide(xp, v, d, x_last)
    wide_got(x, vm, d)
    for vv in (vm, vp):
        send_wide(x, vv, d, *near_x)
    for k in (c, d):
        thin_got(xo, v, k)
        send_thin(xo, v, k, *near_v)
    for k in (c, d):
        wide_got(x, vo, k)
        send_wide(x, vo, k, *near_x)
    for xx in (x, xm, xp, xo):
        thin_got(xx, vm, c)
        send_thin(xx, vm, c, v_next)
        thin_got(xx, vp, d)
        send_thin(xx, vp, d, v_last)

    def q_block(xx, uu):
        right = jnp.concatenate([wq[uu, 0], wq[uu, 1]], axis=1)
        value = jnp.dot(rows[xx].reshape(256, half), right, preferred_element_type=jnp.float32)
        for k in (0, 1):
            q_part[xx, uu, k] = value[:, k * 128:(k + 1) * 128].reshape(4, 64, 128)

    def send_q(g, xx, du, whole=True):
        uu = plus(u, du)

        def to(k):
            send(q_part.at[xx, uu, k], q_got.at[c, u, xx], q_send.at[g, du, k], q_recv.at[c, u, xx], chip(x, uu, v) + k)

        to(d)

        @pl.when(whole)
        def _():
            to(c)

    def kv_group(g, xx):
        value = lax.dot_general(
            wkv[...].reshape(128, half), rows[xx].reshape(256, half), (((1,), (1,)), ((), ())), preferred_element_type=jnp.float32
        )
        kv_part[xx] = value.reshape(4, 2, 16, 256)
        for du in (2, 1, 3, 0):
            uu = plus(u, du)
            for k in ((c, d) if du else (d,)):
                send(kv_part.at[xx, uu, k], kv_got.at[c, u, xx], kv_send.at[g, du, k], kv_recv.at[c, u, xx], chip(x, uu, v) + k)
        kv_got[c, u, xx] = kv_part[xx, u, c]

    def far_rows(t):
        vv = plus(v, t + 3)
        wide_got(xo, vv, c)
        wide_got(xo, vv, d)

        @pl.when(t == 3)
        def _():
            kv_group(3, xo)

        @pl.loop(0, 4)
        def _(j):
            uu = plus(u, 2 + j)
            right = jnp.concatenate([wq[uu, 0], wq[uu, 1]], axis=1)
            value = jnp.dot(rows[xo, vv].reshape(64, half), right, preferred_element_type=jnp.float32)
            for k in (0, 1):
                q_part[xo, uu, k, vv] = value[:, k * 128:(k + 1) * 128]

            def send_far(k):
                send(
                    q_part.at[xo, uu, k, vv], q_got.at[c, u, xo, vv], q_send_far.at[t, uu, k], q_recv.at[c, u, xo],
                    chip(x, uu, v) + k,
                )

            send_far(d)

            @pl.when(j != 2)
            def _():
                send_far(c)

        q_got[c, u, xo, vv] = q_part[xo, u, c, vv]

    senders = [(c, plus(u, n)) for n in (1, 2, 3)] + [(d, n) for n in range(4)]
    place = rem(y, 2) * 4 + x

    def add_kv(g, xx, direct=False):
        for role, n in senders:
            got(kv_got.at[role, n, xx], kv_recv.at[role, n, xx])
        for zz in range(4):
            second = jnp.concatenate([kv_got[1, yy, xx][:, zz * 64:(zz + 1) * 64] for yy in range(4)], axis=1)
            pieces[c, g, place, :, pl.ds(zz * 256, 256)] = (kv_got[0, zz, xx] + second).astype(jnp.bfloat16)
        own = pieces.at[c, g, place]
        for n in range(1, 4):
            send(own, own, piece_send.at[g, n], piece_recv.at[g, place], row_chip(n, y) + c)
            if direct:
                send(own, own, piece_send.at[g, n + 4], piece_recv.at[g, place], row_chip(n, y_pair) + c)
        send(own, own, piece_send.at[g, 0], piece_recv.at[g, place], row_chip(0, y_pair) + c)

    def row_chip(n, yy):
        return ((z * 4 + yy) * 4 + plus(x, n)) * 2

    pair_place = 4 - place + 2 * x

    def pass_kv(g):
        got(pieces.at[c, g, pair_place], piece_recv.at[g, pair_place])
        theirs = pieces.at[c, g, pair_place]
        for n in range(1, 4):
            send(theirs, theirs, piece_send.at[g, n + 4], piece_recv.at[g, pair_place], row_chip(n, y) + c)

    def add_q(xx):
        for role, n in senders:
            got(q_got.at[role, n, xx], q_recv.at[role, n, xx])

        @pl.loop(0, 4)
        def _(zz):
            for yy in range(4):
                q_out[zz, yy, xx] = (q_got[0, zz, xx, yy] + q_got[1, yy, xx, zz]).astype(jnp.bfloat16)

    def share_kv(g, passed=True):
        for n in (1, 2, 3, 5, 6, 7) if passed else range(1, 8):
            there = (pair_place if n >= 4 else place) - x + plus(x, n)
            got(pieces.at[c, g, there], piece_recv.at[g, there])
        send(pieces.at[c, g], pieces.at[c, g], pair_send.at[g], pair_recv.at[g], mate)

    def finish_kv():
        for g in range(4):
            got(pieces.at[d, g], pair_recv.at[g])

        @pl.loop(0, 4)
        def _(zz):
            columns = pl.ds(pl.multiple_of(zz * 256, 256), 256)
            for xx in range(4):
                places = [((xx - n + 1) % 4, n) for n in range(8)]
                wide_pieces = [pieces[k, g, n, :, columns].astype(jnp.float32) for g, n in places for k in (0, 1)]
                for out, first in ((k_out, 0), (v_out, 8)):
                    value = jnp.concatenate([w[first:first + 8] for w in wide_pieces], axis=0).T.astype(jnp.bfloat16)
                    out[zz, :, xx] = value.reshape(4, 64, 128)

    load_wq.wait()
    for vv, k in ((vm, d), (vp, c), (vo, c), (vo, d)):
        thin_got(x, vv, k)

    @pl.loop(0, 1)
    def _(i):
        q_block(x, plus(u, i))
        send_q(1, x, 0, False)

    wq_got(um, c)
    send_wq(wq.at[um, c], um, c, u_next)
    wkv_got(up, d)
    send_wkv(wkv.at[up, d], up, d, u_last)
    pass_x(vm)
    wq_got(up, d)
    send_wq(wq.at[up, d], up, d, u_last)
    pass_x(vp)
    wq_got(um, d)
    wq_got(up, c)

    @pl.loop(0, 2)
    def _(i):
        q_block(x, plus(um, 2 * i))
        send_q(1, x, plus(2 * i, 3))

    pass_x(vo)
    wkv_got(um, d)
    wkv_got(up, c)
    for k in (c, d):
        wkv_got(uo, k)
    for xx, k in ((xm, d), (xp, c)):
        for vv in (v, vm, vp, vo):
            wide_got(xx, vv, k)
        for vv, kk in ((vm, d), (vp, c), (vo, c), (vo, d)):
            thin_got(xx, vv, kk)

    @pl.loop(0, 3)
    def _(g):
        kv_group(g, plus(xm, g))

    @pl.loop(0, 2)
    def _(i):
        @pl.loop(0, 3)
        def _(j):
            q_block(plus(xm, 2 * i), plus(um, j))
            send_q(2 * i, plus(xm, 2 * i), plus(j, 3), j != 1)

    for k in (c, d):
        wq_got(uo, k)

    @pl.loop(0, 3)
    def _(g):
        xx = plus(xm, g)
        q_block(xx, uo)
        send_q(g, xx, 2)
        q_got[c, u, xx] = q_part[xx, u, c]

    for vv, kk in ((vm, d), (vp, c), (vo, c), (vo, d)):
        thin_got(xo, vv, kk)

    @pl.loop(0, 3)
    def _(t):
        far_rows(t)

    for g in range(3):
        add_kv(g, plus(xm, g))

    @pl.loop(3, 4)
    def _(t):
        far_rows(t)

    for g in range(3):
        pass_kv(g)
    for g in range(3):
        add_q(plus(xm, g))

    got(other, row_send.at[0])
    for n, kind in enumerate(counts["kinds"]):
        got(rows.at[0, 0, 0, :, kind], row_send.at[n + 1])
    for n in range(counts["wq"]):
        got(wq.at[0, 0], wq_send.at[n])
    for n in range(counts["wkv"]):
        got(wkv.at[0, 0], wkv_send.at[n])

    @pl.loop(0, 4)
    def _(du):
        def drained(k):
            for g in range(3):
                got(q_part.at[0, 0, 0], q_send.at[g, du, k])
            for t in range(4):
                got(q_part.at[0, 0, 0, 0], q_send_far.at[t, plus(u, du), k])
                got(kv_part.at[0, 0, 0], kv_send.at[t, du, k])

        drained(d)

        @pl.when(du > 0)
        def _():
            drained(c)

    add_kv(3, xo, direct=True)
    for g in range(3):
        share_kv(g)
    add_q(xo)
    share_kv(3, passed=False)
    finish_kv()
    for g in range(4):
        for n in (0, 1, 2, 3, 5, 6, 7):
            got(pieces.at[0, 0, 0], piece_send.at[g, n])
        got(pieces.at[0, 0], pair_send.at[g])


def solution(mesh):
    def local_step(x_rows, norm_gain, w_q, w_k, w_v):
        depth = x_rows.shape[1]
        half = depth // 2
        any_space = pl.BlockSpec(memory_space=pl.ANY)
        vmem = pl.BlockSpec(memory_space=pltpu.VMEM)
        bf16, f32 = jnp.bfloat16, jnp.float32
        out = jax.ShapeDtypeStruct((4, 4, 4, 64, 128), bf16)
        outs = pl.pallas_call(
            functools.partial(kernel, depth, half - half // 8),
            out_shape=(out, out, out),
            in_specs=[any_space, vmem, any_space, any_space, any_space],
            out_specs=(vmem, vmem, vmem),
            scratch_shapes=[
                pltpu.VMEM((32, depth), bf16),
                pltpu.VMEM((32, half), bf16),
                pltpu.VMEM((16, half), bf16),
                pltpu.VMEM((4, 4, 2, 32, half), bf16),
                pltpu.VMEM((4, 2, half, 128), bf16),
                pltpu.VMEM((4, 2, 16, half), bf16),
                pltpu.VMEM((4, 4, 2, 4, 64, 128), f32),
                pltpu.VMEM((4, 4, 2, 16, 256), f32),
                pltpu.VMEM((2, 4, 4, 4, 64, 128), f32),
                pltpu.VMEM((2, 4, 4, 16, 256), f32),
                pltpu.VMEM((2, 4, 8, 16, 1024), bf16),
                DMA((6,)),
                DMA((4, 4, 2)),
                DMA((4, 4, 2)),
                DMA((61,)),
                DMA((4, 2)),
                DMA((4, 2)),
                DMA((7,)),
                DMA((7,)),
                DMA((3, 4, 2)),
                DMA((4, 4, 2)),
                DMA((4, 4, 2)),
                DMA((2, 4, 4)),
                DMA((2, 4, 4)),
                DMA((4, 8)),
                DMA((4, 8)),
                DMA((4,)),
                DMA((4,)),
            ],
            compiler_params=pltpu.CompilerParams(collective_id=0, has_side_effects=True, vmem_limit_bytes=67043328),
        )(x_rows, norm_gain.reshape(1, depth), w_q.reshape(depth, 128), w_k.T, w_v.T)
        return tuple(value.reshape(4096, 1, 128) for value in outs)

    return jax.shard_map(
        local_step,
        mesh=mesh,
        in_specs=(P(("dp", "tp"), None), P(None), P(None, "tp", None), P(None, "tp"), P(None, "tp")),
        out_specs=(P("dp", "tp", None), P("dp", "tp", None), P("dp", "tp", None)),
        check_vma=False,
    )
```

```python
import functools

import jax
import jax.numpy as jnp
from jax import lax
from jax.experimental import pallas as pl
from jax.experimental.pallas import tpu as pltpu
from jax.sharding import PartitionSpec as P

EPSILON = 1e-6
MESH = pl.DeviceIdType.MESH
DMA = pltpu.SemaphoreType.DMA


def rem(a, b):
    return lax.rem(a, b)


def kernel(
    depth, split, x_hbm, gain, wq_hbm, wk_hbm, wv_hbm, q_hbm, pieces_hbm,
    x_in, other, wkv_other, rows, wq, wkv, q_part, kv_part, q_got, kv_got, q_sum, pieces,
    load_sem, wide_recv, thin_recv, row_send, wq_recv, wkv_recv, wq_send, wkv_send, q_send, q_send_far, kv_send, q_recv,
    kv_recv,
    piece_send, piece_recv, pair_send, pair_recv, q_left, pieces_left,
):
    half = depth // 2
    me = lax.axis_index("tp")
    c = rem(me, 2)
    x = rem(me // 2, 4)
    y = rem(me // 8, 4)
    z = me // 32
    u = z + c * (y - z)
    v = y + c * (z - y)
    mate = me + 1 - 2 * c
    d = 1 - c

    def chip(xx, uu, vv):
        zz = uu + c * (vv - uu)
        yy = vv + c * (uu - vv)
        return ((zz * 4 + yy) * 4 + xx) * 2

    def plus(a, n):
        return rem(a + n, 4)

    def send(src, dst, send_sem, recv_sem, target):
        copy = pltpu.make_async_remote_copy(
            src_ref=src, dst_ref=dst, send_sem=send_sem, recv_sem=recv_sem, device_id={"tp": target}, device_id_type=MESH
        )
        copy.start()

    def got(ref, sem):
        pltpu.make_async_copy(ref, ref, sem).wait()

    load_x = pltpu.make_async_copy(x_hbm, x_in, load_sem.at[0])
    load_x.start()
    own_columns = pl.ds(pl.multiple_of(c * half, half), half)
    mate_columns = pl.ds(pl.multiple_of(d * half, half), half)
    loads = [
        pltpu.make_async_copy(wk_hbm.at[:, mate_columns], wkv_other.at[0:8], load_sem.at[1]),
        pltpu.make_async_copy(wv_hbm.at[:, mate_columns], wkv_other.at[8:16], load_sem.at[2]),
        pltpu.make_async_copy(wk_hbm.at[:, own_columns], wkv.at[u, c, 0:8], load_sem.at[3]),
        pltpu.make_async_copy(wv_hbm.at[:, own_columns], wkv.at[u, c, 8:16], load_sem.at[4]),
    ]
    for load in loads:
        load.start()
    load_wq = pltpu.make_async_copy(wq_hbm.at[own_columns, :], wq.at[u, c], load_sem.at[5])
    load_wq.start()

    barrier = pltpu.get_barrier_semaphore()
    y_pair = y + 1 - 2 * rem(y, 2)
    peers = [mate]
    for n in (1, 2, 3):
        for k in (0, 1):
            peers.append(((z * 4 + plus(y, n)) * 4 + x) * 2 + k)
            peers.append(((plus(z, n) * 4 + y) * 4 + x) * 2 + k)
        peers.append(((z * 4 + y) * 4 + plus(x, n)) * 2 + c)
        peers.append(((z * 4 + y_pair) * 4 + plus(x, n)) * 2 + c)
    for peer in peers:
        pl.semaphore_signal(barrier, inc=1, device_id={"tp": peer}, device_id_type=MESH)

    load_x.wait()
    width = min(1024, half)

    def squares(j, total):
        part = x_in[:, pl.ds(pl.multiple_of(j * width, width), width)].astype(jnp.float32)
        return total + part * part

    total = lax.fori_loop(0, depth // width, squares, jnp.zeros((32, width), jnp.float32))
    scale = lax.rsqrt(jnp.sum(total, axis=1, keepdims=True) / depth + EPSILON)

    def normed(first):
        columns = pl.ds(pl.multiple_of(first, width), width)
        return (x_in[:, columns].astype(jnp.float32) * scale * gain[:, columns]).astype(jnp.bfloat16)

    @pl.loop(0, half // width)
    def _(j):
        columns = pl.ds(pl.multiple_of(j * width, width), width)
        other[:, columns] = normed(d * half + j * width)
        rows[x, v, c, :, columns] = normed(c * half + j * width)

    for load in loads:
        load.wait()
    pl.semaphore_wait(barrier, len(peers))

    counts = {"row": 0, "wq": 0, "wkv": 0, "kinds": []}
    wide, thin = slice(0, split), slice(split, half)

    def row_sem():
        counts["row"] += 1
        return row_send.at[counts["row"] - 1]

    def send_wide(xx, vv, k, *to):
        for target in to:
            send(rows.at[xx, vv, k, :, wide], rows.at[xx, vv, k, :, wide], row_sem(), wide_recv.at[xx, vv, k], target)
            counts["kinds"].append(wide)

    def send_thin(xx, vv, k, *to):
        for target in to:
            send(rows.at[xx, vv, k, :, thin], rows.at[xx, vv, k, :, thin], row_sem(), thin_recv.at[xx, vv, k], target)
            counts["kinds"].append(thin)

    def wide_got(xx, vv, k):
        got(rows.at[xx, vv, k, :, wide], wide_recv.at[xx, vv, k])

    def thin_got(xx, vv, k):
        got(rows.at[xx, vv, k, :, thin], thin_recv.at[xx, vv, k])

    def send_wq(src, uu, k, target):
        send(src, wq.at[uu, k], wq_send.at[counts["wq"]], wq_recv.at[uu, k], target)
        counts["wq"] += 1

    def send_wkv(src, uu, k, target):
        send(src, wkv.at[uu, k], wkv_send.at[counts["wkv"]], wkv_recv.at[uu, k], target)
        counts["wkv"] += 1

    def wq_got(uu, k):
        got(wq.at[uu, k], wq_recv.at[uu, k])

    def wkv_got(uu, k):
        got(wkv.at[uu, k], wkv_recv.at[uu, k])

    x_next, x_last = chip(plus(x, 1), u, v) + c, chip(plus(x, 3), u, v) + c
    v_next, v_last = chip(x, u, plus(v, 1)) + c, chip(x, u, plus(v, 3)) + c
    u_next, u_last = chip(x, plus(u, 1), v) + c, chip(x, plus(u, 3), v) + c
    xp, xm, xo = plus(x, 1), plus(x, 3), plus(x, 2)
    vp, vm, vo = plus(v, 1), plus(v, 3), plus(v, 2)
    up, um, uo = plus(u, 1), plus(u, 3), plus(u, 2)

    near_x, near_v, near_u = (x_next, x_last), (v_next, v_last), (u_next, u_last)

    send(other, rows.at[x, u, c], row_sem(), wide_recv.at[x, u, c], mate)
    send_thin(x, v, c, *near_x)
    send_wide(x, v, c, *near_v)
    for target in near_u:
        send_wkv(wkv.at[u, c], u, c, target)
    for target in near_u:
        send_wq(wq_hbm.at[own_columns, :], u, c, target)
    send_wkv(wkv_other, v, c, mate)
    send_wq(wq_hbm.at[mate_columns, :], v, c, mate)
    got(rows.at[x, v, d], wide_recv.at[x, v, d])
    send_thin(x, v, d, *near_x)
    send_wide(x, v, c, *near_x)
    send_wide(x, v, d, *near_v)
    send_wide(x, v, d, *near_x)
    for k in (c, d):
        send_thin(x, v, k, *near_v)
    wkv_got(u, d)
    for target in near_u:
        send_wkv(wkv.at[u, d], u, d, target)
    wq_got(u, d)
    for target in near_u:
        send_wq(wq.at[u, d], u, d, target)

    def pass_thin_x(vv):
        thin_got(xm, vv, c)
        send_thin(xm, vv, c, x_next)
        thin_got(xp, vv, d)
        send_thin(xp, vv, d, x_last)

    def pass_x(vv):
        wide_got(xm, vv, c)
        send_wide(xm, vv, c, x_next)
        wide_got(xp, vv, d)
        send_wide(xp, vv, d, x_last)

    pass_thin_x(v)
    thin_got(xm, v, d)
    thin_got(xp, v, c)
    for xx in (xm, xp):
        for k in (c, d):
            send_thin(xx, v, k, *near_v)

    wide_got(x, vm, c)
    send_wide(x, vm, c, v_next)
    wkv_got(um, c)
    send_wkv(wkv.at[um, c], um, c, u_next)
    wide_got(xm, v, c)
    send_wide(xm, v, c, x_next)
    wide_got(x, vp, c)
    for vv in (vm, vp):
        send_wide(x, vv, c, *near_x)
    wide_got(x, vp, d)
    send_wide(x, vp, d, v_last)
    wide_got(xp, v, d)
    send_wide(xp, v, d, x_last)
    wide_got(x, vm, d)
    for vv in (vm, vp):
        send_wide(x, vv, d, *near_x)
    for k in (c, d):
        thin_got(xo, v, k)
        send_thin(xo, v, k, *near_v)
    for k in (c, d):
        wide_got(x, vo, k)
        send_wide(x, vo, k, *near_x)
    for xx in (x, xm, xp, xo):
        thin_got(xx, vm, c)
        send_thin(xx, vm, c, v_next)
        thin_got(xx, vp, d)
        send_thin(xx, vp, d, v_last)

    def q_block(xx, uu):
        right = jnp.concatenate([wq[uu, 0], wq[uu, 1]], axis=1)
        value = jnp.dot(rows[xx].reshape(256, half), right, preferred_element_type=jnp.float32)
        for k in (0, 1):
            q_part[xx, uu, k] = value[:, k * 128:(k + 1) * 128].reshape(4, 64, 128)

    def send_q(g, xx, du, whole=True):
        uu = plus(u, du)

        def to(k):
            send(q_part.at[xx, uu, k], q_got.at[c, u, xx], q_send.at[g, du, k], q_recv.at[c, u, xx], chip(x, uu, v) + k)

        to(d)

        @pl.when(whole)
        def _():
            to(c)

    def kv_group(g, xx):
        value = lax.dot_general(
            wkv[...].reshape(128, half), rows[xx].reshape(256, half), (((1,), (1,)), ((), ())), preferred_element_type=jnp.float32
        )
        kv_part[xx] = value.reshape(4, 2, 16, 256)
        for du in (2, 1, 3, 0):
            uu = plus(u, du)
            for k in ((c, d) if du else (d,)):
                send(kv_part.at[xx, uu, k], kv_got.at[c, u, xx], kv_send.at[g, du, k], kv_recv.at[c, u, xx], chip(x, uu, v) + k)
        kv_got[c, u, xx] = kv_part[xx, u, c]

    def far_rows(t, vv, first, last):
        @pl.loop(first, last)
        def _(j):
            uu = plus(u, 2 + j)
            right = jnp.concatenate([wq[uu, 0], wq[uu, 1]], axis=1)
            value = jnp.dot(rows[xo, vv].reshape(64, half), right, preferred_element_type=jnp.float32)
            for k in (0, 1):
                q_part[xo, uu, k, vv] = value[:, k * 128:(k + 1) * 128]

            def to(k):
                send(
                    q_part.at[xo, uu, k, vv], q_got.at[c, u, xo, vv], q_send_far.at[t, uu, k], q_recv.at[c, u, xo],
                    chip(x, uu, v) + k,
                )

            to(d)

            @pl.when(j != 2)
            def _():
                to(c)

    def far_got(vv):
        wide_got(xo, vv, c)
        wide_got(xo, vv, d)

    senders = [(c, plus(u, n)) for n in (1, 2, 3)] + [(d, n) for n in range(4)]
    place = rem(y, 2) * 4 + x

    def add_kv(g, xx, direct=False):
        for role, n in senders:
            got(kv_got.at[role, n, xx], kv_recv.at[role, n, xx])
        for zz in range(4):
            second = jnp.concatenate([kv_got[1, yy, xx][:, zz * 64:(zz + 1) * 64] for yy in range(4)], axis=1)
            pieces[c, g, place, :, pl.ds(zz * 256, 256)] = (kv_got[0, zz, xx] + second).astype(jnp.bfloat16)
        own = pieces.at[c, g, place]
        for n in range(1, 4):
            send(own, own, piece_send.at[g, n], piece_recv.at[g, place], row_chip(n, y) + c)
            if direct:
                send(own, own, piece_send.at[g, n + 4], piece_recv.at[g, place], row_chip(n, y_pair) + c)
        send(own, own, piece_send.at[g, 0], piece_recv.at[g, place], row_chip(0, y_pair) + c)

    def row_chip(n, yy):
        return ((z * 4 + yy) * 4 + plus(x, n)) * 2

    pair_place = 4 - place + 2 * x

    def pass_kv(g):
        got(pieces.at[c, g, pair_place], piece_recv.at[g, pair_place])
        theirs = pieces.at[c, g, pair_place]
        for n in range(1, 4):
            send(theirs, theirs, piece_send.at[g, n + 4], piece_recv.at[g, pair_place], row_chip(n, y) + c)

    def add_q(g, xx):
        for role, n in senders:
            got(q_got.at[role, n, xx], q_recv.at[role, n, xx])

        @pl.loop(0, 4)
        def _(zz):
            for yy in range(4):
                q_sum[xx, zz, yy] = (q_got[0, zz, xx, yy] + q_got[1, yy, xx, zz]).astype(jnp.bfloat16)

        pltpu.make_async_copy(q_sum.at[xx], q_hbm.at[xx], q_left.at[g]).start()

    def share_kv(g, passed=True):
        for n in (1, 2, 3, 5, 6, 7) if passed else range(1, 8):
            there = (pair_place if n >= 4 else place) - x + plus(x, n)
            got(pieces.at[c, g, there], piece_recv.at[g, there])
        send(pieces.at[c, g], pieces.at[c, g], pair_send.at[g], pair_recv.at[g], mate)
        pltpu.make_async_copy(pieces.at[c, g], pieces_hbm.at[c, g], pieces_left.at[g, 0]).start()

    def pair_got(g):
        got(pieces.at[d, g], pair_recv.at[g])
        pltpu.make_async_copy(pieces.at[d, g], pieces_hbm.at[d, g], pieces_left.at[g, 1]).start()

    load_wq.wait()
    for vv, k in ((vm, d), (vp, c), (vo, c), (vo, d)):
        thin_got(x, vv, k)

    @pl.loop(0, 1)
    def _(i):
        q_block(x, plus(u, i))
        send_q(1, x, 0, False)

    wq_got(um, c)
    send_wq(wq.at[um, c], um, c, u_next)
    wkv_got(up, d)
    send_wkv(wkv.at[up, d], up, d, u_last)
    pass_x(vm)
    wq_got(up, d)
    send_wq(wq.at[up, d], up, d, u_last)
    pass_x(vp)
    wq_got(um, d)
    wq_got(up, c)

    @pl.loop(0, 2)
    def _(i):
        q_block(x, plus(um, 2 * i))
        send_q(1, x, plus(2 * i, 3))

    thin_got(xo, vm, d)
    thin_got(xo, vp, c)
    thin_got(xo, vo, c)
    thin_got(xo, vo, d)
    far_got(v)
    far_rows(0, v, 1, 4)
    pass_x(vo)
    wkv_got(um, d)
    wkv_got(up, c)
    for k in (c, d):
        wkv_got(uo, k)
    for xx, k in ((xm, d), (xp, c)):
        for vv in (v, vm, vp, vo):
            wide_got(xx, vv, k)
        for vv, kk in ((vm, d), (vp, c), (vo, c), (vo, d)):
            thin_got(xx, vv, kk)

    @pl.loop(0, 3)
    def _(g):
        kv_group(g, plus(xm, g))

    @pl.loop(0, 2)
    def _(i):
        @pl.loop(0, 3)
        def _(j):
            q_block(plus(xm, 2 * i), plus(um, j))
            send_q(2 * i, plus(xm, 2 * i), plus(j, 3), j != 1)

    for k in (c, d):
        wq_got(uo, k)

    @pl.loop(0, 3)
    def _(g):
        xx = plus(xm, g)
        q_block(xx, uo)
        send_q(g, xx, 2)
        q_got[c, u, xx] = q_part[xx, u, c]

    far_rows(0, v, 0, 1)

    @pl.loop(0, 2)
    def _(i):
        far_got(plus(vm, 2 * i))
        far_rows(1 + i, plus(vm, 2 * i), 0, 4)

    for g in range(3):
        add_kv(g, plus(xm, g))
    far_got(vo)
    kv_group(3, xo)
    far_rows(3, vo, 0, 4)
    q_got[c, u, xo] = q_part[xo, u, c]
    for g in range(3):
        pass_kv(g)
    for g in range(3):
        add_q(g, plus(xm, g))

    got(other, row_send.at[0])
    for n, kind in enumerate(counts["kinds"]):
        got(rows.at[0, 0, 0, :, kind], row_send.at[n + 1])
    for n in range(counts["wq"]):
        got(wq.at[0, 0], wq_send.at[n])
    for n in range(counts["wkv"]):
        got(wkv.at[0, 0], wkv_send.at[n])

    @pl.loop(0, 4)
    def _(du):
        def drained(k):
            for g in range(3):
                got(q_part.at[0, 0, 0], q_send.at[g, du, k])
            for t in range(4):
                got(q_part.at[0, 0, 0, 0], q_send_far.at[t, plus(u, du), k])
                got(kv_part.at[0, 0, 0], kv_send.at[t, du, k])

        drained(d)

        @pl.when(du > 0)
        def _():
            drained(c)

    add_kv(3, xo, direct=True)
    for g in range(3):
        share_kv(g)
    add_q(3, xo)
    share_kv(3, passed=False)
    for g in range(4):
        pair_got(g)
    for g in range(4):
        for n in (0, 1, 2, 3, 5, 6, 7):
            got(pieces.at[0, 0, 0], piece_send.at[g, n])
        got(pieces.at[0, 0], pair_send.at[g])
        got(q_sum.at[0], q_left.at[g])
        for n in (0, 1):
            got(pieces.at[0, 0], pieces_left.at[g, n])


def finish_kernel(q_hbm, pieces_hbm, q_out, k_out, v_out, q, pieces, k, v, loads, stores):
    def lanes(zz):
        return slice(zz * 256, (zz + 1) * 256)

    piece_loads = [pltpu.make_async_copy(pieces_hbm.at[..., lanes(zz)], pieces.at[..., lanes(zz)], loads.at[zz]) for zz in range(4)]
    q_loads = [pltpu.make_async_copy(q_hbm.at[xx], q.at[xx], loads.at[4 + xx]) for xx in range(4)]
    for load in piece_loads + q_loads:
        load.start()
    copies = []

    def store(src, dst):
        copy = pltpu.make_async_copy(src, dst, stores.at[len(copies)])
        copy.start()
        copies.append(copy)

    for zz in range(4):
        piece_loads[zz].wait()
        for xx in range(4):
            places = [((xx - n + 1) % 4, n) for n in range(8)]
            wide = [pieces[core, g, n, :, lanes(zz)].astype(jnp.float32) for g, n in places for core in (0, 1)]
            for out, first in ((k, 0), (v, 8)):
                value = jnp.concatenate([w[first:first + 8] for w in wide], axis=0).T.astype(jnp.bfloat16)
                out[zz, :, xx] = value.reshape(4, 64, 128)
        store(k.at[zz], k_out.at[zz])
        store(v.at[zz], v_out.at[zz])
    for xx in range(4):
        q_loads[xx].wait()
        store(q.at[xx], q_out.at[:, :, xx])
    for copy in copies:
        copy.wait()


def solution(mesh):
    def local_step(x_rows, norm_gain, w_q, w_k, w_v):
        depth = x_rows.shape[1]
        half = depth // 2
        any_space = pl.BlockSpec(memory_space=pl.ANY)
        vmem = pl.BlockSpec(memory_space=pltpu.VMEM)
        bf16, f32 = jnp.bfloat16, jnp.float32
        out = jax.ShapeDtypeStruct((4, 4, 4, 64, 128), bf16)
        q_sum, pieces = pl.pallas_call(
            functools.partial(kernel, depth, half - half // 8),
            out_shape=(out, jax.ShapeDtypeStruct((2, 4, 8, 16, 1024), bf16)),
            in_specs=[any_space, vmem, any_space, any_space, any_space],
            out_specs=(any_space, any_space),
            scratch_shapes=[
                pltpu.VMEM((32, depth), bf16),
                pltpu.VMEM((32, half), bf16),
                pltpu.VMEM((16, half), bf16),
                pltpu.VMEM((4, 4, 2, 32, half), bf16),
                pltpu.VMEM((4, 2, half, 128), bf16),
                pltpu.VMEM((4, 2, 16, half), bf16),
                pltpu.VMEM((4, 4, 2, 4, 64, 128), f32),
                pltpu.VMEM((4, 4, 2, 16, 256), f32),
                pltpu.VMEM((2, 4, 4, 4, 64, 128), f32),
                pltpu.VMEM((2, 4, 4, 16, 256), f32),
                pltpu.VMEM((4, 4, 4, 64, 128), bf16),
                pltpu.VMEM((2, 4, 8, 16, 1024), bf16),
                DMA((6,)),
                DMA((4, 4, 2)),
                DMA((4, 4, 2)),
                DMA((61,)),
                DMA((4, 2)),
                DMA((4, 2)),
                DMA((7,)),
                DMA((7,)),
                DMA((3, 4, 2)),
                DMA((4, 4, 2)),
                DMA((4, 4, 2)),
                DMA((2, 4, 4)),
                DMA((2, 4, 4)),
                DMA((4, 8)),
                DMA((4, 8)),
                DMA((4,)),
                DMA((4,)),
                DMA((4,)),
                DMA((4, 2)),
            ],
            compiler_params=pltpu.CompilerParams(collective_id=0, has_side_effects=True, vmem_limit_bytes=67043328),
        )(x_rows, norm_gain.reshape(1, depth), w_q.reshape(depth, 128), w_k.T, w_v.T)
        outs = pl.pallas_call(
            finish_kernel,
            out_shape=(out, out, out),
            in_specs=[any_space, any_space],
            out_specs=(any_space, any_space, any_space),
            scratch_shapes=[
                pltpu.VMEM((4, 4, 4, 64, 128), bf16),
                pltpu.VMEM((2, 4, 8, 16, 1024), bf16),
                pltpu.VMEM((4, 4, 4, 64, 128), bf16),
                pltpu.VMEM((4, 4, 4, 64, 128), bf16),
                DMA((8,)),
                DMA((12,)),
            ],
            compiler_params=pltpu.CompilerParams(vmem_limit_bytes=67043328),
        )(q_sum, pieces)
        return tuple(value.reshape(4096, 1, 128) for value in outs)

    return jax.shard_map(
        local_step,
        mesh=mesh,
        in_specs=(P(("dp", "tp"), None), P(None), P(None, "tp", None), P(None, "tp"), P(None, "tp")),
        out_specs=(P("dp", "tp", None), P("dp", "tp", None), P("dp", "tp", None)),
        check_vma=False,
    )
```

```python
import functools

import jax
import jax.numpy as jnp
from jax import lax
from jax.experimental import pallas as pl
from jax.experimental.pallas import tpu as pltpu
from jax.sharding import PartitionSpec as P

EPSILON = 1e-6
MESH = pl.DeviceIdType.MESH
DMA = pltpu.SemaphoreType.DMA


def rem(a, b):
    return lax.rem(a, b)


def kernel(
    depth, split, x_hbm, gain, wq_hbm, wk_hbm, wv_hbm, q_hbm, pieces_hbm,
    x_in, other, wkv_other, rows, wq, wkv, q_part, kv_part, q_got, kv_got, q_sum, pieces,
    load_sem, wide_recv, thin_recv, row_send, wq_recv, wkv_recv, wq_send, wkv_send, q_send, kv_send, q_recv,
    kv_recv,
    piece_send, piece_recv, pair_send, pair_recv, q_left, pieces_left,
):
    half = depth // 2
    me = lax.axis_index("tp")
    c = rem(me, 2)
    x = rem(me // 2, 4)
    y = rem(me // 8, 4)
    z = me // 32
    u = z + c * (y - z)
    v = y + c * (z - y)
    mate = me + 1 - 2 * c
    d = 1 - c

    def chip(xx, uu, vv):
        zz = uu + c * (vv - uu)
        yy = vv + c * (uu - vv)
        return ((zz * 4 + yy) * 4 + xx) * 2

    def plus(a, n):
        return rem(a + n, 4)

    def send(src, dst, send_sem, recv_sem, target):
        copy = pltpu.make_async_remote_copy(
            src_ref=src, dst_ref=dst, send_sem=send_sem, recv_sem=recv_sem, device_id={"tp": target}, device_id_type=MESH
        )
        copy.start()

    def got(ref, sem):
        pltpu.make_async_copy(ref, ref, sem).wait()

    load_x = pltpu.make_async_copy(x_hbm, x_in, load_sem.at[0])
    load_x.start()
    own_columns = pl.ds(pl.multiple_of(c * half, half), half)
    mate_columns = pl.ds(pl.multiple_of(d * half, half), half)
    loads = [
        pltpu.make_async_copy(wk_hbm.at[:, mate_columns], wkv_other.at[0:8], load_sem.at[1]),
        pltpu.make_async_copy(wv_hbm.at[:, mate_columns], wkv_other.at[8:16], load_sem.at[2]),
        pltpu.make_async_copy(wk_hbm.at[:, own_columns], wkv.at[u, c, 0:8], load_sem.at[3]),
        pltpu.make_async_copy(wv_hbm.at[:, own_columns], wkv.at[u, c, 8:16], load_sem.at[4]),
    ]
    for load in loads:
        load.start()
    load_wq = pltpu.make_async_copy(wq_hbm.at[own_columns, :], wq.at[u, c], load_sem.at[5])
    load_wq.start()

    barrier = pltpu.get_barrier_semaphore()
    y_pair = y + 1 - 2 * rem(y, 2)
    peers = [mate]
    for n in (1, 2, 3):
        for k in (0, 1):
            peers.append(((z * 4 + plus(y, n)) * 4 + x) * 2 + k)
            peers.append(((plus(z, n) * 4 + y) * 4 + x) * 2 + k)
        peers.append(((z * 4 + y) * 4 + plus(x, n)) * 2 + c)
        peers.append(((z * 4 + y_pair) * 4 + plus(x, n)) * 2 + c)
    for peer in peers:
        pl.semaphore_signal(barrier, inc=1, device_id={"tp": peer}, device_id_type=MESH)

    load_x.wait()
    width = min(1024, half)

    def squares(j, total):
        part = x_in[:, pl.ds(pl.multiple_of(j * width, width), width)].astype(jnp.float32)
        return total + part * part

    total = lax.fori_loop(0, depth // width, squares, jnp.zeros((32, width), jnp.float32))
    scale = lax.rsqrt(jnp.sum(total, axis=1, keepdims=True) / depth + EPSILON)

    def normed(first):
        columns = pl.ds(pl.multiple_of(first, width), width)
        return (x_in[:, columns].astype(jnp.float32) * scale * gain[:, columns]).astype(jnp.bfloat16)

    @pl.loop(0, half // width)
    def _(j):
        columns = pl.ds(pl.multiple_of(j * width, width), width)
        other[:, columns] = normed(d * half + j * width)
        rows[x, v, c, :, columns] = normed(c * half + j * width)

    for load in loads:
        load.wait()
    pl.semaphore_wait(barrier, len(peers))

    counts = {"wide": 0, "thin": 0, "wq": 0, "wkv": 0}
    wide, thin = slice(0, split), slice(split, half)

    def row_sem(kind):
        counts[kind] += 1
        return row_send.at[1 if counts[kind] <= 24 else 2]

    def send_wide(xx, vv, k, *to):
        for target in to:
            send(rows.at[xx, vv, k, :, wide], rows.at[xx, vv, k, :, wide], row_sem("wide"), wide_recv.at[xx, vv, k], target)

    def send_thin(xx, vv, k, *to):
        for target in to:
            send(rows.at[xx, vv, k, :, thin], rows.at[xx, vv, k, :, thin], row_sem("thin"), thin_recv.at[xx, vv, k], target)

    def wide_got(xx, vv, k):
        got(rows.at[xx, vv, k, :, wide], wide_recv.at[xx, vv, k])

    def thin_got(xx, vv, k):
        got(rows.at[xx, vv, k, :, thin], thin_recv.at[xx, vv, k])

    def send_wq(src, uu, k, target):
        send(src, wq.at[uu, k], wq_send.at[counts["wq"] // 6], wq_recv.at[uu, k], target)
        counts["wq"] += 1

    def send_wkv(src, uu, k, target):
        send(src, wkv.at[uu, k], wkv_send.at[counts["wkv"] // 6], wkv_recv.at[uu, k], target)
        counts["wkv"] += 1

    def wq_got(uu, k):
        got(wq.at[uu, k], wq_recv.at[uu, k])

    def wkv_got(uu, k):
        got(wkv.at[uu, k], wkv_recv.at[uu, k])

    x_next, x_last = chip(plus(x, 1), u, v) + c, chip(plus(x, 3), u, v) + c
    v_next, v_last = chip(x, u, plus(v, 1)) + c, chip(x, u, plus(v, 3)) + c
    u_next, u_last = chip(x, plus(u, 1), v) + c, chip(x, plus(u, 3), v) + c
    xp, xm, xo = plus(x, 1), plus(x, 3), plus(x, 2)
    vp, vm, vo = plus(v, 1), plus(v, 3), plus(v, 2)
    up, um, uo = plus(u, 1), plus(u, 3), plus(u, 2)

    near_x, near_v, near_u = (x_next, x_last), (v_next, v_last), (u_next, u_last)

    send(other, rows.at[x, u, c], row_send.at[0], wide_recv.at[x, u, c], mate)
    send_thin(x, v, c, *near_x)
    send_wide(x, v, c, *near_v)
    for target in near_u:
        send_wkv(wkv.at[u, c], u, c, target)
    for target in near_u:
        send_wq(wq_hbm.at[own_columns, :], u, c, target)
    send_wkv(wkv_other, v, c, mate)
    send_wq(wq_hbm.at[mate_columns, :], v, c, mate)
    got(rows.at[x, v, d], wide_recv.at[x, v, d])
    send_thin(x, v, d, *near_x)
    send_wide(x, v, c, *near_x)
    send_wide(x, v, d, *near_v)
    send_wide(x, v, d, *near_x)
    for k in (c, d):
        send_thin(x, v, k, *near_v)
    wkv_got(u, d)
    for target in near_u:
        send_wkv(wkv.at[u, d], u, d, target)
    wq_got(u, d)
    for target in near_u:
        send_wq(wq.at[u, d], u, d, target)

    def pass_thin_x(vv):
        thin_got(xm, vv, c)
        send_thin(xm, vv, c, x_next)
        thin_got(xp, vv, d)
        send_thin(xp, vv, d, x_last)

    def pass_x(vv):
        wide_got(xm, vv, c)
        send_wide(xm, vv, c, x_next)
        wide_got(xp, vv, d)
        send_wide(xp, vv, d, x_last)

    pass_thin_x(v)
    thin_got(xm, v, d)
    thin_got(xp, v, c)
    for xx in (xm, xp):
        for k in (c, d):
            send_thin(xx, v, k, *near_v)

    wide_got(x, vm, c)
    send_wide(x, vm, c, v_next)
    wkv_got(um, c)
    send_wkv(wkv.at[um, c], um, c, u_next)
    wide_got(xm, v, c)
    send_wide(xm, v, c, x_next)
    wide_got(x, vp, c)
    for vv in (vm, vp):
        send_wide(x, vv, c, *near_x)
    wide_got(x, vp, d)
    send_wide(x, vp, d, v_last)
    wide_got(xp, v, d)
    send_wide(xp, v, d, x_last)
    wide_got(x, vm, d)
    for vv in (vm, vp):
        send_wide(x, vv, d, *near_x)
    for k in (c, d):
        thin_got(xo, v, k)
        send_thin(xo, v, k, *near_v)
    for k in (c, d):
        wide_got(x, vo, k)
        send_wide(x, vo, k, *near_x)
    for xx in (x, xm, xp, xo):
        thin_got(xx, vm, c)
        send_thin(xx, vm, c, v_next)
        thin_got(xx, vp, d)
        send_thin(xx, vp, d, v_last)

    def q_block(xx, uu):
        right = jnp.concatenate([wq[uu, 0], wq[uu, 1]], axis=1)
        value = jnp.dot(rows[xx].reshape(256, half), right, preferred_element_type=jnp.float32)
        for k in (0, 1):
            q_part[xx, uu, k] = value[:, k * 128:(k + 1) * 128].reshape(4, 64, 128)

    def send_q(xx, du, whole=True):
        uu = plus(u, du)

        def to(k):
            mated = 1 - (du + 3) // 4
            send(q_part.at[xx, uu, k], q_got.at[c, u, xx], q_send.at[mated], q_recv.at[c, xx], chip(x, uu, v) + k)

        to(d)

        @pl.when(whole)
        def _():
            to(c)

    def kv_group(xx):
        value = lax.dot_general(
            wkv[...].reshape(128, half), rows[xx].reshape(256, half), (((1,), (1,)), ((), ())), preferred_element_type=jnp.float32
        )
        kv_part[xx] = value.reshape(4, 2, 16, 256)
        for du in (2, 1, 3, 0):
            uu = plus(u, du)
            for k in ((c, d) if du else (d,)):
                send(kv_part.at[xx, uu, k], kv_got.at[c, u, xx], kv_send.at[0 if du else 1], kv_recv.at[c, xx], chip(x, uu, v) + k)
        kv_got[c, u, xx] = kv_part[xx, u, c]

    def far_rows(vv, first, last, final=False):
        @pl.loop(first, last)
        def _(j):
            uu = plus(u, 2 + j)
            right = jnp.concatenate([wq[uu, 0], wq[uu, 1]], axis=1)
            value = jnp.dot(rows[xo, vv].reshape(64, half), right, preferred_element_type=jnp.float32)
            for k in (0, 1):
                q_part[xo, uu, k, vv] = value[:, k * 128:(k + 1) * 128]
            if final:
                send_q(xo, plus(j, 2), j != 2)

                @pl.when(j == 1)
                def _():
                    for g in range(3):
                        pass_kv(g)

    def far_got(vv):
        wide_got(xo, vv, c)
        wide_got(xo, vv, d)

    place = rem(y, 2) * 4 + x

    def add_kv(g, xx, direct=False):
        got(kv_got.at[0, 0:3, 0], kv_recv.at[c, xx])
        got(kv_got.at[0, :, 0], kv_recv.at[d, xx])
        for zz in range(4):
            second = jnp.concatenate([kv_got[1, yy, xx][:, zz * 64:(zz + 1) * 64] for yy in range(4)], axis=1)
            pieces[c, g, place, :, pl.ds(zz * 256, 256)] = (kv_got[0, zz, xx] + second).astype(jnp.bfloat16)
        own = pieces.at[c, g, place]
        send(own, own, piece_send, piece_recv.at[g, 0], row_chip(0, y_pair) + c)
        for n in range(1, 4):
            send(own, own, piece_send, piece_recv.at[g, 1], row_chip(n, y) + c)
            if direct:
                send(own, own, piece_send, piece_recv.at[g, 1], row_chip(n, y_pair) + c)

    def row_chip(n, yy):
        return ((z * 4 + yy) * 4 + plus(x, n)) * 2

    pair_place = 4 - place + 2 * x

    def pass_kv(g):
        theirs = pieces.at[c, g, pair_place]
        got(theirs, piece_recv.at[g, 0])
        for n in range(1, 4):
            send(theirs, theirs, piece_send, piece_recv.at[g, 1], row_chip(n, y) + c)

    def add_q(g, xx):
        got(q_got.at[0, 0:3, 0], q_recv.at[c, xx])
        got(q_got.at[0, :, 0], q_recv.at[d, xx])

        @pl.loop(0, 4)
        def _(zz):
            for yy in range(4):
                q_sum[xx, zz, yy] = (q_got[0, zz, xx, yy] + q_got[1, yy, xx, zz]).astype(jnp.bfloat16)

        pltpu.make_async_copy(q_sum.at[xx], q_hbm.at[xx], q_left).start()

    def share_kv(g, passed=True):
        if not passed:
            got(pieces.at[c, g, pair_place], piece_recv.at[g, 0])
        got(pieces.at[c, g, 0:6], piece_recv.at[g, 1])
        send(pieces.at[c, g], pieces.at[c, g], pair_send, pair_recv.at[g // 3], mate)
        pltpu.make_async_copy(pieces.at[c, g], pieces_hbm.at[c, g], pieces_left).start()

    load_wq.wait()
    for vv, k in ((vm, d), (vp, c), (vo, c), (vo, d)):
        thin_got(x, vv, k)

    @pl.loop(0, 1)
    def _(i):
        q_block(x, plus(u, i))
        send_q(x, 0, False)

    wq_got(um, c)
    send_wq(wq.at[um, c], um, c, u_next)
    wkv_got(up, d)
    send_wkv(wkv.at[up, d], up, d, u_last)
    pass_x(vm)
    wq_got(up, d)
    send_wq(wq.at[up, d], up, d, u_last)
    pass_x(vp)
    wq_got(um, d)
    wq_got(up, c)

    @pl.loop(0, 2)
    def _(i):
        q_block(x, plus(um, 2 * i))
        send_q(x, plus(2 * i, 3))

    thin_got(xo, vm, d)
    thin_got(xo, vp, c)
    thin_got(xo, vo, c)
    thin_got(xo, vo, d)
    far_got(v)
    far_rows(v, 1, 4)
    pass_x(vo)
    wkv_got(um, d)
    wkv_got(up, c)
    for k in (c, d):
        wkv_got(uo, k)
    for xx, k in ((xm, d), (xp, c)):
        for vv in (v, vm, vp, vo):
            wide_got(xx, vv, k)
        for vv, kk in ((vm, d), (vp, c), (vo, c), (vo, d)):
            thin_got(xx, vv, kk)

    @pl.loop(0, 3)
    def _(g):
        kv_group(plus(xm, g))

    @pl.loop(0, 2)
    def _(i):
        @pl.loop(0, 3)
        def _(j):
            q_block(plus(xm, 2 * i), plus(um, j))
            send_q(plus(xm, 2 * i), plus(j, 3), j != 1)

    for k in (c, d):
        wq_got(uo, k)

    @pl.loop(0, 3)
    def _(g):
        xx = plus(xm, g)
        q_block(xx, uo)
        send_q(xx, 2)
        q_got[c, u, xx] = q_part[xx, u, c]

    for g in range(3):
        add_kv(g, plus(xm, g))
    far_rows(v, 0, 1)

    @pl.loop(0, 2)
    def _(i):
        far_got(plus(vm, 2 * i))
        far_rows(plus(vm, 2 * i), 0, 4)

    far_got(vo)
    kv_group(xo)
    far_rows(vo, 0, 4, True)
    q_got[c, u, xo] = q_part[xo, u, c]
    add_kv(3, xo, direct=True)
    for g in range(3):
        add_q(g, plus(xm, g))
    for g in range(3):
        share_kv(g)

    got(other, row_send.at[0])
    got(rows.at[0:3], row_send.at[1])
    got(rows.at[3, 0:3], row_send.at[2])
    got(wq.at[0:3], wq_send.at[0])
    got(wq.at[3, 0], wq_send.at[1])
    got(wkv.at[0:3], wkv_send.at[0])
    got(wkv.at[3, 0], wkv_send.at[1])
    got(q_part.at[0:3], q_send.at[0])
    got(q_part.at[3, 0:2], q_send.at[1])
    got(kv_part.at[0:3], kv_send.at[0])
    got(kv_part.at[3, 0:2], kv_send.at[1])

    add_q(3, xo)
    got(pieces.at[d, 0:3], pair_recv.at[0])
    for g in range(3):
        pltpu.make_async_copy(pieces.at[d, g], pieces_hbm.at[d, g], pieces_left).start()
    share_kv(3, passed=False)
    got(pieces.at[d, 3], pair_recv.at[1])
    pltpu.make_async_copy(pieces.at[d, 3], pieces_hbm.at[d, 3], pieces_left).start()
    got(pieces.at[0, :, 0:7], piece_send)
    got(pieces.at[0], pair_send)
    got(q_sum, q_left)
    got(pieces, pieces_left)


def finish_kernel(q_hbm, pieces_hbm, q_out, k_out, v_out, q, pieces, k, v, loads, stores):
    def lanes(zz):
        return slice(zz * 256, (zz + 1) * 256)

    piece_loads = [pltpu.make_async_copy(pieces_hbm.at[..., lanes(zz)], pieces.at[..., lanes(zz)], loads.at[zz]) for zz in range(4)]
    q_loads = [pltpu.make_async_copy(q_hbm.at[xx], q.at[xx], loads.at[4 + xx]) for xx in range(4)]
    for load in piece_loads + q_loads:
        load.start()
    copies = []

    def store(src, dst):
        copy = pltpu.make_async_copy(src, dst, stores.at[len(copies)])
        copy.start()
        copies.append(copy)

    for zz in range(4):
        piece_loads[zz].wait()
        for xx in range(4):
            places = [((xx - n + 1) % 4, n) for n in range(8)]
            wide = [pieces[core, g, n, :, lanes(zz)].astype(jnp.float32) for g, n in places for core in (0, 1)]
            for out, first in ((k, 0), (v, 8)):
                value = jnp.concatenate([w[first:first + 8] for w in wide], axis=0).T.astype(jnp.bfloat16)
                out[zz, :, xx] = value.reshape(4, 64, 128)
        store(k.at[zz], k_out.at[zz])
        store(v.at[zz], v_out.at[zz])
    for xx in range(4):
        q_loads[xx].wait()
        store(q.at[xx], q_out.at[:, :, xx])
    for copy in copies:
        copy.wait()


def solution(mesh):
    def local_step(x_rows, norm_gain, w_q, w_k, w_v):
        depth = x_rows.shape[1]
        half = depth // 2
        any_space = pl.BlockSpec(memory_space=pl.ANY)
        vmem = pl.BlockSpec(memory_space=pltpu.VMEM)
        bf16, f32 = jnp.bfloat16, jnp.float32
        out = jax.ShapeDtypeStruct((4, 4, 4, 64, 128), bf16)
        q_sum, pieces = pl.pallas_call(
            functools.partial(kernel, depth, half - 5 * half // 32),
            out_shape=(out, jax.ShapeDtypeStruct((2, 4, 8, 16, 1024), bf16)),
            in_specs=[any_space, vmem, any_space, any_space, any_space],
            out_specs=(any_space, any_space),
            scratch_shapes=[
                pltpu.VMEM((32, depth), bf16),
                pltpu.VMEM((32, half), bf16),
                pltpu.VMEM((16, half), bf16),
                pltpu.VMEM((4, 4, 2, 32, half), bf16),
                pltpu.VMEM((4, 2, half, 128), bf16),
                pltpu.VMEM((4, 2, 16, half), bf16),
                pltpu.VMEM((4, 4, 2, 4, 64, 128), f32),
                pltpu.VMEM((4, 4, 2, 16, 256), f32),
                pltpu.VMEM((2, 4, 4, 4, 64, 128), f32),
                pltpu.VMEM((2, 4, 4, 16, 256), f32),
                pltpu.VMEM((4, 4, 4, 64, 128), bf16),
                pltpu.VMEM((2, 4, 8, 16, 1024), bf16),
                DMA((6,)),
                DMA((4, 4, 2)),
                DMA((4, 4, 2)),
                DMA((3,)),
                DMA((4, 2)),
                DMA((4, 2)),
                DMA((2,)),
                DMA((2,)),
                DMA((2,)),
                DMA((2,)),
                DMA((2, 4)),
                DMA((2, 4)),
                DMA(()),
                DMA((4, 2)),
                DMA(()),
                DMA((2,)),
                DMA(()),
                DMA(()),
            ],
            compiler_params=pltpu.CompilerParams(collective_id=0, has_side_effects=True, vmem_limit_bytes=67043328),
        )(x_rows, norm_gain.reshape(1, depth), w_q.reshape(depth, 128), w_k.T, w_v.T)
        outs = pl.pallas_call(
            finish_kernel,
            out_shape=(out, out, out),
            in_specs=[any_space, any_space],
            out_specs=(any_space, any_space, any_space),
            scratch_shapes=[
                pltpu.VMEM((4, 4, 4, 64, 128), bf16),
                pltpu.VMEM((2, 4, 8, 16, 1024), bf16),
                pltpu.VMEM((4, 4, 4, 64, 128), bf16),
                pltpu.VMEM((4, 4, 4, 64, 128), bf16),
                DMA((8,)),
                DMA((12,)),
            ],
            compiler_params=pltpu.CompilerParams(vmem_limit_bytes=67043328),
        )(q_sum, pieces)
        return tuple(value.reshape(4096, 1, 128) for value in outs)

    return jax.shard_map(
        local_step,
        mesh=mesh,
        in_specs=(P(("dp", "tp"), None), P(None), P(None, "tp", None), P(None, "tp"), P(None, "tp")),
        out_specs=(P("dp", "tp", None), P("dp", "tp", None), P("dp", "tp", None)),
        check_vma=False,
    )
```

```python
import functools

import jax
import jax.numpy as jnp
from jax import lax
from jax.experimental import pallas as pl
from jax.experimental.pallas import tpu as pltpu
from jax.sharding import PartitionSpec as P

EPSILON = 1e-6
MESH = pl.DeviceIdType.MESH
DMA = pltpu.SemaphoreType.DMA


def rem(a, b):
    return lax.rem(a, b)


def kernel(
    depth, split, middle, x_hbm, gain_hbm, wq_hbm, wk_hbm, wv_hbm, q_hbm, pieces_hbm,
    x_in, gain, other, wkv_other, rows, wq, wkv, q_part, kv_part, q_got, kv_got, q_sum, pieces,
    load_sem, wide_recv, late_recv, thin_recv, row_send, wq_recv, wkv_recv, wq_send, wkv_send, q_send, kv_send, q_recv,
    kv_recv,
    piece_send, piece_recv, pair_send, pair_recv, q_left, pieces_left,
):
    half = depth // 2
    me = lax.axis_index("tp")
    c = rem(me, 2)
    x = rem(me // 2, 4)
    y = rem(me // 8, 4)
    z = me // 32
    u = z + c * (y - z)
    v = y + c * (z - y)
    mate = me + 1 - 2 * c
    d = 1 - c

    def chip(xx, uu, vv):
        zz = uu + c * (vv - uu)
        yy = vv + c * (uu - vv)
        return ((zz * 4 + yy) * 4 + xx) * 2

    def plus(a, n):
        return rem(a + n, 4)

    def send(src, dst, send_sem, recv_sem, target):
        copy = pltpu.make_async_remote_copy(
            src_ref=src, dst_ref=dst, send_sem=send_sem, recv_sem=recv_sem, device_id={"tp": target}, device_id_type=MESH
        )
        copy.start()

    def got(ref, sem):
        pltpu.make_async_copy(ref, ref, sem).wait()

    load_x = pltpu.make_async_copy(x_hbm, x_in, load_sem.at[0])
    load_x.start()
    load_gain = pltpu.make_async_copy(gain_hbm, gain, load_sem.at[6])
    load_gain.start()
    own_columns = pl.ds(pl.multiple_of(c * half, half), half)
    mate_columns = pl.ds(pl.multiple_of(d * half, half), half)
    loads = [
        pltpu.make_async_copy(wk_hbm.at[:, mate_columns], wkv_other.at[0:8], load_sem.at[1]),
        pltpu.make_async_copy(wv_hbm.at[:, mate_columns], wkv_other.at[8:16], load_sem.at[2]),
        pltpu.make_async_copy(wk_hbm.at[:, own_columns], wkv.at[u, c, 0:8], load_sem.at[3]),
        pltpu.make_async_copy(wv_hbm.at[:, own_columns], wkv.at[u, c, 8:16], load_sem.at[4]),
    ]
    for load in loads:
        load.start()
    load_wq = pltpu.make_async_copy(wq_hbm.at[own_columns, :], wq.at[u, c], load_sem.at[5])
    load_wq.start()

    barrier = pltpu.get_barrier_semaphore()
    y_pair = y + 1 - 2 * rem(y, 2)
    peers = [mate]
    for n in (1, 2, 3):
        for k in (0, 1):
            peers.append(((z * 4 + plus(y, n)) * 4 + x) * 2 + k)
            peers.append(((plus(z, n) * 4 + y) * 4 + x) * 2 + k)
        peers.append(((z * 4 + y) * 4 + plus(x, n)) * 2 + c)
        peers.append(((z * 4 + y_pair) * 4 + plus(x, n)) * 2 + c)
    for peer in peers:
        pl.semaphore_signal(barrier, inc=1, device_id={"tp": peer}, device_id_type=MESH)

    load_x.wait()
    load_gain.wait()
    width = min(1024, half)

    def squares(j, total):
        part = x_in[:, pl.ds(pl.multiple_of(j * width, width), width)].astype(jnp.float32)
        return total + part * part

    total = lax.fori_loop(0, depth // width, squares, jnp.zeros((32, width), jnp.float32))
    scale = lax.rsqrt(jnp.sum(total, axis=1, keepdims=True) / depth + EPSILON)

    def normed(first):
        columns = pl.ds(pl.multiple_of(first, width), width)
        return (x_in[:, columns].astype(jnp.float32) * scale * gain[:, columns]).astype(jnp.bfloat16)

    @pl.loop(0, half // width)
    def _(j):
        columns = pl.ds(pl.multiple_of(j * width, width), width)
        other[:, columns] = normed(d * half + j * width)
        rows[x, v, c, :, columns] = normed(c * half + j * width)

    for load in loads:
        load.wait()
    pl.semaphore_wait(barrier, len(peers))

    counts = {"wide": 0, "thin": 0, "wq": 0, "wkv": 0}
    wide, thin = slice(0, split), slice(split, half)
    early, late, whole = slice(0, middle), slice(middle, split), slice(0, half)
    rest = slice(middle, half)

    def row_sem(kind):
        counts[kind] += 1
        return row_send.at[1 if counts[kind] <= 24 else 2]

    def send_wide(xx, vv, k, *to):
        for target in to:
            send(rows.at[xx, vv, k, :, wide], rows.at[xx, vv, k, :, wide], row_sem("wide"), wide_recv.at[xx, vv, k], target)

    def send_thin(xx, vv, k, *to):
        for target in to:
            send(rows.at[xx, vv, k, :, thin], rows.at[xx, vv, k, :, thin], row_sem("thin"), thin_recv.at[xx, vv, k], target)

    def send_early(xx, k, *to):
        for target in to:
            send(rows.at[xx, vo, k, :, early], rows.at[xx, vo, k, :, early], row_send.at[2], wide_recv.at[xx, vo, k], target)

    def send_late(xx, k, *to):
        for target in to:
            send(rows.at[xx, vo, k, :, late], rows.at[xx, vo, k, :, late], row_send.at[2], late_recv.at[xx, k], target)

    def early_got(xx, k):
        got(rows.at[xx, vo, k, :, early], wide_recv.at[xx, vo, k])

    def late_got(xx, k):
        got(rows.at[xx, vo, k, :, late], late_recv.at[xx, k])

    def wide_got(xx, vv, k):
        got(rows.at[xx, vv, k, :, wide], wide_recv.at[xx, vv, k])

    def thin_got(xx, vv, k):
        got(rows.at[xx, vv, k, :, thin], thin_recv.at[xx, vv, k])

    def send_wq(src, uu, k, target):
        send(src, wq.at[uu, k], wq_send.at[counts["wq"] // 6], wq_recv.at[uu, k], target)
        counts["wq"] += 1

    def send_wkv(src, uu, k, target):
        send(src, wkv.at[uu, k], wkv_send.at[counts["wkv"] // 6], wkv_recv.at[uu, k], target)
        counts["wkv"] += 1

    def wq_got(uu, k):
        got(wq.at[uu, k], wq_recv.at[uu, k])

    def wkv_got(uu, k):
        got(wkv.at[uu, k], wkv_recv.at[uu, k])

    x_next, x_last = chip(plus(x, 1), u, v) + c, chip(plus(x, 3), u, v) + c
    v_next, v_last = chip(x, u, plus(v, 1)) + c, chip(x, u, plus(v, 3)) + c
    u_next, u_last = chip(x, plus(u, 1), v) + c, chip(x, plus(u, 3), v) + c
    xp, xm, xo = plus(x, 1), plus(x, 3), plus(x, 2)
    vp, vm, vo = plus(v, 1), plus(v, 3), plus(v, 2)
    up, um, uo = plus(u, 1), plus(u, 3), plus(u, 2)

    near_x, near_v, near_u = (x_next, x_last), (v_next, v_last), (u_next, u_last)

    send(other, rows.at[x, u, c], row_send.at[0], wide_recv.at[x, u, c], mate)
    send_thin(x, v, c, *near_x)
    send_wide(x, v, c, *near_v)
    for target in near_u:
        send_wkv(wkv.at[u, c], u, c, target)
    for target in near_u:
        send_wq(wq_hbm.at[own_columns, :], u, c, target)
    send_wkv(wkv_other, v, c, mate)
    send_wq(wq_hbm.at[mate_columns, :], v, c, mate)
    got(rows.at[x, v, d], wide_recv.at[x, v, d])
    send_thin(x, v, d, *near_x)
    send_wide(x, v, c, *near_x)
    send_wide(x, v, d, *near_v)
    send_wide(x, v, d, *near_x)
    for k in (c, d):
        send_thin(x, v, k, *near_v)
    wkv_got(u, d)
    for target in near_u:
        send_wkv(wkv.at[u, d], u, d, target)
    wq_got(u, d)
    for target in near_u:
        send_wq(wq.at[u, d], u, d, target)

    def pass_thin_x(vv):
        thin_got(xm, vv, c)
        send_thin(xm, vv, c, x_next)
        thin_got(xp, vv, d)
        send_thin(xp, vv, d, x_last)

    def pass_x(vv):
        wide_got(xm, vv, c)
        send_wide(xm, vv, c, x_next)
        wide_got(xp, vv, d)
        send_wide(xp, vv, d, x_last)

    pass_thin_x(v)
    thin_got(xm, v, d)
    thin_got(xp, v, c)
    for xx in (xm, xp):
        for k in (c, d):
            send_thin(xx, v, k, *near_v)

    wide_got(x, vm, c)
    send_wide(x, vm, c, v_next)
    wkv_got(um, c)
    send_wkv(wkv.at[um, c], um, c, u_next)
    wide_got(xm, v, c)
    send_wide(xm, v, c, x_next)
    wide_got(x, vp, c)
    for vv in (vm, vp):
        send_wide(x, vv, c, *near_x)
    wide_got(x, vp, d)
    send_wide(x, vp, d, v_last)
    wide_got(xp, v, d)
    send_wide(xp, v, d, x_last)
    wide_got(x, vm, d)
    for vv in (vm, vp):
        send_wide(x, vv, d, *near_x)
    for k in (c, d):
        thin_got(xo, v, k)
        send_thin(xo, v, k, *near_v)
    for k in (c, d):
        wide_got(x, vo, k)
        send_early(x, k, *near_x)
        send_late(x, k, *near_x)
    for xx in (x, xm, xp, xo):
        thin_got(xx, vm, c)
        send_thin(xx, vm, c, v_next)
        thin_got(xx, vp, d)
        send_thin(xx, vp, d, v_last)

    def q_block(xx, uu):
        right = jnp.concatenate([wq[uu, 0], wq[uu, 1]], axis=1)
        value = jnp.dot(rows[xx].reshape(256, half), right, preferred_element_type=jnp.float32)
        for k in (0, 1):
            q_part[xx, uu, k] = value[:, k * 128:(k + 1) * 128].reshape(4, 64, 128)

    def send_q(xx, du, whole=True):
        uu = plus(u, du)

        def to(k):
            mated = 1 - (du + 3) // 4
            send(q_part.at[xx, uu, k], q_got.at[c, u, xx], q_send.at[mated], q_recv.at[c, xx], chip(x, uu, v) + k)

        to(d)

        @pl.when(whole)
        def _():
            to(c)

    def kv_value(xx, columns):
        count = columns.stop - columns.start
        value = lax.dot_general(
            wkv[:, :, :, columns].reshape(128, count), rows[xx, :, :, :, columns].reshape(256, count),
            (((1,), (1,)), ((), ())), preferred_element_type=jnp.float32,
        )
        return value.reshape(4, 2, 16, 256)

    def send_kv(xx):
        for du in (2, 1, 3, 0):
            uu = plus(u, du)
            for k in ((c, d) if du else (d,)):
                send(kv_part.at[xx, uu, k], kv_got.at[c, u, xx], kv_send.at[0 if du else 1], kv_recv.at[c, xx], chip(x, uu, v) + k)
        kv_got[c, u, xx] = kv_part[xx, u, c]

    def far_rows(vv, first, last, columns, second=False):
        count = columns.stop - columns.start

        @pl.loop(first, last)
        def _(j):
            uu = plus(u, 2 + j)
            right = jnp.concatenate([wq[uu, 0, columns], wq[uu, 1, columns]], axis=1)
            left = rows[xo, vv, :, :, columns].reshape(64, count)
            value = jnp.dot(left, right, preferred_element_type=jnp.float32)
            for k in (0, 1):
                part = value[:, k * 128:(k + 1) * 128]
                q_part[xo, uu, k, vv] = q_part[xo, uu, k, vv] + part if second else part
            if second:
                send_q(xo, plus(j, 2), j != 2)

                @pl.when(j == 1)
                def _():
                    for g in range(3):
                        pass_kv(g)

    def far_got(vv):
        wide_got(xo, vv, c)
        wide_got(xo, vv, d)

    place = rem(y, 2) * 4 + x

    def add_kv(g, xx, direct=False):
        got(kv_got.at[0, 0:3, 0], kv_recv.at[c, xx])
        got(kv_got.at[0, :, 0], kv_recv.at[d, xx])
        for zz in range(4):
            second = jnp.concatenate([kv_got[1, yy, xx][:, zz * 64:(zz + 1) * 64] for yy in range(4)], axis=1)
            pieces[c, g, place, :, pl.ds(zz * 256, 256)] = (kv_got[0, zz, xx] + second).astype(jnp.bfloat16)
        own = pieces.at[c, g, place]
        send(own, own, piece_send, piece_recv.at[g, 0], row_chip(0, y_pair) + c)
        for n in range(1, 4):
            send(own, own, piece_send, piece_recv.at[g, 1], row_chip(n, y) + c)
            if direct:
                send(own, own, piece_send, piece_recv.at[g, 1], row_chip(n, y_pair) + c)

    def row_chip(n, yy):
        return ((z * 4 + yy) * 4 + plus(x, n)) * 2

    pair_place = 4 - place + 2 * x

    def pass_kv(g):
        theirs = pieces.at[c, g, pair_place]
        got(theirs, piece_recv.at[g, 0])
        for n in range(1, 4):
            send(theirs, theirs, piece_send, piece_recv.at[g, 1], row_chip(n, y) + c)

    def add_q(g, xx):
        got(q_got.at[0, 0:3, 0], q_recv.at[c, xx])
        got(q_got.at[0, :, 0], q_recv.at[d, xx])

        @pl.loop(0, 4)
        def _(zz):
            for yy in range(4):
                q_sum[xx, zz, yy] = (q_got[0, zz, xx, yy] + q_got[1, yy, xx, zz]).astype(jnp.bfloat16)

        pltpu.make_async_copy(q_sum.at[xx], q_hbm.at[xx], q_left).start()

    def share_kv(g, passed=True):
        if not passed:
            got(pieces.at[c, g, pair_place], piece_recv.at[g, 0])
        got(pieces.at[c, g, 0:6], piece_recv.at[g, 1])
        send(pieces.at[c, g], pieces.at[c, g], pair_send, pair_recv.at[g // 3], mate)
        pltpu.make_async_copy(pieces.at[c, g], pieces_hbm.at[c, g], pieces_left).start()

    load_wq.wait()
    for vv, k in ((vm, d), (vp, c), (vo, c), (vo, d)):
        thin_got(x, vv, k)

    @pl.loop(0, 1)
    def _(i):
        q_block(x, plus(u, i))
        send_q(x, 0, False)

    wq_got(um, c)
    send_wq(wq.at[um, c], um, c, u_next)
    wkv_got(up, d)
    send_wkv(wkv.at[up, d], up, d, u_last)
    pass_x(vm)
    wq_got(up, d)
    send_wq(wq.at[up, d], up, d, u_last)
    pass_x(vp)
    wq_got(um, d)
    wq_got(up, c)

    @pl.loop(0, 2)
    def _(i):
        q_block(x, plus(um, 2 * i))
        send_q(x, plus(2 * i, 3))

    thin_got(xo, vm, d)
    thin_got(xo, vp, c)
    thin_got(xo, vo, c)
    thin_got(xo, vo, d)
    far_got(v)
    far_rows(v, 1, 4, whole)
    for xx, k, target in ((xm, c, x_next), (xp, d, x_last)):
        early_got(xx, k)
        send_early(xx, k, target)
        late_got(xx, k)
        send_late(xx, k, target)
    wkv_got(um, d)
    wkv_got(up, c)
    for k in (c, d):
        wkv_got(uo, k)
    for xx, k in ((xm, d), (xp, c)):
        for vv in (v, vm, vp):
            wide_got(xx, vv, k)
        early_got(xx, k)
        late_got(xx, k)
        for vv, kk in ((vm, d), (vp, c), (vo, c), (vo, d)):
            thin_got(xx, vv, kk)

    @pl.loop(0, 3)
    def _(g):
        xx = plus(xm, g)
        kv_part[xx] = kv_value(xx, slice(0, half))
        send_kv(xx)

    @pl.loop(0, 2)
    def _(i):
        @pl.loop(0, 3)
        def _(j):
            q_block(plus(xm, 2 * i), plus(um, j))
            send_q(plus(xm, 2 * i), plus(j, 3), j != 1)

    for k in (c, d):
        wq_got(uo, k)

    @pl.loop(0, 3)
    def _(g):
        xx = plus(xm, g)
        q_block(xx, uo)
        send_q(xx, 2)
        q_got[c, u, xx] = q_part[xx, u, c]

    for g in range(3):
        add_kv(g, plus(xm, g))
    far_rows(v, 0, 1, whole)

    @pl.loop(0, 2)
    def _(i):
        far_got(plus(vm, 2 * i))
        far_rows(plus(vm, 2 * i), 0, 4, whole)

    for k in (c, d):
        early_got(xo, k)
    kv_part[xo] = kv_value(xo, early)
    far_rows(vo, 0, 4, early)
    for k in (c, d):
        late_got(xo, k)
    kv_part[xo] = kv_part[xo] + kv_value(xo, rest)
    send_kv(xo)
    far_rows(vo, 0, 4, rest, True)
    q_got[c, u, xo] = q_part[xo, u, c]
    add_kv(3, xo, direct=True)
    for g in range(3):
        add_q(g, plus(xm, g))
    for g in range(3):
        share_kv(g)

    got(pieces.at[d, 0:3], pair_recv.at[0])
    for g in range(3):
        pltpu.make_async_copy(pieces.at[d, g], pieces_hbm.at[d, g], pieces_left).start()
    share_kv(3, passed=False)

    got(other, row_send.at[0])
    got(rows.at[0:3], row_send.at[1])
    got(rows.at[3, 0:3], row_send.at[2])
    got(wq.at[0:3], wq_send.at[0])
    got(wq.at[3, 0], wq_send.at[1])
    got(wkv.at[0:3], wkv_send.at[0])
    got(wkv.at[3, 0], wkv_send.at[1])
    got(kv_part.at[0:3], kv_send.at[0])
    got(kv_part.at[3, 0:2], kv_send.at[1])

    got(pieces.at[d, 3], pair_recv.at[1])
    pltpu.make_async_copy(pieces.at[d, 3], pieces_hbm.at[d, 3], pieces_left).start()
    add_q(3, xo)
    got(q_part.at[0:3], q_send.at[0])
    got(q_part.at[3, 0:2], q_send.at[1])
    got(pieces.at[0, :, 0:7], piece_send)
    got(pieces.at[0], pair_send)
    got(q_sum, q_left)
    got(pieces, pieces_left)


def finish_kernel(q_hbm, pieces_hbm, q_out, k_out, v_out, q, pieces, k, v, loads, stores):
    def lanes(zz):
        return slice(zz * 256, (zz + 1) * 256)

    piece_loads = [pltpu.make_async_copy(pieces_hbm.at[..., lanes(zz)], pieces.at[..., lanes(zz)], loads.at[zz]) for zz in range(4)]
    q_loads = [pltpu.make_async_copy(q_hbm.at[xx], q.at[xx], loads.at[4 + xx]) for xx in range(4)]
    for load in piece_loads + q_loads:
        load.start()
    copies = []

    def store(src, dst):
        copy = pltpu.make_async_copy(src, dst, stores.at[len(copies)])
        copy.start()
        copies.append(copy)

    for zz in range(4):
        piece_loads[zz].wait()
        for xx in range(4):
            places = [((xx - n + 1) % 4, n) for n in range(8)]
            wide = [pieces[core, g, n, :, lanes(zz)].astype(jnp.float32) for g, n in places for core in (0, 1)]
            for out, first in ((k, 0), (v, 8)):
                value = jnp.concatenate([w[first:first + 8] for w in wide], axis=0).T.astype(jnp.bfloat16)
                out[zz, :, xx] = value.reshape(4, 64, 128)
        store(k.at[zz], k_out.at[zz])
        store(v.at[zz], v_out.at[zz])
    for xx in range(4):
        q_loads[xx].wait()
        store(q.at[xx], q_out.at[:, :, xx])
    for copy in copies:
        copy.wait()


def solution(mesh):
    def local_step(x_rows, norm_gain, w_q, w_k, w_v):
        depth = x_rows.shape[1]
        half = depth // 2
        any_space = pl.BlockSpec(memory_space=pl.ANY)
        bf16, f32 = jnp.bfloat16, jnp.float32
        out = jax.ShapeDtypeStruct((4, 4, 4, 64, 128), bf16)
        q_sum, pieces = pl.pallas_call(
            functools.partial(kernel, depth, half - 5 * half // 32, 17 * half // 32),
            out_shape=(out, jax.ShapeDtypeStruct((2, 4, 8, 16, 1024), bf16)),
            in_specs=[any_space] * 5,
            out_specs=(any_space, any_space),
            scratch_shapes=[
                pltpu.VMEM((32, depth), bf16),
                pltpu.VMEM((1, depth), f32),
                pltpu.VMEM((32, half), bf16),
                pltpu.VMEM((16, half), bf16),
                pltpu.VMEM((4, 4, 2, 32, half), bf16),
                pltpu.VMEM((4, 2, half, 128), bf16),
                pltpu.VMEM((4, 2, 16, half), bf16),
                pltpu.VMEM((4, 4, 2, 4, 64, 128), f32),
                pltpu.VMEM((4, 4, 2, 16, 256), f32),
                pltpu.VMEM((2, 4, 4, 4, 64, 128), f32),
                pltpu.VMEM((2, 4, 4, 16, 256), f32),
                pltpu.VMEM((4, 4, 4, 64, 128), bf16),
                pltpu.VMEM((2, 4, 8, 16, 1024), bf16),
                DMA((7,)),
                DMA((4, 4, 2)),
                DMA((4, 2)),
                DMA((4, 4, 2)),
                DMA((3,)),
                DMA((4, 2)),
                DMA((4, 2)),
                DMA((2,)),
                DMA((2,)),
                DMA((2,)),
                DMA((2,)),
                DMA((2, 4)),
                DMA((2, 4)),
                DMA(()),
                DMA((4, 2)),
                DMA(()),
                DMA((2,)),
                DMA(()),
                DMA(()),
            ],
            compiler_params=pltpu.CompilerParams(collective_id=0, has_side_effects=True, vmem_limit_bytes=67043328),
        )(x_rows, norm_gain.reshape(1, depth), w_q.reshape(depth, 128), w_k.T, w_v.T)
        outs = pl.pallas_call(
            finish_kernel,
            out_shape=(out, out, out),
            in_specs=[any_space, any_space],
            out_specs=(any_space, any_space, any_space),
            scratch_shapes=[
                pltpu.VMEM((4, 4, 4, 64, 128), bf16),
                pltpu.VMEM((2, 4, 8, 16, 1024), bf16),
                pltpu.VMEM((4, 4, 4, 64, 128), bf16),
                pltpu.VMEM((4, 4, 4, 64, 128), bf16),
                DMA((8,)),
                DMA((12,)),
            ],
            compiler_params=pltpu.CompilerParams(vmem_limit_bytes=67043328),
        )(q_sum, pieces)
        return tuple(value.reshape(4096, 1, 128) for value in outs)

    return jax.shard_map(
        local_step,
        mesh=mesh,
        in_specs=(P(("dp", "tp"), None), P(None), P(None, "tp", None), P(None, "tp"), P(None, "tp")),
        out_specs=(P("dp", "tp", None), P("dp", "tp", None), P("dp", "tp", None)),
        check_vma=False,
    )
```

```python
import functools

import jax
import jax.numpy as jnp
from jax import lax
from jax.experimental import pallas as pl
from jax.experimental.pallas import tpu as pltpu
from jax.sharding import PartitionSpec as P

EPSILON = 1e-6
MESH = pl.DeviceIdType.MESH
DMA = pltpu.SemaphoreType.DMA


def rem(a, b):
    return lax.rem(a, b)


def kernel(
    depth, split, middle, x_hbm, gain_hbm, wq_hbm, wk_hbm, wv_hbm, q_hbm, pieces_hbm,
    x_in, gain, other, wkv_other, rows, wq, wkv, q_part, kv_part, q_got, kv_got, q_sum, pieces,
    load_sem, wide_recv, late_recv, thin_recv, row_send, wq_recv, wkv_recv, wq_send, wkv_send, q_send, kv_send, q_recv,
    kv_recv,
    piece_send, piece_recv, pair_send, pair_recv, q_left, pieces_left,
):
    half = depth // 2
    me = lax.axis_index("tp")
    c = rem(me, 2)
    x = rem(me // 2, 4)
    y = rem(me // 8, 4)
    z = me // 32
    u = z + c * (y - z)
    v = y + c * (z - y)
    mate = me + 1 - 2 * c
    d = 1 - c

    def chip(xx, uu, vv):
        zz = uu + c * (vv - uu)
        yy = vv + c * (uu - vv)
        return ((zz * 4 + yy) * 4 + xx) * 2

    def plus(a, n):
        return rem(a + n, 4)

    def send(src, dst, send_sem, recv_sem, target):
        copy = pltpu.make_async_remote_copy(
            src_ref=src, dst_ref=dst, send_sem=send_sem, recv_sem=recv_sem, device_id={"tp": target}, device_id_type=MESH
        )
        copy.start()

    def got(ref, sem):
        pltpu.make_async_copy(ref, ref, sem).wait()

    load_x = pltpu.make_async_copy(x_hbm, x_in, load_sem.at[0])
    load_x.start()
    load_gain = pltpu.make_async_copy(gain_hbm, gain, load_sem.at[6])
    load_gain.start()
    own_columns = pl.ds(pl.multiple_of(c * half, half), half)
    mate_columns = pl.ds(pl.multiple_of(d * half, half), half)
    loads = [
        pltpu.make_async_copy(wk_hbm.at[:, mate_columns], wkv_other.at[0:8], load_sem.at[1]),
        pltpu.make_async_copy(wv_hbm.at[:, mate_columns], wkv_other.at[8:16], load_sem.at[2]),
        pltpu.make_async_copy(wk_hbm.at[:, own_columns], wkv.at[u, c, 0:8], load_sem.at[3]),
        pltpu.make_async_copy(wv_hbm.at[:, own_columns], wkv.at[u, c, 8:16], load_sem.at[4]),
    ]
    for load in loads:
        load.start()
    load_wq = pltpu.make_async_copy(wq_hbm.at[own_columns, :], wq.at[u, c], load_sem.at[5])
    load_wq.start()

    barrier = pltpu.get_barrier_semaphore()
    y_pair = y + 1 - 2 * rem(y, 2)
    peers = [mate]
    for n in (1, 2, 3):
        for k in (0, 1):
            peers.append(((z * 4 + plus(y, n)) * 4 + x) * 2 + k)
            peers.append(((plus(z, n) * 4 + y) * 4 + x) * 2 + k)
        peers.append(((z * 4 + y) * 4 + plus(x, n)) * 2 + c)
        peers.append(((z * 4 + y_pair) * 4 + plus(x, n)) * 2 + c)
    for peer in peers:
        pl.semaphore_signal(barrier, inc=1, device_id={"tp": peer}, device_id_type=MESH)

    load_x.wait()
    load_gain.wait()
    width = min(1024, half)

    def squares(j, total):
        part = x_in[:, pl.ds(pl.multiple_of(j * width, width), width)].astype(jnp.float32)
        return total + part * part

    total = lax.fori_loop(0, depth // width, squares, jnp.zeros((32, width), jnp.float32))
    scale = lax.rsqrt(jnp.sum(total, axis=1, keepdims=True) / depth + EPSILON)

    def normed(first):
        columns = pl.ds(pl.multiple_of(first, width), width)
        return (x_in[:, columns].astype(jnp.float32) * scale * gain[:, columns]).astype(jnp.bfloat16)

    @pl.loop(0, half // width)
    def _(j):
        columns = pl.ds(pl.multiple_of(j * width, width), width)
        other[:, columns] = normed(d * half + j * width)
        rows[x, v, c, :, columns] = normed(c * half + j * width)

    for load in loads:
        load.wait()
    pl.semaphore_wait(barrier, len(peers))

    counts = {"wide": 0, "thin": 0, "wq": 0, "wkv": 0}
    wide, thin = slice(0, split), slice(split, half)
    early, late, whole = slice(0, middle), slice(middle, split), slice(0, half)
    rest = slice(middle, half)

    def row_sem(kind):
        counts[kind] += 1
        return row_send.at[1 if counts[kind] <= 24 else 2]

    def send_wide(xx, vv, k, *to):
        for target in to:
            send(rows.at[xx, vv, k, :, wide], rows.at[xx, vv, k, :, wide], row_sem("wide"), wide_recv.at[xx, vv, k], target)

    def send_thin(xx, vv, k, *to):
        for target in to:
            send(rows.at[xx, vv, k, :, thin], rows.at[xx, vv, k, :, thin], row_sem("thin"), thin_recv.at[xx, vv, k], target)

    def send_early(xx, k, *to):
        for target in to:
            send(rows.at[xx, vo, k, :, early], rows.at[xx, vo, k, :, early], row_send.at[2], wide_recv.at[xx, vo, k], target)

    def send_late(xx, k, *to):
        for target in to:
            send(rows.at[xx, vo, k, :, late], rows.at[xx, vo, k, :, late], row_send.at[2], late_recv.at[xx, k], target)

    def early_got(xx, k):
        got(rows.at[xx, vo, k, :, early], wide_recv.at[xx, vo, k])

    def late_got(xx, k):
        got(rows.at[xx, vo, k, :, late], late_recv.at[xx, k])

    def wide_got(xx, vv, k):
        got(rows.at[xx, vv, k, :, wide], wide_recv.at[xx, vv, k])

    def thin_got(xx, vv, k):
        got(rows.at[xx, vv, k, :, thin], thin_recv.at[xx, vv, k])

    def send_wq(src, uu, k, target):
        send(src, wq.at[uu, k], wq_send.at[counts["wq"] // 6], wq_recv.at[uu, k], target)
        counts["wq"] += 1

    def send_wkv(src, uu, k, target):
        send(src, wkv.at[uu, k], wkv_send.at[counts["wkv"] // 6], wkv_recv.at[uu, k], target)
        counts["wkv"] += 1

    def wq_got(uu, k):
        got(wq.at[uu, k], wq_recv.at[uu, k])

    def wkv_got(uu, k):
        got(wkv.at[uu, k], wkv_recv.at[uu, k])

    x_next, x_last = chip(plus(x, 1), u, v) + c, chip(plus(x, 3), u, v) + c
    v_next, v_last = chip(x, u, plus(v, 1)) + c, chip(x, u, plus(v, 3)) + c
    u_next, u_last = chip(x, plus(u, 1), v) + c, chip(x, plus(u, 3), v) + c
    xp, xm, xo = plus(x, 1), plus(x, 3), plus(x, 2)
    vp, vm, vo = plus(v, 1), plus(v, 3), plus(v, 2)
    up, um, uo = plus(u, 1), plus(u, 3), plus(u, 2)

    near_x, near_v, near_u = (x_next, x_last), (v_next, v_last), (u_next, u_last)

    send(other, rows.at[x, u, c], row_send.at[0], wide_recv.at[x, u, c], mate)
    send_thin(x, v, c, *near_x)
    send_wide(x, v, c, *near_v)
    for target in near_u:
        send_wkv(wkv.at[u, c], u, c, target)
    for target in near_u:
        send_wq(wq_hbm.at[own_columns, :], u, c, target)
    send_wkv(wkv_other, v, c, mate)
    send_wq(wq_hbm.at[mate_columns, :], v, c, mate)
    got(rows.at[x, v, d], wide_recv.at[x, v, d])
    send_thin(x, v, d, *near_x)
    send_wide(x, v, c, *near_x)
    send_wide(x, v, d, *near_v)
    send_wide(x, v, d, *near_x)
    for k in (c, d):
        send_thin(x, v, k, *near_v)
    wkv_got(u, d)
    for target in near_u:
        send_wkv(wkv.at[u, d], u, d, target)
    wq_got(u, d)
    for target in near_u:
        send_wq(wq.at[u, d], u, d, target)

    def pass_thin_x(vv):
        thin_got(xm, vv, c)
        send_thin(xm, vv, c, x_next)
        thin_got(xp, vv, d)
        send_thin(xp, vv, d, x_last)

    def pass_x(vv):
        wide_got(xm, vv, c)
        send_wide(xm, vv, c, x_next)
        wide_got(xp, vv, d)
        send_wide(xp, vv, d, x_last)

    pass_thin_x(v)
    thin_got(xm, v, d)
    thin_got(xp, v, c)
    for xx in (xm, xp):
        for k in (c, d):
            send_thin(xx, v, k, *near_v)

    wide_got(x, vm, c)
    send_wide(x, vm, c, v_next)
    wkv_got(um, c)
    send_wkv(wkv.at[um, c], um, c, u_next)
    wide_got(xm, v, c)
    send_wide(xm, v, c, x_next)
    wide_got(x, vp, c)
    for vv in (vm, vp):
        send_wide(x, vv, c, *near_x)
    wide_got(x, vp, d)
    send_wide(x, vp, d, v_last)
    wide_got(xp, v, d)
    send_wide(xp, v, d, x_last)
    wide_got(x, vm, d)
    for vv in (vm, vp):
        send_wide(x, vv, d, *near_x)
    for k in (c, d):
        thin_got(xo, v, k)
        send_thin(xo, v, k, *near_v)
    for k in (c, d):
        wide_got(x, vo, k)
        send_early(x, k, *near_x)
        send_late(x, k, *near_x)
    for xx in (x, xm, xp, xo):
        thin_got(xx, vm, c)
        send_thin(xx, vm, c, v_next)
        thin_got(xx, vp, d)
        send_thin(xx, vp, d, v_last)

    def q_block(xx, uu):
        right = jnp.concatenate([wq[uu, 0], wq[uu, 1]], axis=1)
        value = jnp.dot(rows[xx].reshape(256, half), right, preferred_element_type=jnp.float32)
        for k in (0, 1):
            q_part[xx, uu, k] = value[:, k * 128:(k + 1) * 128].reshape(4, 64, 128)

    def send_q(xx, du, whole=True):
        uu = plus(u, du)

        def to(k):
            mated = 1 - (du + 3) // 4
            send(q_part.at[xx, uu, k], q_got.at[c, u, xx], q_send.at[mated], q_recv.at[c, xx], chip(x, uu, v) + k)

        to(d)

        @pl.when(whole)
        def _():
            to(c)

    def kv_value(xx, columns):
        count = columns.stop - columns.start
        value = lax.dot_general(
            wkv[:, :, :, columns].reshape(128, count), rows[xx, :, :, :, columns].reshape(256, count),
            (((1,), (1,)), ((), ())), preferred_element_type=jnp.float32,
        )
        return value.reshape(4, 2, 16, 256)

    def send_kv(xx):
        for du in (2, 1, 3, 0):
            uu = plus(u, du)
            for k in ((c, d) if du else (d,)):
                send(kv_part.at[xx, uu, k], kv_got.at[c, u, xx], kv_send.at[0 if du else 1], kv_recv.at[c, xx], chip(x, uu, v) + k)
        kv_got[c, u, xx] = kv_part[xx, u, c]

    def far_rows(vv, first, last, columns, second=False):
        count = columns.stop - columns.start

        @pl.loop(first, last)
        def _(j):
            uu = plus(u, 2 + j)
            right = jnp.concatenate([wq[uu, 0, columns], wq[uu, 1, columns]], axis=1)
            left = rows[xo, vv, :, :, columns].reshape(64, count)
            value = jnp.dot(left, right, preferred_element_type=jnp.float32)
            for k in (0, 1):
                part = value[:, k * 128:(k + 1) * 128]
                q_part[xo, uu, k, vv] = q_part[xo, uu, k, vv] + part if second else part
            if second:
                send_q(xo, plus(j, 2), j != 2)

                @pl.when(j == 1)
                def _():
                    for g in range(3):
                        pass_on(g, pair_row + x, 0, (ahead, 3), (behind, 1))
                    for g in range(3):
                        pass_on(g, row_place + x_behind, 2, (ahead, 1))

    def far_got(vv):
        wide_got(xo, vv, c)
        wide_got(xo, vv, d)

    place = rem(y, 2) * 4 + x

    def add_kv(g, xx, direct=False):
        got(kv_got.at[0, 0:3, 0], kv_recv.at[c, xx])
        got(kv_got.at[0, :, 0], kv_recv.at[d, xx])
        for zz in range(4):
            second = jnp.concatenate([kv_got[1, yy, xx][:, zz * 64:(zz + 1) * 64] for yy in range(4)], axis=1)
            pieces[c, g, place, :, pl.ds(zz * 256, 256)] = (kv_got[0, zz, xx] + second).astype(jnp.bfloat16)
        own = pieces.at[c, g, place]
        send(own, own, piece_send, piece_recv.at[g, 0], across)
        if direct:
            for n in range(1, 4):
                send(own, own, piece_send, piece_recv.at[g, 1], row_chip(plus(x, n), y) + c)
                send(own, own, piece_send, piece_recv.at[g, 1], row_chip(plus(x, n), y_pair) + c)
        else:
            send(own, own, piece_send, piece_recv.at[g, 2], ahead)
            send(own, own, piece_send, piece_recv.at[g, 1], behind)

    def row_chip(xx, yy):
        return ((z * 4 + yy) * 4 + xx) * 2

    x_behind = plus(x, 3 - 2 * c)
    ahead, behind = row_chip(plus(x, 1 + 2 * c), y) + c, row_chip(x_behind, y) + c
    across = row_chip(x, y_pair) + c
    row_place, pair_row = place - x, 4 - place + x

    def pass_on(g, there, came, *to):
        theirs = pieces.at[c, g, there]
        got(theirs, piece_recv.at[g, came])
        for target, lands in to:
            send(theirs, theirs, piece_send, piece_recv.at[g, lands], target)

    def add_q(g, xx):
        got(q_got.at[0, 0:3, 0], q_recv.at[c, xx])
        got(q_got.at[0, :, 0], q_recv.at[d, xx])

        @pl.loop(0, 4)
        def _(zz):
            for yy in range(4):
                q_sum[xx, zz, yy] = (q_got[0, zz, xx, yy] + q_got[1, yy, xx, zz]).astype(jnp.bfloat16)

        pltpu.make_async_copy(q_sum.at[xx], q_hbm.at[xx], q_left).start()

    def share_kv(g, passed=True):
        if not passed:
            got(pieces.at[c, g, pair_row + x], piece_recv.at[g, 0])
        got(pieces.at[c, g, 0:4 if passed else 6], piece_recv.at[g, 1])
        send(pieces.at[c, g], pieces.at[c, g], pair_send, pair_recv.at[g // 3], mate)
        pltpu.make_async_copy(pieces.at[c, g], pieces_hbm.at[c, g], pieces_left).start()

    load_wq.wait()
    for vv, k in ((vm, d), (vp, c), (vo, c), (vo, d)):
        thin_got(x, vv, k)

    @pl.loop(0, 1)
    def _(i):
        q_block(x, plus(u, i))
        send_q(x, 0, False)

    wq_got(um, c)
    send_wq(wq.at[um, c], um, c, u_next)
    wkv_got(up, d)
    send_wkv(wkv.at[up, d], up, d, u_last)
    pass_x(vm)
    wq_got(up, d)
    send_wq(wq.at[up, d], up, d, u_last)
    pass_x(vp)
    wq_got(um, d)
    wq_got(up, c)

    @pl.loop(0, 2)
    def _(i):
        q_block(x, plus(um, 2 * i))
        send_q(x, plus(2 * i, 3))

    thin_got(xo, vm, d)
    thin_got(xo, vp, c)
    thin_got(xo, vo, c)
    thin_got(xo, vo, d)
    far_got(v)
    far_rows(v, 1, 4, whole)
    for xx, k, target in ((xm, c, x_next), (xp, d, x_last)):
        early_got(xx, k)
        send_early(xx, k, target)
        late_got(xx, k)
        send_late(xx, k, target)
    wkv_got(um, d)
    wkv_got(up, c)
    for k in (c, d):
        wkv_got(uo, k)
    for xx, k in ((xm, d), (xp, c)):
        for vv in (v, vm, vp):
            wide_got(xx, vv, k)
        early_got(xx, k)
        late_got(xx, k)
        for vv, kk in ((vm, d), (vp, c), (vo, c), (vo, d)):
            thin_got(xx, vv, kk)

    @pl.loop(0, 3)
    def _(g):
        xx = plus(xm, g)
        kv_part[xx] = kv_value(xx, slice(0, half))
        send_kv(xx)

    @pl.loop(0, 2)
    def _(i):
        @pl.loop(0, 3)
        def _(j):
            q_block(plus(xm, 2 * i), plus(um, j))
            send_q(plus(xm, 2 * i), plus(j, 3), j != 1)

    for k in (c, d):
        wq_got(uo, k)

    @pl.loop(0, 3)
    def _(g):
        xx = plus(xm, g)
        q_block(xx, uo)
        send_q(xx, 2)
        q_got[c, u, xx] = q_part[xx, u, c]

    for g in range(3):
        add_kv(g, plus(xm, g))
    far_rows(v, 0, 1, whole)

    @pl.loop(0, 2)
    def _(i):
        far_got(plus(vm, 2 * i))
        far_rows(plus(vm, 2 * i), 0, 4, whole)

    for k in (c, d):
        early_got(xo, k)
    kv_part[xo] = kv_value(xo, early)
    far_rows(vo, 0, 4, early)
    for k in (c, d):
        late_got(xo, k)
    kv_part[xo] = kv_part[xo] + kv_value(xo, rest)
    send_kv(xo)
    far_rows(vo, 0, 4, rest, True)
    q_got[c, u, xo] = q_part[xo, u, c]
    add_kv(3, xo, direct=True)
    for g in range(3):
        pass_on(g, pair_row + x_behind, 3, (ahead, 1))
    for g in range(3):
        add_q(g, plus(xm, g))
    for g in range(3):
        share_kv(g)

    got(pieces.at[d, 0:3], pair_recv.at[0])
    for g in range(3):
        pltpu.make_async_copy(pieces.at[d, g], pieces_hbm.at[d, g], pieces_left).start()
    share_kv(3, passed=False)

    got(other, row_send.at[0])
    got(rows.at[0:3], row_send.at[1])
    got(rows.at[3, 0:3], row_send.at[2])
    got(wq.at[0:3], wq_send.at[0])
    got(wq.at[3, 0], wq_send.at[1])
    got(wkv.at[0:3], wkv_send.at[0])
    got(wkv.at[3, 0], wkv_send.at[1])
    got(kv_part.at[0:3], kv_send.at[0])
    got(kv_part.at[3, 0:2], kv_send.at[1])

    got(pieces.at[d, 3], pair_recv.at[1])
    pltpu.make_async_copy(pieces.at[d, 3], pieces_hbm.at[d, 3], pieces_left).start()
    add_q(3, xo)
    got(q_part.at[0:3], q_send.at[0])
    got(q_part.at[3, 0:2], q_send.at[1])
    got(pieces.at[0, :, 0:7], piece_send)
    got(pieces.at[0], pair_send)
    got(q_sum, q_left)
    got(pieces, pieces_left)


def finish_kernel(q_hbm, pieces_hbm, q_out, k_out, v_out, q, pieces, k, v, loads, stores):
    def lanes(zz):
        return slice(zz * 256, (zz + 1) * 256)

    piece_loads = [pltpu.make_async_copy(pieces_hbm.at[..., lanes(zz)], pieces.at[..., lanes(zz)], loads.at[zz]) for zz in range(4)]
    q_loads = [pltpu.make_async_copy(q_hbm.at[xx], q.at[xx], loads.at[4 + xx]) for xx in range(4)]
    for load in piece_loads + q_loads:
        load.start()
    copies = []

    def store(src, dst):
        copy = pltpu.make_async_copy(src, dst, stores.at[len(copies)])
        copy.start()
        copies.append(copy)

    for zz in range(4):
        piece_loads[zz].wait()
        for xx in range(4):
            places = [((xx - n + 1) % 4, n) for n in range(8)]
            wide = [pieces[core, g, n, :, lanes(zz)].astype(jnp.float32) for g, n in places for core in (0, 1)]
            for out, first in ((k, 0), (v, 8)):
                value = jnp.concatenate([w[first:first + 8] for w in wide], axis=0).T.astype(jnp.bfloat16)
                out[zz, :, xx] = value.reshape(4, 64, 128)
        store(k.at[zz], k_out.at[zz])
        store(v.at[zz], v_out.at[zz])
    for xx in range(4):
        q_loads[xx].wait()
        store(q.at[xx], q_out.at[:, :, xx])
    for copy in copies:
        copy.wait()


def solution(mesh):
    def local_step(x_rows, norm_gain, w_q, w_k, w_v):
        depth = x_rows.shape[1]
        half = depth // 2
        any_space = pl.BlockSpec(memory_space=pl.ANY)
        bf16, f32 = jnp.bfloat16, jnp.float32
        out = jax.ShapeDtypeStruct((4, 4, 4, 64, 128), bf16)
        q_sum, pieces = pl.pallas_call(
            functools.partial(kernel, depth, half - 11 * half // 64, 17 * half // 32),
            out_shape=(out, jax.ShapeDtypeStruct((2, 4, 8, 16, 1024), bf16)),
            in_specs=[any_space] * 5,
            out_specs=(any_space, any_space),
            scratch_shapes=[
                pltpu.VMEM((32, depth), bf16),
                pltpu.VMEM((1, depth), f32),
                pltpu.VMEM((32, half), bf16),
                pltpu.VMEM((16, half), bf16),
                pltpu.VMEM((4, 4, 2, 32, half), bf16),
                pltpu.VMEM((4, 2, half, 128), bf16),
                pltpu.VMEM((4, 2, 16, half), bf16),
                pltpu.VMEM((4, 4, 2, 4, 64, 128), f32),
                pltpu.VMEM((4, 4, 2, 16, 256), f32),
                pltpu.VMEM((2, 4, 4, 4, 64, 128), f32),
                pltpu.VMEM((2, 4, 4, 16, 256), f32),
                pltpu.VMEM((4, 4, 4, 64, 128), bf16),
                pltpu.VMEM((2, 4, 8, 16, 1024), bf16),
                DMA((7,)),
                DMA((4, 4, 2)),
                DMA((4, 2)),
                DMA((4, 4, 2)),
                DMA((3,)),
                DMA((4, 2)),
                DMA((4, 2)),
                DMA((2,)),
                DMA((2,)),
                DMA((2,)),
                DMA((2,)),
                DMA((2, 4)),
                DMA((2, 4)),
                DMA(()),
                DMA((4, 4)),
                DMA(()),
                DMA((2,)),
                DMA(()),
                DMA(()),
            ],
            compiler_params=pltpu.CompilerParams(collective_id=0, has_side_effects=True, vmem_limit_bytes=67043328),
        )(x_rows, norm_gain.reshape(1, depth), w_q.reshape(depth, 128), w_k.T, w_v.T)
        outs = pl.pallas_call(
            finish_kernel,
            out_shape=(out, out, out),
            in_specs=[any_space, any_space],
            out_specs=(any_space, any_space, any_space),
            scratch_shapes=[
                pltpu.VMEM((4, 4, 4, 64, 128), bf16),
                pltpu.VMEM((2, 4, 8, 16, 1024), bf16),
                pltpu.VMEM((4, 4, 4, 64, 128), bf16),
                pltpu.VMEM((4, 4, 4, 64, 128), bf16),
                DMA((8,)),
                DMA((12,)),
            ],
            compiler_params=pltpu.CompilerParams(vmem_limit_bytes=67043328),
        )(q_sum, pieces)
        return tuple(value.reshape(4096, 1, 128) for value in outs)

    return jax.shard_map(
        local_step,
        mesh=mesh,
        in_specs=(P(("dp", "tp"), None), P(None), P(None, "tp", None), P(None, "tp"), P(None, "tp")),
        out_specs=(P("dp", "tp", None), P("dp", "tp", None), P("dp", "tp", None)),
        check_vma=False,
    )
```

```python
import functools

import jax
import jax.numpy as jnp
from jax import lax
from jax.experimental import pallas as pl
from jax.experimental.pallas import tpu as pltpu
from jax.sharding import PartitionSpec as P

EPSILON = 1e-6
MESH = pl.DeviceIdType.MESH
DMA = pltpu.SemaphoreType.DMA


def rem(a, b):
    return lax.rem(a, b)


def kernel(
    depth, split, middle, x_hbm, gain_hbm, wq_hbm, wk_hbm, wv_hbm, q_hbm, pieces_hbm,
    x_in, gain, other, wkv_other, rows, wq, wkv, q_part, kv_part, q_got, kv_got, q_sum, pieces,
    load_sem, wide_recv, late_recv, thin_recv, row_send, wq_recv, wkv_recv, wq_send, wkv_send, q_send, kv_send, q_recv,
    kv_recv,
    piece_send, piece_recv, pair_send, pair_recv, q_left, pieces_left,
):
    half = depth // 2
    me = lax.axis_index("tp")
    c = rem(me, 2)
    x = rem(me // 2, 4)
    y = rem(me // 8, 4)
    z = me // 32
    u = z + c * (y - z)
    v = y + c * (z - y)
    mate = me + 1 - 2 * c
    d = 1 - c

    def chip(xx, uu, vv):
        zz = uu + c * (vv - uu)
        yy = vv + c * (uu - vv)
        return ((zz * 4 + yy) * 4 + xx) * 2

    def plus(a, n):
        return rem(a + n, 4)

    def send(src, dst, send_sem, recv_sem, target):
        copy = pltpu.make_async_remote_copy(
            src_ref=src, dst_ref=dst, send_sem=send_sem, recv_sem=recv_sem, device_id={"tp": target}, device_id_type=MESH
        )
        copy.start()

    def got(ref, sem):
        pltpu.make_async_copy(ref, ref, sem).wait()

    load_x = pltpu.make_async_copy(x_hbm, x_in, load_sem.at[0])
    load_x.start()
    load_gain = pltpu.make_async_copy(gain_hbm, gain, load_sem.at[6])
    load_gain.start()
    own_columns = pl.ds(pl.multiple_of(c * half, half), half)
    mate_columns = pl.ds(pl.multiple_of(d * half, half), half)
    loads = [
        pltpu.make_async_copy(wk_hbm.at[:, mate_columns], wkv_other.at[0:8], load_sem.at[1]),
        pltpu.make_async_copy(wv_hbm.at[:, mate_columns], wkv_other.at[8:16], load_sem.at[2]),
        pltpu.make_async_copy(wk_hbm.at[:, own_columns], wkv.at[u, c, 0:8], load_sem.at[3]),
        pltpu.make_async_copy(wv_hbm.at[:, own_columns], wkv.at[u, c, 8:16], load_sem.at[4]),
    ]
    for load in loads:
        load.start()
    load_wq = pltpu.make_async_copy(wq_hbm.at[own_columns, :], wq.at[u, c], load_sem.at[5])
    load_wq.start()

    barrier = pltpu.get_barrier_semaphore()
    y_pair = y + 1 - 2 * rem(y, 2)
    peers = [mate]
    for n in (1, 2, 3):
        for k in (0, 1):
            peers.append(((z * 4 + plus(y, n)) * 4 + x) * 2 + k)
            peers.append(((plus(z, n) * 4 + y) * 4 + x) * 2 + k)
        peers.append(((z * 4 + y) * 4 + plus(x, n)) * 2 + c)
        peers.append(((z * 4 + y_pair) * 4 + plus(x, n)) * 2 + c)
    for peer in peers:
        pl.semaphore_signal(barrier, inc=1, device_id={"tp": peer}, device_id_type=MESH)

    load_x.wait()
    load_gain.wait()
    width = min(1024, half)

    def squares(j, total):
        part = x_in[:, pl.ds(pl.multiple_of(j * width, width), width)].astype(jnp.float32)
        return total + part * part

    total = lax.fori_loop(0, depth // width, squares, jnp.zeros((32, width), jnp.float32))
    scale = lax.rsqrt(jnp.sum(total, axis=1, keepdims=True) / depth + EPSILON)

    def normed(first):
        columns = pl.ds(pl.multiple_of(first, width), width)
        return (x_in[:, columns].astype(jnp.float32) * scale * gain[:, columns]).astype(jnp.bfloat16)

    @pl.loop(0, half // width)
    def _(j):
        columns = pl.ds(pl.multiple_of(j * width, width), width)
        other[:, columns] = normed(d * half + j * width)
        rows[x, v, c, :, columns] = normed(c * half + j * width)

    for load in loads:
        load.wait()
    pl.semaphore_wait(barrier, len(peers))

    counts = {"wide": 0, "thin": 0, "wq": 0, "wkv": 0}
    wide, thin = slice(0, split), slice(split, half)
    early, late, whole = slice(0, middle), slice(middle, split), slice(0, half)
    rest = slice(middle, half)

    def row_sem(kind):
        counts[kind] += 1
        return row_send.at[1 if counts[kind] <= 24 else 2]

    def send_wide(xx, vv, k, *to):
        for target in to:
            send(rows.at[xx, vv, k, :, wide], rows.at[xx, vv, k, :, wide], row_sem("wide"), wide_recv.at[xx, vv, k], target)

    def send_thin(xx, vv, k, *to):
        for target in to:
            send(rows.at[xx, vv, k, :, thin], rows.at[xx, vv, k, :, thin], row_sem("thin"), thin_recv.at[xx, vv, k], target)

    def send_early(xx, k, *to):
        for target in to:
            send(rows.at[xx, vo, k, :, early], rows.at[xx, vo, k, :, early], row_send.at[2], wide_recv.at[xx, vo, k], target)

    def send_late(xx, k, *to):
        for target in to:
            send(rows.at[xx, vo, k, :, late], rows.at[xx, vo, k, :, late], row_send.at[2], late_recv.at[xx, k], target)

    def early_got(xx, k):
        got(rows.at[xx, vo, k, :, early], wide_recv.at[xx, vo, k])

    def late_got(xx, k):
        got(rows.at[xx, vo, k, :, late], late_recv.at[xx, k])

    def wide_got(xx, vv, k):
        got(rows.at[xx, vv, k, :, wide], wide_recv.at[xx, vv, k])

    def thin_got(xx, vv, k):
        got(rows.at[xx, vv, k, :, thin], thin_recv.at[xx, vv, k])

    def send_wq(src, uu, k, target):
        send(src, wq.at[uu, k], wq_send.at[counts["wq"] // 6], wq_recv.at[uu, k], target)
        counts["wq"] += 1

    def send_wkv(src, uu, k, target):
        send(src, wkv.at[uu, k], wkv_send.at[counts["wkv"] // 6], wkv_recv.at[uu, k], target)
        counts["wkv"] += 1

    def wq_got(uu, k):
        got(wq.at[uu, k], wq_recv.at[uu, k])

    def wkv_got(uu, k):
        got(wkv.at[uu, k], wkv_recv.at[uu, k])

    x_next, x_last = chip(plus(x, 1), u, v) + c, chip(plus(x, 3), u, v) + c
    v_next, v_last = chip(x, u, plus(v, 1)) + c, chip(x, u, plus(v, 3)) + c
    u_next, u_last = chip(x, plus(u, 1), v) + c, chip(x, plus(u, 3), v) + c
    xp, xm, xo = plus(x, 1), plus(x, 3), plus(x, 2)
    vp, vm, vo = plus(v, 1), plus(v, 3), plus(v, 2)
    up, um, uo = plus(u, 1), plus(u, 3), plus(u, 2)

    near_x, near_v, near_u = (x_next, x_last), (v_next, v_last), (u_next, u_last)

    send(other, rows.at[x, u, c], row_send.at[0], wide_recv.at[x, u, c], mate)
    send_thin(x, v, c, *near_x)
    send_wide(x, v, c, *near_v)
    for target in near_u:
        send_wkv(wkv.at[u, c], u, c, target)
    for target in near_u:
        send_wq(wq_hbm.at[own_columns, :], u, c, target)
    send_wkv(wkv_other, v, c, mate)
    send_wq(wq_hbm.at[mate_columns, :], v, c, mate)
    got(rows.at[x, v, d], wide_recv.at[x, v, d])
    send_thin(x, v, d, *near_x)
    send_wide(x, v, c, *near_x)
    send_wide(x, v, d, *near_v)
    send_wide(x, v, d, *near_x)
    for k in (c, d):
        send_thin(x, v, k, *near_v)
    wkv_got(u, d)
    for target in near_u:
        send_wkv(wkv.at[u, d], u, d, target)
    wq_got(u, d)
    for target in near_u:
        send_wq(wq.at[u, d], u, d, target)

    def pass_thin_x(vv):
        thin_got(xm, vv, c)
        send_thin(xm, vv, c, x_next)
        thin_got(xp, vv, d)
        send_thin(xp, vv, d, x_last)

    def pass_x(vv):
        wide_got(xm, vv, c)
        send_wide(xm, vv, c, x_next)
        wide_got(xp, vv, d)
        send_wide(xp, vv, d, x_last)

    pass_thin_x(v)
    thin_got(xm, v, d)
    thin_got(xp, v, c)
    for xx in (xm, xp):
        for k in (c, d):
            send_thin(xx, v, k, *near_v)

    wide_got(x, vm, c)
    send_wide(x, vm, c, v_next)
    wkv_got(um, c)
    send_wkv(wkv.at[um, c], um, c, u_next)
    wide_got(xm, v, c)
    send_wide(xm, v, c, x_next)
    wide_got(x, vp, c)
    for vv in (vm, vp):
        send_wide(x, vv, c, *near_x)
    wide_got(x, vp, d)
    send_wide(x, vp, d, v_last)
    wide_got(xp, v, d)
    send_wide(xp, v, d, x_last)
    wide_got(x, vm, d)
    for vv in (vm, vp):
        send_wide(x, vv, d, *near_x)
    for k in (c, d):
        thin_got(xo, v, k)
        send_thin(xo, v, k, *near_v)
    for k in (c, d):
        wide_got(x, vo, k)
        send_early(x, k, *near_x)
        send_late(x, k, *near_x)
    for xx in (x, xm, xp, xo):
        thin_got(xx, vm, c)
        send_thin(xx, vm, c, v_next)
        thin_got(xx, vp, d)
        send_thin(xx, vp, d, v_last)

    def q_block(xx, uu):
        right = jnp.concatenate([wq[uu, 0], wq[uu, 1]], axis=1)
        value = jnp.dot(rows[xx].reshape(256, half), right, preferred_element_type=jnp.float32)
        for k in (0, 1):
            q_part[xx, uu, k] = value[:, k * 128:(k + 1) * 128].reshape(4, 64, 128)

    def send_q(xx, du, whole=True):
        uu = plus(u, du)

        def to(k):
            mated = 1 - (du + 3) // 4
            send(q_part.at[xx, uu, k], q_got.at[c, u, xx], q_send.at[mated], q_recv.at[c, xx], chip(x, uu, v) + k)

        to(d)

        @pl.when(whole)
        def _():
            to(c)

    def kv_value(xx, columns):
        count = columns.stop - columns.start
        value = lax.dot_general(
            wkv[:, :, :, columns].reshape(128, count), rows[xx, :, :, :, columns].reshape(256, count),
            (((1,), (1,)), ((), ())), preferred_element_type=jnp.float32,
        )
        return value.reshape(4, 2, 16, 256)

    def send_kv(xx):
        for du in (2, 1, 3, 0):
            uu = plus(u, du)
            for k in ((c, d) if du else (d,)):
                send(kv_part.at[xx, uu, k], kv_got.at[c, u, xx], kv_send.at[0 if du else 1], kv_recv.at[c, xx], chip(x, uu, v) + k)
        kv_got[c, u, xx] = kv_part[xx, u, c]

    def far_rows(vv, first, last, columns, second=False):
        count = columns.stop - columns.start

        @pl.loop(first, last)
        def _(j):
            uu = plus(u, 2 + j)
            right = jnp.concatenate([wq[uu, 0, columns], wq[uu, 1, columns]], axis=1)
            left = rows[xo, vv, :, :, columns].reshape(64, count)
            value = jnp.dot(left, right, preferred_element_type=jnp.float32)
            for k in (0, 1):
                part = value[:, k * 128:(k + 1) * 128]
                q_part[xo, uu, k, vv] = q_part[xo, uu, k, vv] + part if second else part
            if second:
                send_q(xo, plus(j, 2), j != 2)

                @pl.when(j == 1)
                def _():
                    for g in range(3):
                        pass_on(g, pair_row + x, 0, (ahead, 3), (behind, 1))
                    for g in range(3):
                        pass_on(g, row_place + x_behind, 2, (ahead, 1))

    def far_got(vv):
        wide_got(xo, vv, c)
        wide_got(xo, vv, d)

    place = rem(y, 2) * 4 + x

    def add_kv(g, xx, direct=False):
        got(kv_got.at[0, 0:3, 0], kv_recv.at[c, xx])
        got(kv_got.at[0, :, 0], kv_recv.at[d, xx])
        for zz in range(4):
            second = jnp.concatenate([kv_got[1, yy, xx][:, zz * 64:(zz + 1) * 64] for yy in range(4)], axis=1)
            pieces[c, g, place, :, pl.ds(zz * 256, 256)] = (kv_got[0, zz, xx] + second).astype(jnp.bfloat16)
        own = pieces.at[c, g, place]
        send(own, own, piece_send, piece_recv.at[g, 0], across)
        if direct:
            for n in range(1, 4):
                send(own, own, piece_send, piece_recv.at[g, 1], row_chip(plus(x, n), y) + c)
                send(own, own, piece_send, piece_recv.at[g, 1], row_chip(plus(x, n), y_pair) + c)
        else:
            send(own, own, piece_send, piece_recv.at[g, 2], ahead)
            send(own, own, piece_send, piece_recv.at[g, 1], behind)

    def row_chip(xx, yy):
        return ((z * 4 + yy) * 4 + xx) * 2

    x_behind = plus(x, 3 - 2 * c)
    ahead, behind = row_chip(plus(x, 1 + 2 * c), y) + c, row_chip(x_behind, y) + c
    across = row_chip(x, y_pair) + c
    row_place, pair_row = place - x, 4 - place + x

    def pass_on(g, there, came, *to):
        theirs = pieces.at[c, g, there]
        got(theirs, piece_recv.at[g, came])
        for target, lands in to:
            send(theirs, theirs, piece_send, piece_recv.at[g, lands], target)

    def add_q(g, xx):
        got(q_got.at[0, 0:3, 0], q_recv.at[c, xx])
        got(q_got.at[0, :, 0], q_recv.at[d, xx])

        @pl.loop(0, 4)
        def _(zz):
            for yy in range(4):
                q_sum[xx, zz, yy] = (q_got[0, zz, xx, yy] + q_got[1, yy, xx, zz]).astype(jnp.bfloat16)

        pltpu.make_async_copy(q_sum.at[xx], q_hbm.at[xx], q_left).start()

    def share_kv(g, passed=True):
        if not passed:
            got(pieces.at[c, g, pair_row + x], piece_recv.at[g, 0])
        got(pieces.at[c, g, 0:4 if passed else 6], piece_recv.at[g, 1])
        send(pieces.at[c, g], pieces.at[c, g], pair_send, pair_recv.at[g // 3], mate)
        pltpu.make_async_copy(pieces.at[c, g], pieces_hbm.at[c, g], pieces_left).start()

    load_wq.wait()
    for vv, k in ((vm, d), (vp, c), (vo, c), (vo, d)):
        thin_got(x, vv, k)

    @pl.loop(0, 1)
    def _(i):
        q_block(x, plus(u, i))
        send_q(x, 0, False)

    wq_got(um, c)
    send_wq(wq.at[um, c], um, c, u_next)
    wkv_got(up, d)
    send_wkv(wkv.at[up, d], up, d, u_last)
    pass_x(vm)
    wq_got(up, d)
    send_wq(wq.at[up, d], up, d, u_last)
    pass_x(vp)
    wq_got(um, d)
    wq_got(up, c)

    @pl.loop(0, 2)
    def _(i):
        q_block(x, plus(um, 2 * i))
        send_q(x, plus(2 * i, 3))

    thin_got(xo, vm, d)
    thin_got(xo, vp, c)
    thin_got(xo, vo, c)
    thin_got(xo, vo, d)
    far_got(v)
    far_rows(v, 1, 4, whole)
    for xx, k, target in ((xm, c, x_next), (xp, d, x_last)):
        early_got(xx, k)
        send_early(xx, k, target)
        late_got(xx, k)
        send_late(xx, k, target)
    wkv_got(um, d)
    wkv_got(up, c)
    for k in (c, d):
        wkv_got(uo, k)
    for xx, k in ((xm, d), (xp, c)):
        for vv in (v, vm, vp):
            wide_got(xx, vv, k)
        early_got(xx, k)
        late_got(xx, k)
        for vv, kk in ((vm, d), (vp, c), (vo, c), (vo, d)):
            thin_got(xx, vv, kk)

    @pl.loop(0, 3)
    def _(g):
        xx = plus(xm, g)
        kv_part[xx] = kv_value(xx, slice(0, half))
        send_kv(xx)

    @pl.loop(0, 2)
    def _(i):
        @pl.loop(0, 3)
        def _(j):
            q_block(plus(xm, 2 * i), plus(um, j))
            send_q(plus(xm, 2 * i), plus(j, 3), j != 1)

    for k in (c, d):
        wq_got(uo, k)

    @pl.loop(0, 3)
    def _(g):
        xx = plus(xm, g)
        q_block(xx, uo)
        send_q(xx, 2)
        q_got[c, u, xx] = q_part[xx, u, c]

    for g in range(3):
        add_kv(g, plus(xm, g))
    far_rows(v, 0, 1, whole)

    @pl.loop(0, 2)
    def _(i):
        far_got(plus(vm, 2 * i))
        far_rows(plus(vm, 2 * i), 0, 4, whole)

    for k in (c, d):
        early_got(xo, k)
    kv_part[xo] = kv_value(xo, early)
    far_rows(vo, 0, 4, early)
    for k in (c, d):
        late_got(xo, k)
    kv_part[xo] = kv_part[xo] + kv_value(xo, rest)
    send_kv(xo)
    far_rows(vo, 0, 4, rest, True)
    q_got[c, u, xo] = q_part[xo, u, c]
    add_kv(3, xo, direct=True)
    for g in range(3):
        pass_on(g, pair_row + x_behind, 3, (ahead, 1))
    for g in range(3):
        add_q(g, plus(xm, g))
    for g in range(3):
        share_kv(g)

    share_kv(3, passed=False)
    add_q(3, xo)
    got(pieces.at[d, 0:3], pair_recv.at[0])
    for g in range(3):
        pltpu.make_async_copy(pieces.at[d, g], pieces_hbm.at[d, g], pieces_left).start()
    got(pieces.at[d, 3], pair_recv.at[1])
    pltpu.make_async_copy(pieces.at[d, 3], pieces_hbm.at[d, 3], pieces_left).start()

    got(other, row_send.at[0])
    got(rows.at[0:3], row_send.at[1])
    got(rows.at[3, 0:3], row_send.at[2])
    got(wq.at[0:3], wq_send.at[0])
    got(wq.at[3, 0], wq_send.at[1])
    got(wkv.at[0:3], wkv_send.at[0])
    got(wkv.at[3, 0], wkv_send.at[1])
    got(kv_part.at[0:3], kv_send.at[0])
    got(kv_part.at[3, 0:2], kv_send.at[1])

    got(q_part.at[0:3], q_send.at[0])
    got(q_part.at[3, 0:2], q_send.at[1])
    got(pieces.at[0, :, 0:7], piece_send)
    got(pieces.at[0], pair_send)
    got(q_sum, q_left)
    got(pieces, pieces_left)


def finish_kernel(q_hbm, pieces_hbm, q_out, k_out, v_out, q, pieces, k, v, loads, stores):
    def lanes(zz):
        return slice(zz * 256, (zz + 1) * 256)

    piece_loads = [pltpu.make_async_copy(pieces_hbm.at[..., lanes(zz)], pieces.at[..., lanes(zz)], loads.at[zz]) for zz in range(4)]
    q_loads = [pltpu.make_async_copy(q_hbm.at[xx], q.at[xx], loads.at[4 + xx]) for xx in range(4)]
    for load in piece_loads + q_loads:
        load.start()
    copies = []

    def store(src, dst):
        copy = pltpu.make_async_copy(src, dst, stores.at[len(copies)])
        copy.start()
        copies.append(copy)

    for zz in range(4):
        piece_loads[zz].wait()
        for xx in range(4):
            places = [((xx - n + 1) % 4, n) for n in range(8)]
            wide = [pieces[core, g, n, :, lanes(zz)].astype(jnp.float32) for g, n in places for core in (0, 1)]
            for out, first in ((k, 0), (v, 8)):
                value = jnp.concatenate([w[first:first + 8] for w in wide], axis=0).T.astype(jnp.bfloat16)
                out[zz, :, xx] = value.reshape(4, 64, 128)
        store(k.at[zz], k_out.at[zz])
        store(v.at[zz], v_out.at[zz])
    for xx in range(4):
        q_loads[xx].wait()
        store(q.at[xx], q_out.at[:, :, xx])
    for copy in copies:
        copy.wait()


def solution(mesh):
    def local_step(x_rows, norm_gain, w_q, w_k, w_v):
        depth = x_rows.shape[1]
        half = depth // 2
        any_space = pl.BlockSpec(memory_space=pl.ANY)
        bf16, f32 = jnp.bfloat16, jnp.float32
        out = jax.ShapeDtypeStruct((4, 4, 4, 64, 128), bf16)
        q_sum, pieces = pl.pallas_call(
            functools.partial(kernel, depth, half - 11 * half // 64, 17 * half // 32),
            out_shape=(out, jax.ShapeDtypeStruct((2, 4, 8, 16, 1024), bf16)),
            in_specs=[any_space] * 5,
            out_specs=(any_space, any_space),
            scratch_shapes=[
                pltpu.VMEM((32, depth), bf16),
                pltpu.VMEM((1, depth), f32),
                pltpu.VMEM((32, half), bf16),
                pltpu.VMEM((16, half), bf16),
                pltpu.VMEM((4, 4, 2, 32, half), bf16),
                pltpu.VMEM((4, 2, half, 128), bf16),
                pltpu.VMEM((4, 2, 16, half), bf16),
                pltpu.VMEM((4, 4, 2, 4, 64, 128), f32),
                pltpu.VMEM((4, 4, 2, 16, 256), f32),
                pltpu.VMEM((2, 4, 4, 4, 64, 128), f32),
                pltpu.VMEM((2, 4, 4, 16, 256), f32),
                pltpu.VMEM((4, 4, 4, 64, 128), bf16),
                pltpu.VMEM((2, 4, 8, 16, 1024), bf16),
                DMA((7,)),
                DMA((4, 4, 2)),
                DMA((4, 2)),
                DMA((4, 4, 2)),
                DMA((3,)),
                DMA((4, 2)),
                DMA((4, 2)),
                DMA((2,)),
                DMA((2,)),
                DMA((2,)),
                DMA((2,)),
                DMA((2, 4)),
                DMA((2, 4)),
                DMA(()),
                DMA((4, 4)),
                DMA(()),
                DMA((2,)),
                DMA(()),
                DMA(()),
            ],
            compiler_params=pltpu.CompilerParams(collective_id=0, has_side_effects=True, vmem_limit_bytes=67043328),
        )(x_rows, norm_gain.reshape(1, depth), w_q.reshape(depth, 128), w_k.T, w_v.T)
        outs = pl.pallas_call(
            finish_kernel,
            out_shape=(out, out, out),
            in_specs=[any_space, any_space],
            out_specs=(any_space, any_space, any_space),
            scratch_shapes=[
                pltpu.VMEM((4, 4, 4, 64, 128), bf16),
                pltpu.VMEM((2, 4, 8, 16, 1024), bf16),
                pltpu.VMEM((4, 4, 4, 64, 128), bf16),
                pltpu.VMEM((4, 4, 4, 64, 128), bf16),
                DMA((8,)),
                DMA((12,)),
            ],
            compiler_params=pltpu.CompilerParams(vmem_limit_bytes=67043328),
        )(q_sum, pieces)
        return tuple(value.reshape(4096, 1, 128) for value in outs)

    return jax.shard_map(
        local_step,
        mesh=mesh,
        in_specs=(P(("dp", "tp"), None), P(None), P(None, "tp", None), P(None, "tp"), P(None, "tp")),
        out_specs=(P("dp", "tp", None), P("dp", "tp", None), P("dp", "tp", None)),
        check_vma=False,
    )
```
